32 devices in a mesh: dp: 1 (over z), sp: 32 (over y, x, core).
Axes of the slice: x: 4, y: 4, z: 1, core: 2. Of those that a mesh axis runs over, the one named last changes fastest.
The devices are a block of a 4x4x8 slice.
Arguments:
- hidden: bfloat16 [512, 2048], P(('dp', 'sp'))
- w_q: bfloat16 [2048, 4096], replicated
- w_k: bfloat16 [2048, 512], replicated
- w_v: bfloat16 [2048, 512], replicated
- w_o: bfloat16 [4096, 2048], replicated
- expert_ids: int32 [512, 2], P(('dp', 'sp'))
- router_probs: float32 [512, 128], P(('dp', 'sp'))
Outputs:
- output 1: bfloat16 [512, 2048], P(('dp', 'sp'))
- output 2: bfloat16 [128, 512, 2048], P(('dp', 'sp'))
All inputs are finite; a program needn't handle non-finite values.
Results may differ from the reference program's by a relative error of at most 0.00957174.
Values are sent between devices in bfloat16 or wider.
A program may use at most 768 MiB of HBM per device.

```python
import math
import jax
import jax.numpy as jnp
from jax import lax

D = 2048
HEADS = 32
KV_HEADS = 4
HEAD = 128
EXPERTS = 128
TOKENS_DEV = 16
GROUP = 32

SEQ = TOKENS_DEV * GROUP
Q_PER_KV = HEADS // KV_HEADS
Q_WIDTH = HEADS * HEAD
KV_WIDTH = KV_HEADS * HEAD
SCORE_SCALE = 1.0 / math.sqrt(HEAD)


def draw_routes(route_key):
    key_first, key_second, key_pick, key_cold, key_order = jax.random.split(route_key, 5)
    hot_first = jax.random.randint(key_first, (), 0, EXPERTS)
    hot_second = (hot_first + 1 + jax.random.randint(key_second, (), 0, EXPERTS - 1)) % EXPERTS
    pick_hot = jax.random.randint(key_pick, (SEQ,), 0, 2)
    cold_ids = (hot_first + 1 + jax.random.randint(key_cold, (SEQ,), 0, EXPERTS - 1)) % EXPERTS
    other_ids = jnp.where(pick_hot == 1, hot_second, cold_ids)
    first_ids = jnp.full((SEQ,), hot_first)
    swap_bits = jax.random.randint(key_order, (SEQ,), 0, 2)
    col_zero = jnp.where(swap_bits == 1, other_ids, first_ids)
    col_one = jnp.where(swap_bits == 1, first_ids, other_ids)
    return jnp.stack([col_zero, col_one], axis=1).astype(jnp.int32)


def setup_inputs(seed: int = 0, part: int = 0) -> dict:
    base_key = jax.random.key(seed)
    part_key = jax.random.fold_in(base_key, part)
    weight_keys = jax.random.split(base_key, 4)
    part_keys = jax.random.split(part_key, 3)
    q_gain = math.sqrt(0.5 * math.log(SEQ))
    o_gain = 0.5 * SEQ ** 0.25
    hidden = jax.random.normal(part_keys[0], (SEQ, D), jnp.float32).astype(jnp.bfloat16)
    w_q = (jax.random.normal(weight_keys[0], (D, Q_WIDTH), jnp.float32) * (q_gain / math.sqrt(D))).astype(jnp.bfloat16)
    w_k = (jax.random.normal(weight_keys[1], (D, KV_WIDTH), jnp.float32) / math.sqrt(D)).astype(jnp.bfloat16)
    w_v = (jax.random.normal(weight_keys[2], (D, KV_WIDTH), jnp.float32) / math.sqrt(D)).astype(jnp.bfloat16)
    w_o = (jax.random.normal(weight_keys[3], (Q_WIDTH, D), jnp.float32) * (o_gain / math.sqrt(Q_WIDTH))).astype(jnp.bfloat16)
    expert_ids = draw_routes(part_keys[1])
    router_probs = jax.nn.softmax(1.5 * jax.random.normal(part_keys[2], (SEQ, EXPERTS), jnp.float32), axis=1)
    return {'hidden': hidden, 'w_q': w_q, 'w_k': w_k, 'w_v': w_v, 'w_o': w_o, 'expert_ids': expert_ids, 'router_probs': router_probs}


def reference(hidden, w_q, w_k, w_v, w_o, expert_ids, router_probs):
    q_all = jnp.dot(hidden, w_q, preferred_element_type=jnp.float32).astype(jnp.bfloat16)
    k_all = jnp.dot(hidden, w_k, preferred_element_type=jnp.float32).astype(jnp.bfloat16)
    v_all = jnp.dot(hidden, w_v, preferred_element_type=jnp.float32).astype(jnp.bfloat16)
    q_groups = q_all.reshape(SEQ, KV_HEADS, Q_PER_KV, HEAD).transpose(1, 0, 2, 3)
    k_groups = k_all.reshape(SEQ, KV_HEADS, HEAD).transpose(1, 0, 2)
    v_groups = v_all.reshape(SEQ, KV_HEADS, HEAD).transpose(1, 0, 2)
    positions = jnp.arange(SEQ)
    causal = positions[:, None] >= positions[None, :]

    def one_group(group_in):
        q_grp, k_grp, v_grp = group_in
        scores = jnp.einsum('qmd,kd->mqk', q_grp.astype(jnp.float32), k_grp.astype(jnp.float32)) * SCORE_SCALE
        scores = jnp.where(causal[None, :, :], scores, -1e30)
        weights = jax.nn.softmax(scores, axis=-1).astype(jnp.bfloat16)
        out_grp = jnp.einsum('mqk,kd->qmd', weights.astype(jnp.float32), v_grp.astype(jnp.float32))
        return out_grp.astype(jnp.bfloat16)

    attn_out = lax.map(one_group, (q_groups, k_groups, v_groups))
    attn_out = attn_out.transpose(1, 0, 2, 3).reshape(SEQ, Q_WIDTH)
    out_proj = jnp.dot(attn_out, w_o, preferred_element_type=jnp.float32)
    hidden_out = (hidden.astype(jnp.float32) + out_proj).astype(jnp.bfloat16)
    picked = jnp.take_along_axis(router_probs, expert_ids, axis=1)
    gate_w = picked / jnp.sum(picked, axis=1, keepdims=True)
    gated = (gate_w[:, :, None] * hidden_out.astype(jnp.float32)[:, None, :]).astype(jnp.bfloat16)
    ids_blk = expert_ids.reshape(GROUP, TOKENS_DEV, 2)
    token_hits = jnp.sum((ids_blk[:, :, :, None] == jnp.arange(EXPERTS)).astype(jnp.int32), axis=2)
    earlier = jnp.cumsum(token_hits, axis=1) - token_hits
    slot_rank = jnp.take_along_axis(earlier, ids_blk, axis=2)
    dest_rows = jnp.arange(GROUP)[:, None, None] * TOKENS_DEV + slot_rank
    buffer = jnp.zeros((EXPERTS, GROUP * TOKENS_DEV, D), jnp.bfloat16)
    buffer = buffer.at[ids_blk, dest_rows].set(gated.reshape(GROUP, TOKENS_DEV, 2, D))
    return (hidden_out, buffer)
```

```python
import functools
import math

import jax
import jax.numpy as jnp
from jax import lax
from jax.experimental import pallas as pl
from jax.experimental.pallas import tpu as pltpu
from jax.sharding import PartitionSpec as P

HEAD_DIM = 128
SCORE_SCALE = 1.0 / math.sqrt(HEAD_DIM)
MESH_IDS = pl.DeviceIdType.MESH
LANES = 128
CORES = 2
Q_COLS = 512
F32 = jnp.float32
BF16 = jnp.bfloat16


def block_kernel(side, x_hbm, wq_hbm, wk_hbm, wv_hbm, wo_hbm, ids_ref, probs_ref,
                 buf_out, h_out,
                 xbuf, wq_v, wk_v, wv_v, wo_v, kvbuf, meta_own, meta_buf, q_s, o_own, o_sib, h_buf, sel_s, gate_s,
                 wsem, xsem, pair_send, pair_recv, kv_send, kv_recv, mt_send, mt_recv, h_send, h_recv,
                 d_send, d_recv):
    tok = x_hbm.shape[0]
    width = x_hbm.shape[1]
    tok2 = CORES * tok
    half_q = wq_v.shape[1]
    half_kv = wk_v.shape[1]
    half_w = wo_v.shape[1]
    kv_half_heads = half_kv // HEAD_DIM
    q_half_heads = half_q // HEAD_DIM
    per_kv = q_half_heads // kv_half_heads
    own_experts = buf_out.shape[0]
    experts = probs_ref.shape[1]
    n_chips = side * side

    me = lax.axis_index('sp')
    core = me % CORES
    chip = me // CORES
    cy = chip // side
    cx = chip % side
    a0 = cx + (cy - cx) * core
    b0 = cy + (cx - cy) * core

    def chip_of(da, db):
        a = (a0 + (da + side)) % side
        b = (b0 + (db + side)) % side
        y = b + (a - b) * core
        x = a + (b - a) * core
        return y * side + x

    def dev_of(da, db):
        return {'sp': chip_of(da, db) * CORES + core}

    sib = {'sp': chip * CORES + (1 - core)}

    my_rows = pl.ds(pl.multiple_of(core * tok, tok), tok)
    x_load = pltpu.make_async_copy(x_hbm, xbuf.at[my_rows, :], xsem)
    x_load.start()
    loads = {}

    def load(name, src, dst):
        loads[name] = pltpu.make_async_copy(src, dst, wsem.at[len(loads)])
        loads[name].start()

    kv_cols = pl.ds(pl.multiple_of(core * half_kv, half_kv), half_kv)
    load('k', wk_hbm.at[:, kv_cols], wk_v)
    load('v', wv_hbm.at[:, kv_cols], wv_v)
    n_q = half_q // Q_COLS
    for i in range(n_q):
        load(('q', i), wq_hbm.at[:, pl.ds(pl.multiple_of(core * half_q + i * Q_COLS, Q_COLS), Q_COLS)],
             wq_v.at[:, pl.ds(i * Q_COLS, Q_COLS)])
    o_cols = pl.ds(pl.multiple_of(core * half_w, half_w), half_w)
    load('o0', wo_hbm.at[pl.ds(pl.multiple_of(core * half_q, half_q), half_q), o_cols], wo_v.at[pl.ds(0, half_q), :])
    load('o1', wo_hbm.at[pl.ds(pl.multiple_of((1 - core) * half_q, half_q), half_q), o_cols],
         wo_v.at[pl.ds(half_q, half_q), :])

    barrier = pltpu.get_barrier_semaphore()
    partners = [dev_of(1, 0), dev_of(-1, 0), dev_of(0, 1), dev_of(0, -1), sib]
    for p in partners:
        pl.semaphore_signal(barrier, inc=1, device_id=p, device_id_type=MESH_IDS)

    ids = ids_ref[...]
    probs = probs_ref[...]
    lane_e = lax.broadcasted_iota(jnp.int32, (tok, experts), 1)
    p0 = jnp.sum(jnp.where(lane_e == ids[:, 0:1], probs, 0.0), axis=1, keepdims=True)
    p1 = jnp.sum(jnp.where(lane_e == ids[:, 1:2], probs, 0.0), axis=1, keepdims=True)
    psum = p0 + p1
    idf = ids.astype(F32)
    lane_t = lax.broadcasted_iota(jnp.int32, (tok, LANES), 1)
    row_t = lax.broadcasted_iota(jnp.int32, (tok, LANES), 0)
    eye = lane_t == row_t + core * tok

    def to_lanes(col):
        return jnp.sum(jnp.where(eye, col, 0.0), axis=0, keepdims=True)

    meta_rows = [to_lanes(idf[:, 0:1]), to_lanes(idf[:, 1:2]), to_lanes(p0 / psum), to_lanes(p1 / psum)]
    meta_own[0] = jnp.concatenate(meta_rows + [jnp.zeros((4, LANES), F32)], axis=0)

    def remote(src, dst, ss, rs, dev):
        return pltpu.make_async_remote_copy(src_ref=src, dst_ref=dst, send_sem=ss, recv_sem=rs,
                                            device_id=dev, device_id_type=MESH_IDS)

    x_load.wait()
    pl.semaphore_wait(barrier, len(partners))
    x_pair = remote(xbuf.at[my_rows, :], xbuf.at[my_rows, :], pair_send.at[0], pair_recv.at[0], sib)
    x_pair.start()
    m_pair = remote(meta_own.at[0], meta_own.at[1], pair_send.at[1], pair_recv.at[1], sib)
    m_pair.start()

    started = []

    class Gather:
        def __init__(self, items):
            self.items = items
            self.flight = {}

        def start(self, key, n, da, db, to_a, to_b):
            slot = chip_of(da, db)
            dev = dev_of(to_a, to_b)
            self.flight[key] = []
            for ref, ss, rs in self.items:
                c = remote(ref(slot), ref(slot), ss.at[n], rs.at[n], dev)
                c.start()
                self.flight[key].append(c)
                started.append(c)

        def wait(self, key):
            for c in self.flight[key]:
                c.wait_recv()

        def open(self):
            self.start((1, 0), 0, 0, 0, 1, 0)
            self.start((3, 0), 1, 0, 0, -1, 0)
            self.spread(0)

        def spread(self, j):
            self.start((j, 1), 3 + 3 * j, -j, 0, 0, 1)
            self.start((j, 3), 3 + 3 * j + 1, -j, 0, 0, -1)

        def relay(self, j):
            if j % 2 == 0:
                self.start((j, 2), 3 + 3 * j + 2, -j, -1, 0, 1)
            else:
                self.start((j, 2), 3 + 3 * j + 2, -j, -3, 0, -1)

        def steps(self):
            self.wait((1, 0))
            self.start((2, 0), 2, -1, 0, 1, 0)
            self.spread(1)
            yield (1, 0)
            self.wait((3, 0))
            self.spread(3)
            yield (3, 0)
            self.wait((0, 1))
            self.relay(0)
            yield (0, 1)
            self.wait((0, 3))
            yield (0, 3)
            self.wait((2, 0))
            self.spread(2)
            yield (2, 0)
            self.wait((1, 3))
            self.relay(1)
            yield (1, 3)
            self.wait((3, 3))
            self.relay(3)
            yield (3, 3)
            for key in ((1, 1), (3, 1), (0, 2)):
                self.wait(key)
                yield key
            self.wait((2, 1))
            self.relay(2)
            yield (2, 1)
            for key in ((2, 3), (1, 2), (3, 2), (2, 2)):
                self.wait(key)
                yield key

    m_pair.wait_recv()
    meta_buf[chip] = meta_own[0] + meta_own[1]
    x_pair.wait_recv()
    xs = xbuf[...]
    loads['k'].wait()
    kvbuf[chip, :, 0:half_kv] = jnp.dot(xs, wk_v[...], preferred_element_type=F32).astype(BF16)
    loads['v'].wait()
    kvbuf[chip, :, half_kv:2 * half_kv] = jnp.dot(xs, wv_v[...], preferred_element_type=F32).astype(BF16)

    kv = Gather([(lambda s: kvbuf.at[s], kv_send, kv_recv), (lambda s: meta_buf.at[s], mt_send, mt_recv)])
    kv.open()

    for i in range(n_q):
        loads[('q', i)].wait()
        cols = slice(i * Q_COLS, (i + 1) * Q_COLS)
        q_s[:, cols] = jnp.dot(xs, wq_v[:, cols], preferred_element_type=F32).astype(BF16)

    for _ in kv.steps():
        pass

    seq = n_chips * tok2
    q_pos = chip * tok2 + lax.broadcasted_iota(jnp.int32, (per_kv * tok2, seq), 0) % tok2
    k_pos = lax.broadcasted_iota(jnp.int32, (per_kv * tok2, seq), 1)
    causal = k_pos <= q_pos
    o_pairs = []
    for g in range(kv_half_heads):
        kc = slice(g * HEAD_DIM, (g + 1) * HEAD_DIM)
        vc = slice(half_kv + g * HEAD_DIM, half_kv + (g + 1) * HEAD_DIM)
        k_all = kvbuf[:, :, kc].reshape(seq, HEAD_DIM)
        v_all = kvbuf[:, :, vc].reshape(seq, HEAD_DIM)
        q_g = jnp.concatenate([q_s[:, (g * per_kv + h) * HEAD_DIM:(g * per_kv + h + 1) * HEAD_DIM]
                               for h in range(per_kv)], axis=0)
        s = lax.dot_general(q_g, k_all, (((1,), (1,)), ((), ())), preferred_element_type=F32) * SCORE_SCALE
        s = jnp.where(causal, s, -1e30)
        e = jnp.exp(s - jnp.max(s, axis=1, keepdims=True))
        w = (e / jnp.sum(e, axis=1, keepdims=True)).astype(BF16)
        o_g = jnp.dot(w, v_all, preferred_element_type=F32).astype(BF16)
        gw = per_kv * HEAD_DIM
        for h in range(per_kv):
            o_own[:, g * gw + h * HEAD_DIM:g * gw + (h + 1) * HEAD_DIM] = o_g[h * tok2:(h + 1) * tok2, :]
        cols = pl.ds(g * gw, gw)
        c = remote(o_own.at[:, cols], o_sib.at[:, cols], pair_send.at[2 + g], pair_recv.at[2 + g], sib)
        c.start()
        o_pairs.append(c)

    loads['o0'].wait()
    acc = jnp.dot(o_own[...], wo_v[0:half_q, :], preferred_element_type=F32)
    loads['o1'].wait()
    for c in o_pairs:
        c.wait_recv()
    acc = acc + jnp.dot(o_sib[...], wo_v[half_q:2 * half_q, :], preferred_element_type=F32)
    my_cols = pl.ds(pl.multiple_of(core * half_w, half_w), half_w)
    h_buf[core, chip] = (xbuf[:, my_cols].astype(F32) + acc).astype(BF16)

    hg = Gather([(lambda s: h_buf.at[core, s], h_send, h_recv)])
    across = {}

    def cross(n, da, db):
        slot = chip_of(da, db)
        c = remote(h_buf.at[core, slot], h_buf.at[core, slot], d_send.at[n], d_recv.at[n], sib)
        c.start()
        across[n] = c
        started.append(c)

    cross(0, 0, 0)
    hg.open()

    lane_1 = lax.broadcasted_iota(jnp.int32, (1, LANES), 1)
    t_row = lax.broadcasted_iota(jnp.int32, (LANES, LANES), 0)
    t_col = lax.broadcasted_iota(jnp.int32, (LANES, LANES), 1)
    before = jnp.where((t_row < t_col) & (t_row // tok == t_col // tok), 1.0, 0.0).astype(BF16)
    source_base = ((lane_1 // tok) * tok).astype(F32)
    live = lane_1 < tok2
    slot_row = lax.broadcasted_iota(jnp.int32, (tok2, LANES), 0).astype(F32)

    def select_rows(s, carry):
        m = meta_buf[s]
        e_first, e_second = m[0:1, :], m[1:2, :]
        sels, gates = [], []
        for k in range(own_experts):
            expert = (me * own_experts + k).astype(F32)
            hit0 = (e_first == expert) & live
            hit1 = (e_second == expert) & live
            hit = jnp.where(hit0 | hit1, 1.0, 0.0)
            slot = jnp.dot(jnp.broadcast_to(hit, (8, LANES)).astype(BF16), before, preferred_element_type=F32)[0:1, :]
            row = jnp.where(hit0 | hit1, slot + source_base, -1.0)
            gate = jnp.where(hit0, m[2:3, :], jnp.where(hit1, m[3:4, :], 0.0))
            pick = slot_row == row
            sels.append(jnp.where(pick, 1.0, 0.0))
            gates.append(jnp.broadcast_to(jnp.sum(jnp.where(pick, gate, 0.0), axis=1, keepdims=True), (tok2, LANES)))
        sel_s[s] = jnp.concatenate(sels, axis=0).astype(BF16)
        gate_s[s] = jnp.concatenate(gates, axis=0)
        return carry

    lax.fori_loop(0, n_chips, select_rows, 0)

    def build(slot, col_half):
        sel = sel_s[slot][:, 0:tok2]
        rows = jnp.dot(sel, h_buf[col_half, slot], preferred_element_type=F32)
        gate = gate_s[slot]
        rows = jnp.concatenate([rows[:, i * LANES:(i + 1) * LANES] * gate for i in range(half_w // LANES)], axis=1)
        rows = rows.astype(BF16)
        at = pl.ds(pl.multiple_of(slot * tok2, tok2), tok2)
        cols = pl.ds(pl.multiple_of(col_half * half_w, half_w), half_w)
        for k in range(own_experts):
            buf_out[k, at, cols] = rows[k * tok2:(k + 1) * tok2, :]

    build(chip, core)
    arrived = [(0, 0)]
    for n, key in enumerate(hg.steps()):
        j, d = key
        cross(n + 1, -j, -d)
        build(chip_of(-j, -d), core)
        arrived.append(key)
    for n, (j, d) in enumerate(arrived):
        across[n].wait_recv()
        build(chip_of(-d, -j), 1 - core)
    h_out[:, 0:half_w] = h_buf[0, chip, my_rows, :]
    h_out[:, half_w:2 * half_w] = h_buf[1, chip, my_rows, :]

    for c in [x_pair, m_pair] + o_pairs + started:
        c.wait_send()


def store_kernel(buf_ref, h_ref, buf_out, h_out, sem):
    n = buf_ref.shape[0]
    copies = [pltpu.make_async_copy(buf_ref.at[k], buf_out.at[k], sem.at[k]) for k in range(n)]
    copies.append(pltpu.make_async_copy(h_ref, h_out, sem.at[n]))
    for c in copies:
        c.start()
    for c in copies:
        c.wait()


def solution(mesh):
    group = mesh.shape['sp']
    side = math.isqrt(group // CORES)
    row_spec = P(('dp', 'sp'), None)
    buf_spec = P(('dp', 'sp'), None, None)
    any_spec = pl.BlockSpec(memory_space=pl.ANY)
    vmem_spec = pl.BlockSpec(memory_space=pltpu.VMEM)

    def device_step(x_loc, w_q, w_k, w_v, w_o, ids_loc, probs_loc):
        tok, width = x_loc.shape
        experts = probs_loc.shape[1]
        own = experts // group
        chips = side * side
        tok2 = CORES * tok
        half_q = w_q.shape[1] // CORES
        half_kv = w_k.shape[1] // CORES
        half_w = width // CORES
        dma = pltpu.SemaphoreType.DMA
        n_loads = 4 + half_q // Q_COLS
        kv_half_heads = half_kv // HEAD_DIM
        buf, h = pl.pallas_call(
            functools.partial(block_kernel, side),
            out_shape=(pltpu.VMEM((own, tok * group, width), BF16), pltpu.VMEM((tok, width), BF16)),
            in_specs=[any_spec] * 5 + [vmem_spec] * 2,
            out_specs=(vmem_spec, vmem_spec),
            scratch_shapes=[
                pltpu.VMEM((tok2, width), BF16),
                pltpu.VMEM((width, half_q), BF16),
                pltpu.VMEM((width, half_kv), BF16),
                pltpu.VMEM((width, half_kv), BF16),
                pltpu.VMEM((2 * half_q, half_w), BF16),
                pltpu.VMEM((chips, tok2, 2 * half_kv), BF16),
                pltpu.VMEM((CORES, 8, LANES), F32),
                pltpu.VMEM((chips, 8, LANES), F32),
                pltpu.VMEM((tok2, half_q), BF16),
                pltpu.VMEM((tok2, half_q), BF16),
                pltpu.VMEM((tok2, half_q), BF16),
                pltpu.VMEM((CORES, chips, tok2, half_w), BF16),
                pltpu.VMEM((chips, own * tok2, LANES), BF16),
                pltpu.VMEM((chips, own * tok2, LANES), F32),
                dma((n_loads,)), dma,
                dma((2 + kv_half_heads,)), dma((2 + kv_half_heads,)),
                dma((chips,)), dma((chips,)), dma((chips,)), dma((chips,)),
                dma((chips,)), dma((chips,)), dma((chips,)), dma((chips,)),
            ],
            compiler_params=pltpu.CompilerParams(collective_id=0, has_side_effects=True,
                                                 vmem_limit_bytes=44 * 2 ** 20),
            name='attention_block',
        )(x_loc, w_q, w_k, w_v, w_o, ids_loc, probs_loc)
        buf, h = pl.pallas_call(
            store_kernel,
            out_shape=(jax.ShapeDtypeStruct((own, tok * group, width), BF16), jax.ShapeDtypeStruct((tok, width), BF16)),
            in_specs=[vmem_spec, vmem_spec],
            out_specs=(any_spec, any_spec),
            scratch_shapes=[dma((own + 1,))],
            compiler_params=pltpu.CompilerParams(vmem_limit_bytes=16 * 2 ** 20),
            name='store_outputs',
        )(buf, h)
        return h, buf

    return jax.shard_map(device_step, mesh=mesh, in_specs=(row_spec, P(), P(), P(), P(), row_spec, row_spec), out_specs=(row_spec, buf_spec), check_vma=False)
```

```python
import functools
import math

import jax
import jax.numpy as jnp
from jax import lax
from jax.experimental import pallas as pl
from jax.experimental.pallas import tpu as pltpu
from jax.sharding import PartitionSpec as P

HEAD_DIM = 128
SCORE_SCALE = 1.0 / math.sqrt(HEAD_DIM)
MESH_IDS = pl.DeviceIdType.MESH
LANES = 128
CORES = 2
Q_COLS = 512
F32 = jnp.float32
BF16 = jnp.bfloat16


def block_kernel(side, x_hbm, wq_hbm, wk_hbm, wv_hbm, wo_hbm, ids_hbm, probs_hbm,
                 buf_out, h_out,
                 xbuf, wq_v, wk_v, wv_v, wo_v, ids_v, probs_v, kv_own, kvbuf, meta_own, meta_buf, q_s, o_own, o_sib,
                 h_buf, sel_s, gate_s,
                 wsem, pair_send, pair_recv, kv_send, kv_recv, mt_send, mt_recv, h_send, h_recv,
                 d_send, d_recv):
    tok = x_hbm.shape[0]
    tok2 = CORES * tok
    half_q = wq_v.shape[1]
    half_kv = wk_v.shape[1] // CORES
    half_w = wo_v.shape[1]
    kv_half_heads = half_kv // HEAD_DIM
    q_half_heads = half_q // HEAD_DIM
    per_kv = q_half_heads // kv_half_heads
    own_experts = buf_out.shape[0]
    experts = probs_v.shape[1]
    n_chips = side * side
    n_dev = n_chips * CORES

    me = lax.axis_index('sp')
    core = me % CORES
    chip = me // CORES
    cy = chip // side
    cx = chip % side
    a0 = cx + (cy - cx) * core
    b0 = cy + (cx - cy) * core

    def chip_at(a, b):
        y = b + (a - b) * core
        x = a + (b - a) * core
        return y * side + x

    def peer(c):
        return {'sp': c * CORES + core}

    sib = {'sp': chip * CORES + (1 - core)}

    def remote(src, dst, ss, rs, dev):
        return pltpu.make_async_remote_copy(src_ref=src, dst_ref=dst, send_sem=ss, recv_sem=rs,
                                            device_id=dev, device_id_type=MESH_IDS)

    my_rows = pl.ds(pl.multiple_of(core * tok, tok), tok)
    loads = {}

    def load(name, src, dst):
        loads[name] = pltpu.make_async_copy(src, dst, wsem.at[len(loads)])
        loads[name].start()

    load('x', x_hbm, xbuf.at[my_rows, :])
    load('ids', ids_hbm, ids_v)
    load('probs', probs_hbm, probs_v)
    load('k', wk_hbm, wk_v)
    load('v', wv_hbm, wv_v)
    n_q = half_q // Q_COLS
    for i in range(n_q):
        load(('q', i), wq_hbm.at[:, pl.ds(pl.multiple_of(core * half_q + i * Q_COLS, Q_COLS), Q_COLS)],
             wq_v.at[:, pl.ds(i * Q_COLS, Q_COLS)])
    o_cols = pl.ds(pl.multiple_of(core * half_w, half_w), half_w)
    load('o0', wo_hbm.at[pl.ds(pl.multiple_of(core * half_q, half_q), half_q), o_cols], wo_v.at[pl.ds(0, half_q), :])
    load('o1', wo_hbm.at[pl.ds(pl.multiple_of((1 - core) * half_q, half_q), half_q), o_cols],
         wo_v.at[pl.ds(half_q, half_q), :])

    kvbuf[...] = jnp.zeros_like(kvbuf)

    barrier = pltpu.get_barrier_semaphore()
    for i in range(1, n_dev):
        pl.semaphore_signal(barrier, inc=1, device_id={'sp': (me + i) % n_dev}, device_id_type=MESH_IDS)

    loads['x'].wait()
    loads['ids'].wait()
    loads['probs'].wait()
    idf = ids_v[...].astype(F32)
    probs = probs_v[...]
    lane_e = lax.broadcasted_iota(jnp.int32, (tok, experts), 1).astype(F32)
    eye_t = lax.broadcasted_iota(jnp.int32, (tok, tok), 0) == lax.broadcasted_iota(jnp.int32, (tok, tok), 1)
    id0 = jnp.sum(jnp.where(eye_t, idf[0:1, :], 0.0), axis=1, keepdims=True)
    id1 = jnp.sum(jnp.where(eye_t, idf[1:2, :], 0.0), axis=1, keepdims=True)
    p0 = jnp.sum(jnp.where(lane_e == id0, probs, 0.0), axis=1, keepdims=True)
    p1 = jnp.sum(jnp.where(lane_e == id1, probs, 0.0), axis=1, keepdims=True)
    psum = p0 + p1
    lane_t = lax.broadcasted_iota(jnp.int32, (tok, LANES), 1)
    row_t = lax.broadcasted_iota(jnp.int32, (tok, LANES), 0)
    eye = lane_t == row_t + core * tok

    def to_lanes(col):
        return jnp.sum(jnp.where(eye, col, 0.0), axis=0, keepdims=True)

    meta_rows = [to_lanes(id0), to_lanes(id1), to_lanes(p0 / psum), to_lanes(p1 / psum)]
    meta_own[0] = jnp.concatenate(meta_rows + [jnp.zeros((4, LANES), F32)], axis=0)

    x_own = xbuf[my_rows, :]
    for name, w_ref, at in (('k', wk_v, 0), ('v', wv_v, half_kv)):
        loads[name].wait()
        out = jnp.dot(x_own, w_ref[...], preferred_element_type=F32).astype(BF16)
        for c in range(CORES):
            kv_own[c, :, at:at + half_kv] = out[:, c * half_kv:(c + 1) * half_kv]
    kvbuf[chip, my_rows, :] = kv_own[core]

    pl.semaphore_wait(barrier, n_dev - 1)
    x_pair = remote(xbuf.at[my_rows, :], xbuf.at[my_rows, :], pair_send.at[0], pair_recv.at[0], sib)
    x_pair.start()
    m_pair = remote(meta_own.at[0], meta_own.at[1], pair_send.at[1], pair_recv.at[1], sib)
    m_pair.start()
    kv_pair = remote(kv_own.at[1 - core], kvbuf.at[chip, my_rows, :], pair_send.at[2], pair_recv.at[2], sib)
    kv_pair.start()

    def kv_copy(k, c, slot, rows, src_core):
        return remote(kv_own.at[c], kvbuf.at[slot, rows, :], kv_send.at[CORES * k + c],
                      kv_recv.at[CORES * k + src_core], {'sp': (chip + k) % n_chips * CORES + c})

    for k in range(1, n_chips):
        @pl.when(chip + k < n_chips)
        def _():
            for c in range(CORES):
                kv_copy(k, c, chip, my_rows, core).start()

    class Gather:
        def __init__(self, ref, ss, rs):
            self.ref, self.ss, self.rs = ref, ss, rs

        def first(self, d, slot):
            return remote(self.ref(slot), self.ref(slot), self.ss.at[d], self.rs.at[a0],
                          peer(chip_at((a0 + d) % side, b0)))

        def first_from(self, i, slot):
            return remote(self.ref(slot), self.ref(slot), self.ss.at[0], self.rs.at[i], sib)

        def second(self, i, d, slot):
            return remote(self.ref(slot), self.ref(slot), self.ss.at[side + i * side + d],
                          self.rs.at[side + i * side + b0], peer(chip_at(a0, (b0 + d) % side)))

        def second_from(self, i, j, slot):
            return remote(self.ref(slot), self.ref(slot), self.ss.at[0], self.rs.at[side + i * side + j], sib)

        def open(self):
            for d in (1, side - 1, 2):
                self.first(d, chip).start()
            self.spread(a0)

        def spread(self, i):
            for d in (1, side - 1, 2):
                self.second(i, d, chip_at(i, b0)).start()

        def sent(self):
            for d in range(1, side):
                self.first(d, chip).wait_send()
                for i in range(side):
                    self.second(i, d, chip_at(i, b0)).wait_send()

    x_pair.wait_recv()
    xs = xbuf[...]
    for i in range(n_q):
        loads[('q', i)].wait()
        cols = slice(i * Q_COLS, (i + 1) * Q_COLS)
        q_s[:, cols] = jnp.dot(xs, wq_v[:, cols], preferred_element_type=F32).astype(BF16)

    m_pair.wait_recv()
    meta_buf[chip] = meta_own[0] + meta_own[1]
    mt = Gather(lambda s: meta_buf.at[s], mt_send, mt_recv)
    mt.open()

    kv_pair.wait_recv()
    for k in range(1, n_chips):
        @pl.when(chip >= k)
        def _():
            for c in range(CORES):
                kv_copy(k, c, chip - k, pl.ds(c * tok, tok), c).wait_recv()

    seq = n_chips * tok2
    q_pos = chip * tok2 + lax.broadcasted_iota(jnp.int32, (per_kv * tok2, seq), 0) % tok2
    k_pos = lax.broadcasted_iota(jnp.int32, (per_kv * tok2, seq), 1)
    causal = k_pos <= q_pos
    o_pairs = []
    for g in range(kv_half_heads):
        kc = slice(g * HEAD_DIM, (g + 1) * HEAD_DIM)
        vc = slice(half_kv + g * HEAD_DIM, half_kv + (g + 1) * HEAD_DIM)
        k_all = kvbuf[:, :, kc].reshape(seq, HEAD_DIM)
        v_all = kvbuf[:, :, vc].reshape(seq, HEAD_DIM)
        q_g = jnp.concatenate([q_s[:, (g * per_kv + h) * HEAD_DIM:(g * per_kv + h + 1) * HEAD_DIM]
                               for h in range(per_kv)], axis=0)
        s = lax.dot_general(q_g, k_all, (((1,), (1,)), ((), ())), preferred_element_type=F32) * SCORE_SCALE
        s = jnp.where(causal, s, -1e30)
        e = jnp.exp(s - jnp.max(s, axis=1, keepdims=True))
        w = (e / jnp.sum(e, axis=1, keepdims=True)).astype(BF16)
        o_g = jnp.dot(w, v_all, preferred_element_type=F32).astype(BF16)
        gw = per_kv * HEAD_DIM
        for h in range(per_kv):
            o_own[:, g * gw + h * HEAD_DIM:g * gw + (h + 1) * HEAD_DIM] = o_g[h * tok2:(h + 1) * tok2, :]
        cols = pl.ds(g * gw, gw)
        c = remote(o_own.at[:, cols], o_sib.at[:, cols], pair_send.at[3 + g], pair_recv.at[3 + g], sib)
        c.start()
        o_pairs.append(c)

    def pass_meta(i, carry):
        @pl.when(i != a0)
        def _():
            mt.first_from(i, chip_at(i, b0)).wait_recv()
            mt.spread(i)
        return carry

    lax.fori_loop(0, side, pass_meta, 0)

    loads['o0'].wait()
    acc = jnp.dot(o_own[...], wo_v[0:half_q, :], preferred_element_type=F32)
    loads['o1'].wait()
    for c in o_pairs:
        c.wait_recv()
    acc = acc + jnp.dot(o_sib[...], wo_v[half_q:2 * half_q, :], preferred_element_type=F32)
    my_cols = pl.ds(pl.multiple_of(core * half_w, half_w), half_w)
    h_buf[core, chip] = (xbuf[:, my_cols].astype(F32) + acc).astype(BF16)

    hg = Gather(lambda s: h_buf.at[core, s], h_send, h_recv)

    def cross(slot):
        return remote(h_buf.at[core, slot], h_buf.at[core, slot], d_send.at[slot], d_recv.at[slot], sib)

    def cross_from(slot):
        return remote(h_buf.at[1 - core, slot], h_buf.at[1 - core, slot], d_send.at[slot], d_recv.at[slot], sib)

    hg.open()
    cross(chip).start()

    def meta_done(n, carry):
        i, j = n // side, n % side

        @pl.when(j != b0)
        def _():
            mt.second_from(i, j, chip_at(i, j)).wait_recv()
        return carry

    lax.fori_loop(0, n_chips, meta_done, 0)

    lane_1 = lax.broadcasted_iota(jnp.int32, (1, LANES), 1)
    t_row = lax.broadcasted_iota(jnp.int32, (LANES, LANES), 0)
    t_col = lax.broadcasted_iota(jnp.int32, (LANES, LANES), 1)
    before = jnp.where((t_row < t_col) & (t_row // tok == t_col // tok), 1.0, 0.0).astype(BF16)
    source_base = ((lane_1 // tok) * tok).astype(F32)
    live = lane_1 < tok2
    slot_row = lax.broadcasted_iota(jnp.int32, (tok2, LANES), 0).astype(F32)

    def select_rows(s, carry):
        m = meta_buf[s]
        e_first, e_second = m[0:1, :], m[1:2, :]
        sels, gates = [], []
        for k in range(own_experts):
            expert = (me * own_experts + k).astype(F32)
            hit0 = (e_first == expert) & live
            hit1 = (e_second == expert) & live
            hit = jnp.where(hit0 | hit1, 1.0, 0.0)
            slot = jnp.dot(jnp.broadcast_to(hit, (8, LANES)).astype(BF16), before, preferred_element_type=F32)[0:1, :]
            row = jnp.where(hit0 | hit1, slot + source_base, -1.0)
            gate = jnp.where(hit0, m[2:3, :], jnp.where(hit1, m[3:4, :], 0.0))
            pick = slot_row == row
            sels.append(jnp.where(pick, 1.0, 0.0))
            gates.append(jnp.broadcast_to(jnp.sum(jnp.where(pick, gate, 0.0), axis=1, keepdims=True), (tok2, LANES)))
        sel_s[s] = jnp.concatenate(sels, axis=0).astype(BF16)
        gate_s[s] = jnp.concatenate(gates, axis=0)
        return carry

    lax.fori_loop(0, n_chips, select_rows, 0)

    def build(slot, col_half):
        sel = sel_s[slot][:, 0:tok2]
        rows = jnp.dot(sel, h_buf[col_half, slot], preferred_element_type=F32)
        gate = gate_s[slot]
        rows = jnp.concatenate([rows[:, i * LANES:(i + 1) * LANES] * gate for i in range(half_w // LANES)], axis=1)
        rows = rows.astype(BF16)
        at = pl.ds(pl.multiple_of(slot * tok2, tok2), tok2)
        cols = pl.ds(pl.multiple_of(col_half * half_w, half_w), half_w)
        for k in range(own_experts):
            buf_out[k, at, cols] = rows[k * tok2:(k + 1) * tok2, :]

    build(chip, core)

    def pass_first(i, carry):
        @pl.when(i != a0)
        def _():
            slot = chip_at(i, b0)
            hg.first_from(i, slot).wait_recv()
            hg.spread(i)
            cross(slot).start()
            build(slot, core)
        return carry

    lax.fori_loop(0, side, pass_first, 0)

    lag = side

    def pass_second(slot, carry):
        y, x = slot // side, slot % side
        i = x + (y - x) * core
        j = y + (x - y) * core

        @pl.when((slot < n_chips) & (j != b0))
        def _():
            hg.second_from(i, j, slot).wait_recv()
            cross(slot).start()
            build(slot, core)

        @pl.when(slot >= lag)
        def _():
            cross_from(slot - lag).wait_recv()
            build(slot - lag, 1 - core)
        return carry

    lax.fori_loop(0, n_chips + lag, pass_second, 0)
    h_out[:, 0:half_w] = h_buf[0, chip, my_rows, :]
    h_out[:, half_w:2 * half_w] = h_buf[1, chip, my_rows, :]

    for c in [x_pair, m_pair, kv_pair] + o_pairs:
        c.wait_send()
    for k in range(1, n_chips):
        @pl.when(chip + k < n_chips)
        def _():
            for c in range(CORES):
                kv_copy(k, c, chip, my_rows, core).wait_send()
    mt.sent()
    hg.sent()
    for slot in range(n_chips):
        cross(slot).wait_send()


def store_kernel(buf_ref, h_ref, buf_out, h_out, sem):
    n = buf_ref.shape[0]
    copies = [pltpu.make_async_copy(buf_ref.at[k], buf_out.at[k], sem.at[k]) for k in range(n)]
    copies.append(pltpu.make_async_copy(h_ref, h_out, sem.at[n]))
    for c in copies:
        c.start()
    for c in copies:
        c.wait()


def solution(mesh):
    group = mesh.shape['sp']
    side = math.isqrt(group // CORES)
    row_spec = P(('dp', 'sp'), None)
    buf_spec = P(('dp', 'sp'), None, None)
    any_spec = pl.BlockSpec(memory_space=pl.ANY)
    hbm_spec = pl.BlockSpec(memory_space=pltpu.HBM)
    vmem_spec = pl.BlockSpec(memory_space=pltpu.VMEM)

    def device_step(x_loc, w_q, w_k, w_v, w_o, ids_loc, probs_loc):
        tok, width = x_loc.shape
        experts = probs_loc.shape[1]
        own = experts // group
        chips = side * side
        tok2 = CORES * tok
        half_q = w_q.shape[1] // CORES
        half_kv = w_k.shape[1] // CORES
        half_w = width // CORES
        dma = pltpu.SemaphoreType.DMA
        n_loads = 7 + half_q // Q_COLS
        kv_half_heads = half_kv // HEAD_DIM
        buf, h = pl.pallas_call(
            functools.partial(block_kernel, side),
            out_shape=(pltpu.VMEM((own, tok * group, width), BF16), pltpu.VMEM((tok, width), BF16)),
            in_specs=[hbm_spec] * 7,
            out_specs=(vmem_spec, vmem_spec),
            scratch_shapes=[
                pltpu.VMEM((tok2, width), BF16),
                pltpu.VMEM((width, half_q), BF16),
                pltpu.VMEM((width, CORES * half_kv), BF16),
                pltpu.VMEM((width, CORES * half_kv), BF16),
                pltpu.VMEM((2 * half_q, half_w), BF16),
                pltpu.VMEM((2, tok), jnp.int32),
                pltpu.VMEM((tok, experts), F32),
                pltpu.VMEM((CORES, tok, 2 * half_kv), BF16),
                pltpu.VMEM((chips, tok2, 2 * half_kv), BF16),
                pltpu.VMEM((CORES, 8, LANES), F32),
                pltpu.VMEM((chips, 8, LANES), F32),
                pltpu.VMEM((tok2, half_q), BF16),
                pltpu.VMEM((tok2, half_q), BF16),
                pltpu.VMEM((tok2, half_q), BF16),
                pltpu.VMEM((CORES, chips, tok2, half_w), BF16),
                pltpu.VMEM((chips, own * tok2, LANES), BF16),
                pltpu.VMEM((chips, own * tok2, LANES), F32),
                dma((n_loads,)),
                dma((3 + kv_half_heads,)), dma((3 + kv_half_heads,)),
                dma((group,)), dma((group,)),
                dma((side + chips,)), dma((side + chips,)), dma((side + chips,)), dma((side + chips,)),
                dma((chips,)), dma((chips,)),
            ],
            compiler_params=pltpu.CompilerParams(collective_id=0, has_side_effects=True,
                                                 vmem_limit_bytes=55 * 2 ** 20 + 850 * 1024),
            name='attention_block',
        )(x_loc, w_q, w_k, w_v, w_o, ids_loc.T, probs_loc)
        buf, h = pl.pallas_call(
            store_kernel,
            out_shape=(jax.ShapeDtypeStruct((own, tok * group, width), BF16), jax.ShapeDtypeStruct((tok, width), BF16)),
            in_specs=[vmem_spec, vmem_spec],
            out_specs=(any_spec, any_spec),
            scratch_shapes=[dma((own + 1,))],
            compiler_params=pltpu.CompilerParams(vmem_limit_bytes=16 * 2 ** 20),
            name='store_outputs',
        )(buf, h)
        return h, buf

    return jax.shard_map(device_step, mesh=mesh, in_specs=(row_spec, P(), P(), P(), P(), row_spec, row_spec), out_specs=(row_spec, buf_spec), check_vma=False)
```

```python
import functools
import math

import jax
import jax.numpy as jnp
from jax import lax
from jax.experimental import pallas as pl
from jax.experimental.pallas import tpu as pltpu
from jax.sharding import PartitionSpec as P

HEAD_DIM = 128
SCORE_SCALE = 1.0 / math.sqrt(HEAD_DIM)
MESH_IDS = pl.DeviceIdType.MESH
LANES = 128
CORES = 2
Q_COLS = 512
F32 = jnp.float32
BF16 = jnp.bfloat16


def block_kernel(side, x_hbm, wq_hbm, wk_hbm, wv_hbm, wo_hbm, ids_hbm, probs_hbm,
                 buf_out, h_out,
                 xbuf, wq_v, wk_v, wv_v, wo_v, ids_v, probs_v, kv_own, kvbuf, meta_own, meta_buf, q_s, o_own, o_sib,
                 h_buf, sel_s, gate_s,
                 wsem, pair_send, pair_recv, kv_send, kv_recv, kv2_send, kv2_recv, mt_send, mt_recv, h_send, h_recv,
                 d_send, d_recv):
    tok = x_hbm.shape[0]
    tok2 = CORES * tok
    half_q = wq_v.shape[1]
    half_kv = wk_v.shape[1] // CORES
    half_w = wo_v.shape[1]
    kv_half_heads = half_kv // HEAD_DIM
    q_half_heads = half_q // HEAD_DIM
    per_kv = q_half_heads // kv_half_heads
    own_experts = buf_out.shape[0]
    experts = probs_v.shape[1]
    n_chips = side * side

    me = lax.axis_index('sp')
    core = me % CORES
    chip = me // CORES
    cy = chip // side
    cx = chip % side
    a0 = cx + (cy - cx) * core
    b0 = cy + (cx - cy) * core

    def chip_at(a, b):
        y = b + (a - b) * core
        x = a + (b - a) * core
        return y * side + x

    def peer(c):
        return {'sp': c * CORES + core}

    sib = {'sp': chip * CORES + (1 - core)}

    def remote(src, dst, ss, rs, dev):
        return pltpu.make_async_remote_copy(src_ref=src, dst_ref=dst, send_sem=ss, recv_sem=rs,
                                            device_id=dev, device_id_type=MESH_IDS)

    my_rows = pl.ds(pl.multiple_of(core * tok, tok), tok)
    loads = {}

    def load(name, src, dst):
        loads[name] = pltpu.make_async_copy(src, dst, wsem.at[len(loads)])
        loads[name].start()

    load('x', x_hbm, xbuf.at[my_rows, :])
    load('ids', ids_hbm, ids_v)
    load('probs', probs_hbm, probs_v)
    load('k', wk_hbm, wk_v)
    load('v', wv_hbm, wv_v)
    n_q = half_q // Q_COLS
    for i in range(n_q):
        load(('q', i), wq_hbm.at[:, pl.ds(pl.multiple_of(core * half_q + i * Q_COLS, Q_COLS), Q_COLS)],
             wq_v.at[:, pl.ds(i * Q_COLS, Q_COLS)])
    o_cols = pl.ds(pl.multiple_of(core * half_w, half_w), half_w)
    load('o0', wo_hbm.at[pl.ds(pl.multiple_of(core * half_q, half_q), half_q), o_cols], wo_v.at[pl.ds(0, half_q), :])
    load('o1', wo_hbm.at[pl.ds(pl.multiple_of((1 - core) * half_q, half_q), half_q), o_cols],
         wo_v.at[pl.ds(half_q, half_q), :])

    kvbuf[...] = jnp.zeros_like(kvbuf)

    barrier = pltpu.get_barrier_semaphore()
    partners = [sib]
    for d in range(1, side):
        for c in range(CORES):
            partners.append({'sp': (cy * side + (cx + d) % side) * CORES + c})
            partners.append({'sp': ((cy + d) % side * side + cx) * CORES + c})
    for p in partners:
        pl.semaphore_signal(barrier, inc=1, device_id=p, device_id_type=MESH_IDS)

    loads['x'].wait()
    loads['ids'].wait()
    loads['probs'].wait()
    idf = ids_v[...].astype(F32)
    probs = probs_v[...]
    lane_e = lax.broadcasted_iota(jnp.int32, (tok, experts), 1).astype(F32)
    eye_t = lax.broadcasted_iota(jnp.int32, (tok, tok), 0) == lax.broadcasted_iota(jnp.int32, (tok, tok), 1)
    id0 = jnp.sum(jnp.where(eye_t, idf[0:1, :], 0.0), axis=1, keepdims=True)
    id1 = jnp.sum(jnp.where(eye_t, idf[1:2, :], 0.0), axis=1, keepdims=True)
    p0 = jnp.sum(jnp.where(lane_e == id0, probs, 0.0), axis=1, keepdims=True)
    p1 = jnp.sum(jnp.where(lane_e == id1, probs, 0.0), axis=1, keepdims=True)
    psum = p0 + p1
    lane_t = lax.broadcasted_iota(jnp.int32, (tok, LANES), 1)
    row_t = lax.broadcasted_iota(jnp.int32, (tok, LANES), 0)
    eye = lane_t == row_t + core * tok

    def to_lanes(col):
        return jnp.sum(jnp.where(eye, col, 0.0), axis=0, keepdims=True)

    meta_rows = [to_lanes(id0), to_lanes(id1), to_lanes(p0 / psum), to_lanes(p1 / psum)]
    meta_own[0] = jnp.concatenate(meta_rows + [jnp.zeros((4, LANES), F32)], axis=0)

    x_own = xbuf[my_rows, :]
    for name, w_ref, at in (('k', wk_v, 0), ('v', wv_v, half_kv)):
        loads[name].wait()
        out = jnp.dot(x_own, w_ref[...], preferred_element_type=F32).astype(BF16)
        for c in range(CORES):
            kv_own[c, :, at:at + half_kv] = out[:, c * half_kv:(c + 1) * half_kv]
    kvbuf[chip, my_rows, :] = kv_own[core]

    pl.semaphore_wait(barrier, len(partners))
    x_pair = remote(xbuf.at[my_rows, :], xbuf.at[my_rows, :], pair_send.at[0], pair_recv.at[0], sib)
    x_pair.start()
    m_pair = remote(meta_own.at[0], meta_own.at[1], pair_send.at[1], pair_recv.at[1], sib)
    m_pair.start()
    kv_pair = remote(kv_own.at[1 - core], kvbuf.at[chip, my_rows, :], pair_send.at[2], pair_recv.at[2], sib)
    kv_pair.start()

    def kv_first(d, c):
        y = (cy + d * c) % side
        x = (cx + d * (1 - c)) % side
        i = cx + (cy - cx) * c
        return remote(kv_own.at[c], kvbuf.at[chip, my_rows, :], kv_send.at[CORES * d + c],
                      kv_recv.at[CORES * i + core], {'sp': (y * side + x) * CORES + c})

    def kv_first_from(i, c):
        return remote(kv_own.at[c], kvbuf.at[chip_at(i, b0), pl.ds(c * tok, tok), :], kv_send.at[0],
                      kv_recv.at[CORES * i + c], sib)

    for d in (2, 1, side - 1):
        for c in range(CORES):
            kv_first(d, c).start()

    class Gather:
        def __init__(self, ref, ss, rs):
            self.ref, self.ss, self.rs = ref, ss, rs

        def first(self, d, slot):
            return remote(self.ref(slot), self.ref(slot), self.ss.at[d], self.rs.at[a0],
                          peer(chip_at((a0 + d) % side, b0)))

        def first_from(self, i, slot):
            return remote(self.ref(slot), self.ref(slot), self.ss.at[0], self.rs.at[i], sib)

        def second(self, i, d, slot):
            return remote(self.ref(slot), self.ref(slot), self.ss.at[side + i * side + d],
                          self.rs.at[side + i * side + b0], peer(chip_at(a0, (b0 + d) % side)))

        def second_from(self, i, j, slot):
            return remote(self.ref(slot), self.ref(slot), self.ss.at[0], self.rs.at[side + i * side + j], sib)

        def open(self):
            for d in (2, 1, side - 1):
                self.first(d, chip).start()
            self.spread(a0)

        def spread(self, i):
            for d in (2, 1, side - 1):
                self.second(i, d, chip_at(i, b0)).start()

        def sent(self):
            for d in range(1, side):
                self.first(d, chip).wait_send()
                for i in range(side):
                    self.second(i, d, chip_at(i, b0)).wait_send()

    kvg = Gather(lambda s: kvbuf.at[s], kv2_send, kv2_recv)

    def kv_second(i, wait):
        slot = chip_at(i, b0)
        for d in (2, 1, side - 1):
            @pl.when(chip_at(a0, (b0 + d) % side) > slot)
            def _():
                c = kvg.second(i, d, slot)
                if wait:
                    c.wait_send()
                else:
                    c.start()

    kv_pair.wait_recv()
    kv_second(a0, False)

    x_pair.wait_recv()
    xs = xbuf[...]
    for i in range(n_q):
        loads[('q', i)].wait()
        cols = slice(i * Q_COLS, (i + 1) * Q_COLS)
        q_s[:, cols] = jnp.dot(xs, wq_v[:, cols], preferred_element_type=F32).astype(BF16)

    m_pair.wait_recv()
    meta_buf[chip] = meta_own[0] + meta_own[1]
    mt = Gather(lambda s: meta_buf.at[s], mt_send, mt_recv)
    mt.open()

    def kv_pass(i, carry):
        @pl.when(i != a0)
        def _():
            for c in range(CORES):
                kv_first_from(i, c).wait_recv()
            kv_second(i, False)
        return carry

    lax.fori_loop(0, side, kv_pass, 0)

    def kv_done(n, carry):
        i, j = n // side, n % side

        @pl.when((j != b0) & (chip_at(i, j) < chip))
        def _():
            kvg.second_from(i, j, chip_at(i, j)).wait_recv()
        return carry

    lax.fori_loop(0, n_chips, kv_done, 0)

    seq = n_chips * tok2
    q_pos = chip * tok2 + lax.broadcasted_iota(jnp.int32, (per_kv * tok2, seq), 0) % tok2
    k_pos = lax.broadcasted_iota(jnp.int32, (per_kv * tok2, seq), 1)
    causal = k_pos <= q_pos
    o_pairs = []
    for g in range(kv_half_heads):
        kc = slice(g * HEAD_DIM, (g + 1) * HEAD_DIM)
        vc = slice(half_kv + g * HEAD_DIM, half_kv + (g + 1) * HEAD_DIM)
        k_all = kvbuf[:, :, kc].reshape(seq, HEAD_DIM)
        v_all = kvbuf[:, :, vc].reshape(seq, HEAD_DIM)
        q_g = jnp.concatenate([q_s[:, (g * per_kv + h) * HEAD_DIM:(g * per_kv + h + 1) * HEAD_DIM]
                               for h in range(per_kv)], axis=0)
        s = lax.dot_general(q_g, k_all, (((1,), (1,)), ((), ())), preferred_element_type=F32) * SCORE_SCALE
        s = jnp.where(causal, s, -1e30)
        e = jnp.exp(s - jnp.max(s, axis=1, keepdims=True))
        w = (e / jnp.sum(e, axis=1, keepdims=True)).astype(BF16)
        o_g = jnp.dot(w, v_all, preferred_element_type=F32).astype(BF16)
        gw = per_kv * HEAD_DIM
        for h in range(per_kv):
            o_own[:, g * gw + h * HEAD_DIM:g * gw + (h + 1) * HEAD_DIM] = o_g[h * tok2:(h + 1) * tok2, :]
        cols = pl.ds(g * gw, gw)
        c = remote(o_own.at[:, cols], o_sib.at[:, cols], pair_send.at[3 + g], pair_recv.at[3 + g], sib)
        c.start()
        o_pairs.append(c)

    def pass_meta(i, carry):
        @pl.when(i != a0)
        def _():
            mt.first_from(i, chip_at(i, b0)).wait_recv()
            mt.spread(i)
        return carry

    lax.fori_loop(0, side, pass_meta, 0)

    loads['o0'].wait()
    acc = jnp.dot(o_own[...], wo_v[0:half_q, :], preferred_element_type=F32)
    loads['o1'].wait()
    for c in o_pairs:
        c.wait_recv()
    acc = acc + jnp.dot(o_sib[...], wo_v[half_q:2 * half_q, :], preferred_element_type=F32)
    my_cols = pl.ds(pl.multiple_of(core * half_w, half_w), half_w)
    h_buf[core, chip] = (xbuf[:, my_cols].astype(F32) + acc).astype(BF16)

    hg = Gather(lambda s: h_buf.at[core, s], h_send, h_recv)

    def cross(slot):
        return remote(h_buf.at[core, slot], h_buf.at[core, slot], d_send.at[slot], d_recv.at[slot], sib)

    def cross_from(slot):
        return remote(h_buf.at[1 - core, slot], h_buf.at[1 - core, slot], d_send.at[slot], d_recv.at[slot], sib)

    hg.open()
    cross(chip).start()

    def meta_done(n, carry):
        i, j = n // side, n % side

        @pl.when(j != b0)
        def _():
            mt.second_from(i, j, chip_at(i, j)).wait_recv()
        return carry

    lax.fori_loop(0, n_chips, meta_done, 0)

    lane_1 = lax.broadcasted_iota(jnp.int32, (1, LANES), 1)
    t_row = lax.broadcasted_iota(jnp.int32, (LANES, LANES), 0)
    t_col = lax.broadcasted_iota(jnp.int32, (LANES, LANES), 1)
    before = jnp.where((t_row < t_col) & (t_row // tok == t_col // tok), 1.0, 0.0).astype(BF16)
    source_base = ((lane_1 // tok) * tok).astype(F32)
    live = lane_1 < tok2
    slot_row = lax.broadcasted_iota(jnp.int32, (tok2, LANES), 0).astype(F32)

    def select_rows(s, carry):
        m = meta_buf[s]
        e_first, e_second = m[0:1, :], m[1:2, :]
        sels, gates = [], []
        for k in range(own_experts):
            expert = (me * own_experts + k).astype(F32)
            hit0 = (e_first == expert) & live
            hit1 = (e_second == expert) & live
            hit = jnp.where(hit0 | hit1, 1.0, 0.0)
            slot = jnp.dot(jnp.broadcast_to(hit, (8, LANES)).astype(BF16), before, preferred_element_type=F32)[0:1, :]
            row = jnp.where(hit0 | hit1, slot + source_base, -1.0)
            gate = jnp.where(hit0, m[2:3, :], jnp.where(hit1, m[3:4, :], 0.0))
            pick = slot_row == row
            sels.append(jnp.where(pick, 1.0, 0.0))
            gates.append(jnp.broadcast_to(jnp.sum(jnp.where(pick, gate, 0.0), axis=1, keepdims=True), (tok2, LANES)))
        sel_s[s] = jnp.concatenate(sels, axis=0).astype(BF16)
        gate_s[s] = jnp.concatenate(gates, axis=0)
        return carry

    lax.fori_loop(0, n_chips, select_rows, 0)

    def build(slot, col_half):
        sel = sel_s[slot][:, 0:tok2]
        rows = jnp.dot(sel, h_buf[col_half, slot], preferred_element_type=F32)
        gate = gate_s[slot]
        rows = jnp.concatenate([rows[:, i * LANES:(i + 1) * LANES] * gate for i in range(half_w // LANES)], axis=1)
        rows = rows.astype(BF16)
        at = pl.ds(pl.multiple_of(slot * tok2, tok2), tok2)
        cols = pl.ds(pl.multiple_of(col_half * half_w, half_w), half_w)
        for k in range(own_experts):
            buf_out[k, at, cols] = rows[k * tok2:(k + 1) * tok2, :]

    build(chip, core)

    def pass_first(i, carry):
        @pl.when(i != a0)
        def _():
            slot = chip_at(i, b0)
            hg.first_from(i, slot).wait_recv()
            hg.spread(i)
            cross(slot).start()
            build(slot, core)
        return carry

    lax.fori_loop(0, side, pass_first, 0)

    lag = side

    def pass_second(slot, carry):
        y, x = slot // side, slot % side
        i = x + (y - x) * core
        j = y + (x - y) * core

        @pl.when((slot < n_chips) & (j != b0))
        def _():
            hg.second_from(i, j, slot).wait_recv()
            cross(slot).start()
            build(slot, core)

        @pl.when(slot >= lag)
        def _():
            cross_from(slot - lag).wait_recv()
            build(slot - lag, 1 - core)
        return carry

    lax.fori_loop(0, n_chips + lag, pass_second, 0)
    h_out[:, 0:half_w] = h_buf[0, chip, my_rows, :]
    h_out[:, half_w:2 * half_w] = h_buf[1, chip, my_rows, :]

    for c in [x_pair, m_pair, kv_pair] + o_pairs:
        c.wait_send()
    for d in range(1, side):
        for c in range(CORES):
            kv_first(d, c).wait_send()
    for i in range(side):
        kv_second(i, True)
    mt.sent()
    hg.sent()
    for slot in range(n_chips):
        cross(slot).wait_send()


def store_kernel(buf_ref, h_ref, buf_out, h_out, sem):
    n = buf_ref.shape[0]
    copies = [pltpu.make_async_copy(buf_ref.at[k], buf_out.at[k], sem.at[k]) for k in range(n)]
    copies.append(pltpu.make_async_copy(h_ref, h_out, sem.at[n]))
    for c in copies:
        c.start()
    for c in copies:
        c.wait()


def solution(mesh):
    group = mesh.shape['sp']
    side = math.isqrt(group // CORES)
    row_spec = P(('dp', 'sp'), None)
    buf_spec = P(('dp', 'sp'), None, None)
    any_spec = pl.BlockSpec(memory_space=pl.ANY)
    hbm_spec = pl.BlockSpec(memory_space=pltpu.HBM)
    vmem_spec = pl.BlockSpec(memory_space=pltpu.VMEM)

    def device_step(x_loc, w_q, w_k, w_v, w_o, ids_loc, probs_loc):
        tok, width = x_loc.shape
        experts = probs_loc.shape[1]
        own = experts // group
        chips = side * side
        tok2 = CORES * tok
        half_q = w_q.shape[1] // CORES
        half_kv = w_k.shape[1] // CORES
        half_w = width // CORES
        dma = pltpu.SemaphoreType.DMA
        n_loads = 7 + half_q // Q_COLS
        kv_half_heads = half_kv // HEAD_DIM
        buf, h = pl.pallas_call(
            functools.partial(block_kernel, side),
            out_shape=(pltpu.VMEM((own, tok * group, width), BF16), pltpu.VMEM((tok, width), BF16)),
            in_specs=[hbm_spec] * 7,
            out_specs=(vmem_spec, vmem_spec),
            scratch_shapes=[
                pltpu.VMEM((tok2, width), BF16),
                pltpu.VMEM((width, half_q), BF16),
                pltpu.VMEM((width, CORES * half_kv), BF16),
                pltpu.VMEM((width, CORES * half_kv), BF16),
                pltpu.VMEM((2 * half_q, half_w), BF16),
                pltpu.VMEM((2, tok), jnp.int32),
                pltpu.VMEM((tok, experts), F32),
                pltpu.VMEM((CORES, tok, 2 * half_kv), BF16),
                pltpu.VMEM((chips, tok2, 2 * half_kv), BF16),
                pltpu.VMEM((CORES, 8, LANES), F32),
                pltpu.VMEM((chips, 8, LANES), F32),
                pltpu.VMEM((tok2, half_q), BF16),
                pltpu.VMEM((tok2, half_q), BF16),
                pltpu.VMEM((tok2, half_q), BF16),
                pltpu.VMEM((CORES, chips, tok2, half_w), BF16),
                pltpu.VMEM((chips, own * tok2, LANES), BF16),
                pltpu.VMEM((chips, own * tok2, LANES), F32),
                dma((n_loads,)),
                dma((3 + kv_half_heads,)), dma((3 + kv_half_heads,)),
                dma((CORES * side,)), dma((CORES * side,)),
                dma((side + chips,)), dma((side + chips,)), dma((side + chips,)), dma((side + chips,)),
                dma((side + chips,)), dma((side + chips,)),
                dma((chips,)), dma((chips,)),
            ],
            compiler_params=pltpu.CompilerParams(collective_id=0, has_side_effects=True,
                                                 vmem_limit_bytes=55 * 2 ** 20 + 850 * 1024),
            name='attention_block',
        )(x_loc, w_q, w_k, w_v, w_o, ids_loc.T, probs_loc)
        buf, h = pl.pallas_call(
            store_kernel,
            out_shape=(jax.ShapeDtypeStruct((own, tok * group, width), BF16), jax.ShapeDtypeStruct((tok, width), BF16)),
            in_specs=[vmem_spec, vmem_spec],
            out_specs=(any_spec, any_spec),
            scratch_shapes=[dma((own + 1,))],
            compiler_params=pltpu.CompilerParams(vmem_limit_bytes=16 * 2 ** 20),
            name='store_outputs',
        )(buf, h)
        return h, buf

    return jax.shard_map(device_step, mesh=mesh, in_specs=(row_spec, P(), P(), P(), P(), row_spec, row_spec), out_specs=(row_spec, buf_spec), check_vma=False)
```

```python
import functools
import math

import jax
import jax.numpy as jnp
from jax import lax
from jax.experimental import pallas as pl
from jax.experimental.pallas import tpu as pltpu
from jax.sharding import PartitionSpec as P

HEAD_DIM = 128
SCORE_SCALE = 1.0 / math.sqrt(HEAD_DIM)
MESH_IDS = pl.DeviceIdType.MESH
LANES = 128
CORES = 2
Q_COLS = 512
B_COLS = 256
F32 = jnp.float32
BF16 = jnp.bfloat16


def block_kernel(side, x_hbm, wq_hbm, wk_hbm, wv_hbm, wo_hbm, ids_hbm, probs_hbm,
                 buf_out, h_out,
                 xbuf, wq_v, wk_v, wv_v, wo_v, ids_v, probs_v, kv_own, kvbuf, meta_own, meta_buf, q_s, o_own, o_sib,
                 h_buf, sel_s, gate_s,
                 wsem, pair_send, pair_recv, kv_send, kv_recv, kv2_send, kv2_recv, mt_send, mt_recv, h_send, h_recv,
                 d_send, d_recv):
    tok = x_hbm.shape[0]
    tok2 = CORES * tok
    half_q = wq_v.shape[1]
    half_kv = wk_v.shape[1] // CORES
    half_w = wo_v.shape[1]
    kv_half_heads = half_kv // HEAD_DIM
    q_half_heads = half_q // HEAD_DIM
    per_kv = q_half_heads // kv_half_heads
    own_experts = buf_out.shape[0]
    experts = probs_v.shape[1]
    n_chips = side * side

    me = lax.axis_index('sp')
    core = me % CORES
    chip = me // CORES
    cy = chip // side
    cx = chip % side
    a0 = cx + (cy - cx) * core
    b0 = cy + (cx - cy) * core

    def chip_at(a, b):
        y = b + (a - b) * core
        x = a + (b - a) * core
        return y * side + x

    def peer(c):
        return {'sp': c * CORES + core}

    sib = {'sp': chip * CORES + (1 - core)}

    def remote(src, dst, ss, rs, dev):
        return pltpu.make_async_remote_copy(src_ref=src, dst_ref=dst, send_sem=ss, recv_sem=rs,
                                            device_id=dev, device_id_type=MESH_IDS)

    barrier = pltpu.get_barrier_semaphore()
    partners = [sib]
    for d in range(1, side):
        for c in range(CORES):
            partners.append({'sp': (cy * side + (cx + d) % side) * CORES + c})
            partners.append({'sp': ((cy + d) % side * side + cx) * CORES + c})
    for p in partners:
        pl.semaphore_signal(barrier, inc=1, device_id=p, device_id_type=MESH_IDS)

    my_rows = pl.ds(pl.multiple_of(core * tok, tok), tok)
    loads = {}

    def load(name, src, dst):
        loads[name] = pltpu.make_async_copy(src, dst, wsem.at[len(loads)])
        loads[name].start()

    load('x', x_hbm, xbuf.at[my_rows, :])
    load('ids', ids_hbm, ids_v)
    load('probs', probs_hbm, probs_v)
    load('k', wk_hbm, wk_v)
    load('v', wv_hbm, wv_v)
    n_q = half_q // Q_COLS
    for i in range(n_q):
        load(('q', i), wq_hbm.at[:, pl.ds(pl.multiple_of(core * half_q + i * Q_COLS, Q_COLS), Q_COLS)],
             wq_v.at[:, pl.ds(i * Q_COLS, Q_COLS)])
    o_cols = pl.ds(pl.multiple_of(core * half_w, half_w), half_w)
    load('o0', wo_hbm.at[pl.ds(pl.multiple_of(core * half_q, half_q), half_q), o_cols], wo_v.at[pl.ds(0, half_q), :])
    load('o1', wo_hbm.at[pl.ds(pl.multiple_of((1 - core) * half_q, half_q), half_q), o_cols],
         wo_v.at[pl.ds(half_q, half_q), :])

    for slot in range(n_chips):
        y, x = slot // side, slot % side

        @pl.when((slot > chip) & (y + (x - y) * core != b0))
        def _():
            kvbuf[slot] = jnp.zeros(kvbuf.shape[1:], BF16)

    loads['x'].wait()
    loads['ids'].wait()
    loads['probs'].wait()
    idf = ids_v[...].astype(F32)
    probs = probs_v[...]
    lane_e = lax.broadcasted_iota(jnp.int32, (tok, experts), 1).astype(F32)
    eye_t = lax.broadcasted_iota(jnp.int32, (tok, tok), 0) == lax.broadcasted_iota(jnp.int32, (tok, tok), 1)
    id0 = jnp.sum(jnp.where(eye_t, idf[0:1, :], 0.0), axis=1, keepdims=True)
    id1 = jnp.sum(jnp.where(eye_t, idf[1:2, :], 0.0), axis=1, keepdims=True)
    p0 = jnp.sum(jnp.where(lane_e == id0, probs, 0.0), axis=1, keepdims=True)
    p1 = jnp.sum(jnp.where(lane_e == id1, probs, 0.0), axis=1, keepdims=True)
    psum = p0 + p1
    lane_t = lax.broadcasted_iota(jnp.int32, (tok, LANES), 1)
    row_t = lax.broadcasted_iota(jnp.int32, (tok, LANES), 0)
    per_group = LANES // tok2
    eye = lane_t == row_t + core * tok + chip % per_group * tok2

    def to_lanes(col):
        return jnp.sum(jnp.where(eye, col, 0.0), axis=0, keepdims=True)

    meta_rows = [to_lanes(id0), to_lanes(id1), to_lanes(p0 / psum), to_lanes(p1 / psum)]
    meta_own[0] = jnp.concatenate(meta_rows + [jnp.zeros((4, LANES), F32)], axis=0)

    x_own = xbuf[my_rows, :]
    for name, w_ref, at in (('k', wk_v, 0), ('v', wv_v, half_kv)):
        loads[name].wait()
        out = jnp.dot(x_own, w_ref[...], preferred_element_type=F32).astype(BF16)
        for c in range(CORES):
            kv_own[c, :, at:at + half_kv] = out[:, c * half_kv:(c + 1) * half_kv]
    kvbuf[chip, my_rows, :] = kv_own[core]

    pl.semaphore_wait(barrier, len(partners))
    x_pair = remote(xbuf.at[my_rows, :], xbuf.at[my_rows, :], pair_send.at[0], pair_recv.at[0], sib)
    x_pair.start()
    m_pair = remote(meta_own.at[0], meta_own.at[1], pair_send.at[1], pair_recv.at[1], sib)
    m_pair.start()
    kv_pair = remote(kv_own.at[1 - core], kvbuf.at[chip, my_rows, :], pair_send.at[2], pair_recv.at[2], sib)
    kv_pair.start()

    def kv_first(d, c):
        y = (cy + d * c) % side
        x = (cx + d * (1 - c)) % side
        i = cx + (cy - cx) * c
        return remote(kv_own.at[c], kvbuf.at[chip, my_rows, :], kv_send.at[CORES * d + c],
                      kv_recv.at[CORES * i + core], {'sp': (y * side + x) * CORES + c})

    def kv_first_from(i, c):
        return remote(kv_own.at[c], kvbuf.at[chip_at(i, b0), pl.ds(c * tok, tok), :], kv_send.at[0],
                      kv_recv.at[CORES * i + c], sib)

    for d in (2, 1, side - 1):
        for c in range(CORES):
            kv_first(d, c).start()

    class Gather:
        def __init__(self, ref, ss, rs):
            self.ref, self.ss, self.rs = ref, ss, rs

        def first(self, d, slot):
            return remote(self.ref(slot), self.ref(slot), self.ss.at[d], self.rs.at[a0],
                          peer(chip_at((a0 + d) % side, b0)))

        def first_from(self, i, slot):
            return remote(self.ref(slot), self.ref(slot), self.ss.at[0], self.rs.at[i], sib)

        def second(self, i, d, slot):
            return remote(self.ref(slot), self.ref(slot), self.ss.at[side + i * side + d],
                          self.rs.at[side + i * side + b0], peer(chip_at(a0, (b0 + d) % side)))

        def relay(self, i, step):
            j = (b0 - step + side) % side
            slot = chip_at(i, j)
            return remote(self.ref(slot), self.ref(slot), self.ss.at[side + i * side + 2],
                          self.rs.at[side + i * side + j], peer(chip_at(a0, (b0 + step + side) % side)))

        def second_from(self, i, j, slot):
            return remote(self.ref(slot), self.ref(slot), self.ss.at[0], self.rs.at[side + i * side + j], sib)

        def open(self):
            for d in (2, 1, side - 1):
                self.first(d, chip).start()
            self.spread(a0)

        def spread(self, i):
            for d in (2, 1, side - 1):
                self.second(i, d, chip_at(i, b0)).start()

        def sent(self):
            for d in range(1, side):
                self.first(d, chip).wait_send()
                for i in range(side):
                    self.second(i, d, chip_at(i, b0)).wait_send()

    kvg = Gather(lambda s: kvbuf.at[s], kv2_send, kv2_recv)

    def kv_second(i, wait):
        slot = chip_at(i, b0)
        for d in (2, 1, side - 1):
            @pl.when(chip_at(a0, (b0 + d) % side) > slot)
            def _():
                c = kvg.second(i, d, slot)
                if wait:
                    c.wait_send()
                else:
                    c.start()

    kv_pair.wait_recv()
    kv_second(a0, False)
    m_pair.wait_recv()
    meta_buf[chip] = meta_own[0] + meta_own[1]
    mt = Gather(lambda s: meta_buf.at[s], mt_send, mt_recv)
    mt.open()

    x_pair.wait_recv()
    xs = xbuf[...]
    for i in range(n_q):
        loads[('q', i)].wait()
        cols = slice(i * Q_COLS, (i + 1) * Q_COLS)
        q_s[:, cols] = jnp.dot(xs, wq_v[:, cols], preferred_element_type=F32).astype(BF16)

    def kv_pass(i, carry):
        @pl.when(i != a0)
        def _():
            for c in range(CORES):
                kv_first_from(i, c).wait_recv()
            kv_second(i, False)
            mt.first_from(i, chip_at(i, b0)).wait_recv()
            mt.spread(i)
        return carry

    lax.fori_loop(0, side, kv_pass, 0)

    def kv_done(n, carry):
        i, j = n // side, n % side

        @pl.when((j != b0) & (chip_at(i, j) < chip))
        def _():
            kvg.second_from(i, j, chip_at(i, j)).wait_recv()
        return carry

    lax.fori_loop(0, n_chips, kv_done, 0)

    seq = n_chips * tok2
    q_pos = chip * tok2 + lax.broadcasted_iota(jnp.int32, (per_kv * tok2, seq), 0) % tok2
    k_pos = lax.broadcasted_iota(jnp.int32, (per_kv * tok2, seq), 1)
    causal = k_pos <= q_pos
    o_pairs = []
    for g in range(kv_half_heads):
        kc = slice(g * HEAD_DIM, (g + 1) * HEAD_DIM)
        vc = slice(half_kv + g * HEAD_DIM, half_kv + (g + 1) * HEAD_DIM)
        k_all = kvbuf[:, :, kc].reshape(seq, HEAD_DIM)
        v_all = kvbuf[:, :, vc].reshape(seq, HEAD_DIM)
        q_g = jnp.concatenate([q_s[:, (g * per_kv + h) * HEAD_DIM:(g * per_kv + h + 1) * HEAD_DIM]
                               for h in range(per_kv)], axis=0)
        s = lax.dot_general(q_g, k_all, (((1,), (1,)), ((), ())), preferred_element_type=F32) * SCORE_SCALE
        s = jnp.where(causal, s, -1e30)
        e = jnp.exp(s - jnp.max(s, axis=1, keepdims=True))
        w = (e / jnp.sum(e, axis=1, keepdims=True)).astype(BF16)
        o_g = jnp.dot(w, v_all, preferred_element_type=F32).astype(BF16)
        gw = per_kv * HEAD_DIM
        for h in range(per_kv):
            o_own[:, g * gw + h * HEAD_DIM:g * gw + (h + 1) * HEAD_DIM] = o_g[h * tok2:(h + 1) * tok2, :]
        cols = pl.ds(g * gw, gw)
        c = remote(o_own.at[:, cols], o_sib.at[:, cols], pair_send.at[3 + g], pair_recv.at[3 + g], sib)
        c.start()
        o_pairs.append(c)

    loads['o0'].wait()
    acc = jnp.dot(o_own[...], wo_v[0:half_q, :], preferred_element_type=F32)
    loads['o1'].wait()
    for c in o_pairs:
        c.wait_recv()
    acc = acc + jnp.dot(o_sib[...], wo_v[half_q:2 * half_q, :], preferred_element_type=F32)
    my_cols = pl.ds(pl.multiple_of(core * half_w, half_w), half_w)
    h_buf[core, chip] = (xbuf[:, my_cols].astype(F32) + acc).astype(BF16)

    hg = Gather(lambda s: h_buf.at[core, s], h_send, h_recv)

    def cross(slot):
        at = h_buf.at[core, slot]
        return remote(at, at, d_send.at[slot], d_recv.at[slot], sib)

    def cross_from(slot):
        at = h_buf.at[1 - core, slot]
        return remote(at, at, d_send.at[slot], d_recv.at[slot], sib)

    relays = ((0, 1), (1, -1), (3, -1))

    def h_spread(k):
        i = (a0 - k + side) % side
        slot = chip_at(i, b0)
        for d in (1, side - 1):
            hg.second(i, d, slot).start()
        if k == 2:
            hg.second(i, 2, slot).start()

    for d in (1, side - 1, 2):
        hg.first(d, chip).start()
    h_spread(0)
    cross(chip).start()

    def meta_done(n, carry):
        i, j = n // side, n % side

        @pl.when(j != b0)
        def _():
            mt.second_from(i, j, chip_at(i, j)).wait_recv()
        return carry

    lax.fori_loop(0, n_chips, meta_done, 0)

    g_tok = per_group * tok2
    n_groups = n_chips // per_group
    t_row = lax.broadcasted_iota(jnp.int32, (g_tok, g_tok), 0)
    t_col = lax.broadcasted_iota(jnp.int32, (g_tok, g_tok), 1)
    before = jnp.where((t_row < t_col) & (t_row // tok == t_col // tok), 1.0, 0.0).astype(BF16)
    lane_8 = lax.broadcasted_iota(jnp.int32, (8, g_tok), 1)
    source_base = (lane_8 // tok * tok).astype(F32)
    expert_8 = (lax.broadcasted_iota(jnp.int32, (8, g_tok), 0) + me * own_experts).astype(F32)
    slot_row = t_row.astype(F32)

    def select_rows(g, carry):
        m = meta_buf[g * per_group]
        for c in range(1, per_group):
            m = m + meta_buf[g * per_group + c]
        hit0 = m[0:1, :] == expert_8
        hit1 = m[1:2, :] == expert_8
        hit = hit0 | hit1
        slot = jnp.dot(jnp.where(hit, 1.0, 0.0).astype(BF16), before, preferred_element_type=F32)
        row = jnp.where(hit, slot + source_base, -1.0)
        gate = jnp.where(hit0, m[2:3, :], jnp.where(hit1, m[3:4, :], 0.0))
        for k in range(own_experts):
            rows = pl.ds(k * g_tok, g_tok)
            pick = slot_row == row[k:k + 1, :]
            sel_s[g, rows, :] = jnp.where(pick, 1.0, 0.0).astype(BF16)
            gate_k = jnp.sum(jnp.where(pick, gate[k:k + 1, :], 0.0), axis=1, keepdims=True)
            gate_s[g, rows, :] = jnp.broadcast_to(gate_k, (g_tok, LANES))
        return carry

    lax.fori_loop(0, n_groups, select_rows, 0)

    def build(g, col_half):
        at = pl.ds(pl.multiple_of(g * g_tok, g_tok), g_tok)
        h_g = h_buf[col_half, pl.ds(g * per_group, per_group)].reshape(g_tok, half_w)
        for n in range(half_w // B_COLS):
            rows = jnp.dot(sel_s[g], h_g[:, n * B_COLS:(n + 1) * B_COLS], preferred_element_type=F32)
            gate = gate_s[g]
            rows = jnp.concatenate([rows[:, i * LANES:(i + 1) * LANES] * gate for i in range(B_COLS // LANES)], axis=1)
            rows = rows.astype(BF16)
            cols = pl.ds(pl.multiple_of(col_half * half_w + n * B_COLS, B_COLS), B_COLS)
            for k in range(own_experts):
                buf_out[k, at, cols] = rows[k * g_tok:(k + 1) * g_tok, :]

    def take_first(k):
        i = (a0 - k + side) % side
        slot = chip_at(i, b0)
        hg.first_from(i, slot).wait_recv()
        h_spread(k)
        cross(slot).start()

    def take_relay(k, step):
        i = (a0 - k + side) % side
        j = (b0 - step + side) % side
        slot = chip_at(i, j)
        hg.second_from(i, j, slot).wait_recv()
        hg.relay(i, step).start()
        cross(slot).start()

    take_first(1)
    take_first(side - 1)
    take_relay(*relays[0])
    take_first(2)
    take_relay(*relays[1])
    take_relay(*relays[2])

    def take_rest(g, carry):
        @pl.when(g < n_groups)
        def _():
            for c in range(per_group):
                slot = g * per_group + c
                y, x = slot // side, slot % side
                i = x + (y - x) * core
                j = y + (x - y) * core
                todo = j != b0
                for k, step in relays:
                    todo = todo & ((i != (a0 - k + side) % side) | (j != (b0 - step + side) % side))

                @pl.when(todo)
                def _():
                    hg.second_from(i, j, slot).wait_recv()
                    cross(slot).start()
            build(g, core)

        @pl.when(g > 0)
        def _():
            for c in range(per_group):
                cross_from((g - 1) * per_group + c).wait_recv()
            build(g - 1, 1 - core)
        return carry

    lax.fori_loop(0, n_groups + 1, take_rest, 0)
    for c in range(CORES):
        h_out[:, c * half_w:(c + 1) * half_w] = h_buf[c, chip, my_rows, :]

    for c in [x_pair, m_pair, kv_pair] + o_pairs:
        c.wait_send()
    for d in range(1, side):
        for c in range(CORES):
            kv_first(d, c).wait_send()
    for i in range(side):
        kv_second(i, True)
    mt.sent()
    hg.sent()
    for slot in range(n_chips):
        cross(slot).wait_send()


def store_kernel(buf_ref, h_ref, buf_out, h_out, sem):
    n = buf_ref.shape[0]
    copies = [pltpu.make_async_copy(buf_ref.at[k], buf_out.at[k], sem.at[k]) for k in range(n)]
    copies.append(pltpu.make_async_copy(h_ref, h_out, sem.at[n]))
    for c in copies:
        c.start()
    for c in copies:
        c.wait()


def solution(mesh):
    group = mesh.shape['sp']
    side = math.isqrt(group // CORES)
    row_spec = P(('dp', 'sp'), None)
    buf_spec = P(('dp', 'sp'), None, None)
    any_spec = pl.BlockSpec(memory_space=pl.ANY)
    hbm_spec = pl.BlockSpec(memory_space=pltpu.HBM)
    vmem_spec = pl.BlockSpec(memory_space=pltpu.VMEM)

    def device_step(x_loc, w_q, w_k, w_v, w_o, ids_loc, probs_loc):
        tok, width = x_loc.shape
        experts = probs_loc.shape[1]
        own = experts // group
        chips = side * side
        tok2 = CORES * tok
        half_q = w_q.shape[1] // CORES
        half_kv = w_k.shape[1] // CORES
        half_w = width // CORES
        dma = pltpu.SemaphoreType.DMA
        n_loads = 7 + half_q // Q_COLS
        kv_half_heads = half_kv // HEAD_DIM
        buf, h = pl.pallas_call(
            functools.partial(block_kernel, side),
            out_shape=(pltpu.VMEM((own, tok * group, width), BF16), pltpu.VMEM((tok, width), BF16)),
            in_specs=[hbm_spec] * 7,
            out_specs=(vmem_spec, vmem_spec),
            scratch_shapes=[
                pltpu.VMEM((tok2, width), BF16),
                pltpu.VMEM((width, half_q), BF16),
                pltpu.VMEM((width, CORES * half_kv), BF16),
                pltpu.VMEM((width, CORES * half_kv), BF16),
                pltpu.VMEM((2 * half_q, half_w), BF16),
                pltpu.VMEM((2, tok), jnp.int32),
                pltpu.VMEM((tok, experts), F32),
                pltpu.VMEM((CORES, tok, 2 * half_kv), BF16),
                pltpu.VMEM((chips, tok2, 2 * half_kv), BF16),
                pltpu.VMEM((CORES, 8, LANES), F32),
                pltpu.VMEM((chips, 8, LANES), F32),
                pltpu.VMEM((tok2, half_q), BF16),
                pltpu.VMEM((tok2, half_q), BF16),
                pltpu.VMEM((tok2, half_q), BF16),
                pltpu.VMEM((CORES, chips, tok2, half_w), BF16),
                pltpu.VMEM((chips * tok2 // LANES, own * LANES, LANES), BF16),
                pltpu.VMEM((chips * tok2 // LANES, own * LANES, LANES), F32),
                dma((n_loads,)),
                dma((3 + kv_half_heads,)), dma((3 + kv_half_heads,)),
                dma((CORES * side,)), dma((CORES * side,)),
                dma((side + chips,)), dma((side + chips,)), dma((side + chips,)), dma((side + chips,)),
                dma((side + chips,)), dma((side + chips,)),
                dma((chips,)), dma((chips,)),
            ],
            compiler_params=pltpu.CompilerParams(collective_id=0, has_side_effects=True,
                                                 vmem_limit_bytes=55 * 2 ** 20 + 850 * 1024),
            name='attention_block',
        )(x_loc, w_q, w_k, w_v, w_o, ids_loc.T, probs_loc)
        buf, h = pl.pallas_call(
            store_kernel,
            out_shape=(jax.ShapeDtypeStruct((own, tok * group, width), BF16), jax.ShapeDtypeStruct((tok, width), BF16)),
            in_specs=[vmem_spec, vmem_spec],
            out_specs=(any_spec, any_spec),
            scratch_shapes=[dma((own + 1,))],
            compiler_params=pltpu.CompilerParams(vmem_limit_bytes=16 * 2 ** 20),
            name='store_outputs',
        )(buf, h)
        return h, buf

    return jax.shard_map(device_step, mesh=mesh, in_specs=(row_spec, P(), P(), P(), P(), row_spec, row_spec), out_specs=(row_spec, buf_spec), check_vma=False)
```

```python
import functools
import math

import jax
import jax.numpy as jnp
from jax import lax
from jax.experimental import pallas as pl
from jax.experimental.pallas import tpu as pltpu
from jax.sharding import PartitionSpec as P

HEAD_DIM = 128
SCORE_SCALE = 1.0 / math.sqrt(HEAD_DIM)
MESH_IDS = pl.DeviceIdType.MESH
LANES = 128
CORES = 2
Q_COLS = 512
Q_EARLY = 0
B_COLS = 256
F32 = jnp.float32
BF16 = jnp.bfloat16


def block_kernel(side, x_hbm, wq_hbm, wk_hbm, wv_hbm, wo_hbm, ids_hbm, probs_hbm,
                 buf_out, h_out,
                 xbuf, wq_v, wk_v, wv_v, wo_v, ids_v, probs_v, kv_own, kvbuf, meta_own, meta_buf, q_s, o_own, o_sib,
                 h_buf, sel_s, gate_s,
                 wsem, pair_send, pair_recv, kv_send, kv_recv, kv2_send, kv2_recv, mt_send, mt_recv, h_send, h_recv,
                 d_send, d_recv):
    tok = x_hbm.shape[0]
    tok2 = CORES * tok
    half_q = wq_v.shape[1]
    half_kv = wk_v.shape[1] // CORES
    half_w = wo_v.shape[1]
    kv_half_heads = half_kv // HEAD_DIM
    q_half_heads = half_q // HEAD_DIM
    per_kv = q_half_heads // kv_half_heads
    own_experts = buf_out.shape[0]
    experts = probs_v.shape[1]
    n_chips = side * side

    me = lax.axis_index('sp')
    core = me % CORES
    chip = me // CORES
    cy = chip // side
    cx = chip % side
    a0 = cx + (cy - cx) * core
    b0 = cy + (cx - cy) * core

    def chip_at(a, b):
        y = b + (a - b) * core
        x = a + (b - a) * core
        return y * side + x

    def peer(c):
        return {'sp': c * CORES + core}

    sib = {'sp': chip * CORES + (1 - core)}

    def remote(src, dst, ss, rs, dev):
        return pltpu.make_async_remote_copy(src_ref=src, dst_ref=dst, send_sem=ss, recv_sem=rs,
                                            device_id=dev, device_id_type=MESH_IDS)

    barrier = pltpu.get_barrier_semaphore()
    partners = [sib]
    for d in range(1, side):
        for c in range(CORES):
            partners.append({'sp': (cy * side + (cx + d) % side) * CORES + c})
            partners.append({'sp': ((cy + d) % side * side + cx) * CORES + c})
    for p in partners:
        pl.semaphore_signal(barrier, inc=1, device_id=p, device_id_type=MESH_IDS)

    my_rows = pl.ds(pl.multiple_of(core * tok, tok), tok)
    loads = {}

    def load(name, src, dst):
        loads[name] = pltpu.make_async_copy(src, dst, wsem.at[len(loads)])
        loads[name].start()

    load('x', x_hbm, xbuf.at[my_rows, :])
    load('ids', ids_hbm, ids_v)
    load('probs', probs_hbm, probs_v)
    load('k', wk_hbm, wk_v)
    load('v', wv_hbm, wv_v)
    n_q = half_q // Q_COLS
    for i in range(n_q):
        load(('q', i), wq_hbm.at[:, pl.ds(pl.multiple_of(core * half_q + i * Q_COLS, Q_COLS), Q_COLS)],
             wq_v.at[:, pl.ds(i * Q_COLS, Q_COLS)])
    o_cols = pl.ds(pl.multiple_of(core * half_w, half_w), half_w)
    load('o0', wo_hbm.at[pl.ds(pl.multiple_of(core * half_q, half_q), half_q), o_cols], wo_v.at[pl.ds(0, half_q), :])
    load('o1', wo_hbm.at[pl.ds(pl.multiple_of((1 - core) * half_q, half_q), half_q), o_cols],
         wo_v.at[pl.ds(half_q, half_q), :])

    for slot in range(n_chips):
        y, x = slot // side, slot % side

        @pl.when((slot > chip) & (y + (x - y) * core != b0))
        def _():
            kvbuf[slot] = jnp.zeros(kvbuf.shape[1:], BF16)

    loads['x'].wait()
    loads['ids'].wait()
    loads['probs'].wait()
    idf = ids_v[...].astype(F32)
    probs = probs_v[...]
    lane_e = lax.broadcasted_iota(jnp.int32, (tok, experts), 1).astype(F32)
    eye_t = lax.broadcasted_iota(jnp.int32, (tok, tok), 0) == lax.broadcasted_iota(jnp.int32, (tok, tok), 1)
    id0 = jnp.sum(jnp.where(eye_t, idf[0:1, :], 0.0), axis=1, keepdims=True)
    id1 = jnp.sum(jnp.where(eye_t, idf[1:2, :], 0.0), axis=1, keepdims=True)
    p0 = jnp.sum(jnp.where(lane_e == id0, probs, 0.0), axis=1, keepdims=True)
    p1 = jnp.sum(jnp.where(lane_e == id1, probs, 0.0), axis=1, keepdims=True)
    psum = p0 + p1
    lane_t = lax.broadcasted_iota(jnp.int32, (tok, LANES), 1)
    row_t = lax.broadcasted_iota(jnp.int32, (tok, LANES), 0)
    meta_rows = []
    for place in (cx, cy):
        eye = lane_t == row_t + core * tok + place * tok2
        for col in (id0, id1, p0 / psum, p1 / psum):
            meta_rows.append(jnp.sum(jnp.where(eye, col, 0.0), axis=0, keepdims=True))
    meta_own[0] = jnp.concatenate(meta_rows, axis=0)

    x_own = xbuf[my_rows, :]
    for name, w_ref, at in (('k', wk_v, 0), ('v', wv_v, half_kv)):
        loads[name].wait()
        out = jnp.dot(x_own, w_ref[...], preferred_element_type=F32).astype(BF16)
        for c in range(CORES):
            kv_own[c, :, at:at + half_kv] = out[:, c * half_kv:(c + 1) * half_kv]
    kvbuf[chip, my_rows, :] = kv_own[core]

    pl.semaphore_wait(barrier, len(partners))
    x_pair = remote(xbuf.at[my_rows, :], xbuf.at[my_rows, :], pair_send.at[0], pair_recv.at[0], sib)
    x_pair.start()
    m_pair = remote(meta_own.at[0], meta_own.at[1], pair_send.at[1], pair_recv.at[1], sib)
    m_pair.start()
    kv_pair = remote(kv_own.at[1 - core], kvbuf.at[chip, my_rows, :], pair_send.at[2], pair_recv.at[2], sib)
    kv_pair.start()

    def kv_first(d, c):
        y = (cy + d * c) % side
        x = (cx + d * (1 - c)) % side
        i = cx + (cy - cx) * c
        return remote(kv_own.at[c], kvbuf.at[chip, my_rows, :], kv_send.at[CORES * d + c],
                      kv_recv.at[CORES * i + core], {'sp': (y * side + x) * CORES + c})

    def kv_first_from(i, c):
        return remote(kv_own.at[c], kvbuf.at[chip_at(i, b0), pl.ds(c * tok, tok), :], kv_send.at[0],
                      kv_recv.at[CORES * i + c], sib)

    for d in (2, 1, side - 1):
        for c in range(CORES):
            kv_first(d, c).start()

    class Gather:
        def __init__(self, ref, ss, rs):
            self.ref, self.ss, self.rs = ref, ss, rs

        def copy(self, i, j, s, r, dev):
            return remote(self.ref(i, j), self.ref(i, j), self.ss.at[s], self.rs.at[r], dev)

        def first(self, d):
            return self.copy(a0, b0, d, a0, peer(chip_at((a0 + d) % side, b0)))

        def first_from(self, i):
            return self.copy(i, b0, 0, i, sib)

        def second(self, i, d):
            return self.copy(i, b0, side + i * side + d, side + i * side + b0, peer(chip_at(a0, (b0 + d) % side)))

        def relay(self, i, step):
            j = (b0 - step + side) % side
            return self.copy(i, j, side + i * side + 2, side + i * side + j,
                             peer(chip_at(a0, (b0 + step + side) % side)))

        def second_from(self, i, j):
            return self.copy(i, j, 0, side + i * side + j, sib)

        def open(self):
            for d in (2, 1, side - 1):
                self.first(d).start()
            self.spread(a0)

        def spread(self, i):
            for d in (2, 1, side - 1):
                self.second(i, d).start()

        def sent(self):
            for d in range(1, side):
                self.first(d).wait_send()
                for i in range(side):
                    self.second(i, d).wait_send()

    kvg = Gather(lambda i, j: kvbuf.at[chip_at(i, j)], kv2_send, kv2_recv)

    def kv_second(i, wait):
        slot = chip_at(i, b0)
        for d in (2, 1, side - 1):
            @pl.when(chip_at(a0, (b0 + d) % side) > slot)
            def _():
                c = kvg.second(i, d)
                if wait:
                    c.wait_send()
                else:
                    c.start()

    kv_pair.wait_recv()
    kv_second(a0, False)
    m_pair.wait_recv()
    meta_buf[chip] = meta_own[0] + meta_own[1]
    mt = Gather(lambda i, j: meta_buf.at[chip_at(i, j)], mt_send, mt_recv)
    mt.open()

    def project_q(chunks):
        for n in chunks:
            loads[('q', n)].wait()
            cols = slice(n * Q_COLS, (n + 1) * Q_COLS)
            q_s[:, cols] = jnp.dot(xbuf[...], wq_v[:, cols], preferred_element_type=F32).astype(BF16)

    x_pair.wait_recv()
    project_q(range(Q_EARLY))

    def kv_pass(i, carry):
        @pl.when(i != a0)
        def _():
            for c in range(CORES):
                kv_first_from(i, c).wait_recv()
            kv_second(i, False)
            mt.first_from(i).wait_recv()
            mt.spread(i)
        return carry

    lax.fori_loop(0, side, kv_pass, 0)

    project_q(range(Q_EARLY, n_q))

    def kv_done(n, carry):
        i, j = n // side, n % side

        @pl.when((j != b0) & (chip_at(i, j) < chip))
        def _():
            kvg.second_from(i, j).wait_recv()
        return carry

    lax.fori_loop(0, n_chips, kv_done, 0)

    seq = n_chips * tok2
    q_pos = chip * tok2 + lax.broadcasted_iota(jnp.int32, (per_kv * tok2, seq), 0) % tok2
    k_pos = lax.broadcasted_iota(jnp.int32, (per_kv * tok2, seq), 1)
    causal = k_pos <= q_pos
    o_pairs = []
    for g in range(kv_half_heads):
        kc = slice(g * HEAD_DIM, (g + 1) * HEAD_DIM)
        vc = slice(half_kv + g * HEAD_DIM, half_kv + (g + 1) * HEAD_DIM)
        k_all = kvbuf[:, :, kc].reshape(seq, HEAD_DIM)
        v_all = kvbuf[:, :, vc].reshape(seq, HEAD_DIM)
        q_g = jnp.concatenate([q_s[:, (g * per_kv + h) * HEAD_DIM:(g * per_kv + h + 1) * HEAD_DIM]
                               for h in range(per_kv)], axis=0)
        s = lax.dot_general(q_g, k_all, (((1,), (1,)), ((), ())), preferred_element_type=F32) * SCORE_SCALE
        s = jnp.where(causal, s, -1e30)
        e = jnp.exp(s - jnp.max(s, axis=1, keepdims=True))
        w = (e / jnp.sum(e, axis=1, keepdims=True)).astype(BF16)
        o_g = jnp.dot(w, v_all, preferred_element_type=F32).astype(BF16)
        gw = per_kv * HEAD_DIM
        for h in range(per_kv):
            o_own[:, g * gw + h * HEAD_DIM:g * gw + (h + 1) * HEAD_DIM] = o_g[h * tok2:(h + 1) * tok2, :]
        cols = pl.ds(g * gw, gw)
        c = remote(o_own.at[:, cols], o_sib.at[:, cols], pair_send.at[3 + g], pair_recv.at[3 + g], sib)
        c.start()
        o_pairs.append(c)

    loads['o0'].wait()
    acc = jnp.dot(o_own[...], wo_v[0:half_q, :], preferred_element_type=F32)
    loads['o1'].wait()
    for c in o_pairs:
        c.wait_recv()
    acc = acc + jnp.dot(o_sib[...], wo_v[half_q:2 * half_q, :], preferred_element_type=F32)
    my_cols = pl.ds(pl.multiple_of(core * half_w, half_w), half_w)
    h_buf[core, b0 * side + a0] = (xbuf[:, my_cols].astype(F32) + acc).astype(BF16)

    hg = Gather(lambda i, j: h_buf.at[core, j * side + i], h_send, h_recv)

    def cross(i, j):
        at = h_buf.at[core, j * side + i]
        return remote(at, at, d_send.at[j * side + i], d_recv.at[j * side + i], sib)

    def cross_from(n):
        at = h_buf.at[1 - core, n]
        return remote(at, at, d_send.at[n], d_recv.at[n], sib)

    relays = {0: 1, 1: -1, side - 1: -1}

    def back(at, d):
        return (at - d + side) % side

    def h_spread(k):
        for d in (1, side - 1) if k in relays else (1, side - 1, 2):
            hg.second(back(a0, k), d).start()

    for d in (1, side - 1, 2):
        hg.first(d).start()
    h_spread(0)
    cross(a0, b0).start()

    def meta_done(n, carry):
        i, j = n // side, n % side

        @pl.when(j != b0)
        def _():
            mt.second_from(i, j).wait_recv()
        return carry

    lax.fori_loop(0, n_chips, meta_done, 0)

    g_tok = side * tok2
    t_row = lax.broadcasted_iota(jnp.int32, (g_tok, g_tok), 0)
    t_col = lax.broadcasted_iota(jnp.int32, (g_tok, g_tok), 1)
    before = jnp.where((t_row < t_col) & (t_row // tok == t_col // tok), 1.0, 0.0).astype(BF16)
    lane_8 = lax.broadcasted_iota(jnp.int32, (8, g_tok), 1)
    source_base = (lane_8 // tok * tok).astype(F32)
    expert_8 = (lax.broadcasted_iota(jnp.int32, (8, g_tok), 0) + me * own_experts).astype(F32)
    slot_row = t_row.astype(F32)

    def select_rows(g, carry):
        for half in range(CORES):
            m = jnp.zeros((8, g_tok), F32)
            for a in range(side):
                m = m + meta_buf[a * side + g if half else g * side + a]
            m = m[4 * half:4 * half + 4, :]
            hit0 = m[0:1, :] == expert_8
            hit1 = m[1:2, :] == expert_8
            hit = hit0 | hit1
            slot = jnp.dot(jnp.where(hit, 1.0, 0.0).astype(BF16), before, preferred_element_type=F32)
            row = jnp.where(hit, slot + source_base, -1.0)
            gate = jnp.where(hit0, m[2:3, :], jnp.where(hit1, m[3:4, :], 0.0))
            for k in range(own_experts):
                rows = pl.ds(k * g_tok, g_tok)
                pick = slot_row == row[k:k + 1, :]
                sel_s[half * side + g, rows, :] = jnp.where(pick, 1.0, 0.0).astype(BF16)
                gate_k = jnp.sum(jnp.where(pick, gate[k:k + 1, :], 0.0), axis=1, keepdims=True)
                gate_s[half * side + g, rows, :] = jnp.broadcast_to(gate_k, (g_tok, LANES))
        return carry

    lax.fori_loop(0, side, select_rows, 0)

    def build(half, g):
        n = half * side + g
        for q in range(half_w // B_COLS):
            h_g = h_buf[half, pl.ds(g * side, side), :, q * B_COLS:(q + 1) * B_COLS].reshape(g_tok, B_COLS)
            rows = jnp.dot(sel_s[n], h_g, preferred_element_type=F32)
            gate = gate_s[n]
            rows = jnp.concatenate([rows[:, i * LANES:(i + 1) * LANES] * gate for i in range(B_COLS // LANES)], axis=1)
            rows = rows.astype(BF16)
            cols = pl.ds(pl.multiple_of(half * half_w + q * B_COLS, B_COLS), B_COLS)
            for a in range(side):
                slot = (g + (a - g) * half) * side + a + (g - a) * half
                at = pl.ds(pl.multiple_of(slot * tok2, tok2), tok2)
                for k in range(own_experts):
                    buf_out[k, at, cols] = rows[k * g_tok + a * tok2:k * g_tok + (a + 1) * tok2, :]

    def take_first(k):
        i = back(a0, k)
        hg.first_from(i).wait_recv()
        h_spread(k)
        cross(i, b0).start()

    def take(k, d):
        i, j = back(a0, k), back(b0, d)
        hg.second_from(i, j).wait_recv()
        if k in relays and d == (relays[k] + side) % side:
            hg.relay(i, relays[k]).start()
        cross(i, j).start()

    def build_other(d):
        g = back(a0, d)
        for a in range(side):
            cross_from(g * side + a).wait_recv()
        build(1 - core, g)

    take_first(1)
    take_first(side - 1)
    take(0, 1)
    take_first(2)
    build(core, b0)
    take(1, side - 1)
    take(side - 1, side - 1)
    for k in (1, side - 1, 2):
        take(k, 1)
    build(core, back(b0, 1))
    build_other(0)
    take(0, side - 1)
    take(2, side - 1)
    build(core, back(b0, side - 1))
    build_other(1)
    for k in (0, 2, 1, side - 1):
        take(k, 2)
    build_other(side - 1)
    build(core, back(b0, 2))
    build_other(2)
    for c in range(CORES):
        h_out[:, c * half_w:(c + 1) * half_w] = h_buf[c, cx * side + cy if c else chip, my_rows, :]

    for c in [x_pair, m_pair, kv_pair] + o_pairs:
        c.wait_send()
    for d in range(1, side):
        for c in range(CORES):
            kv_first(d, c).wait_send()
    for i in range(side):
        kv_second(i, True)
    mt.sent()
    hg.sent()
    for i in range(side):
        for j in range(side):
            cross(i, j).wait_send()


def store_kernel(buf_ref, h_ref, buf_out, h_out, sem):
    n = buf_ref.shape[0]
    copies = [pltpu.make_async_copy(buf_ref.at[k], buf_out.at[k], sem.at[k]) for k in range(n)]
    copies.append(pltpu.make_async_copy(h_ref, h_out, sem.at[n]))
    for c in copies:
        c.start()
    for c in copies:
        c.wait()


def solution(mesh):
    group = mesh.shape['sp']
    side = math.isqrt(group // CORES)
    row_spec = P(('dp', 'sp'), None)
    buf_spec = P(('dp', 'sp'), None, None)
    any_spec = pl.BlockSpec(memory_space=pl.ANY)
    hbm_spec = pl.BlockSpec(memory_space=pltpu.HBM)
    vmem_spec = pl.BlockSpec(memory_space=pltpu.VMEM)

    def device_step(x_loc, w_q, w_k, w_v, w_o, ids_loc, probs_loc):
        tok, width = x_loc.shape
        experts = probs_loc.shape[1]
        own = experts // group
        chips = side * side
        tok2 = CORES * tok
        half_q = w_q.shape[1] // CORES
        half_kv = w_k.shape[1] // CORES
        half_w = width // CORES
        dma = pltpu.SemaphoreType.DMA
        n_loads = 7 + half_q // Q_COLS
        kv_half_heads = half_kv // HEAD_DIM
        buf, h = pl.pallas_call(
            functools.partial(block_kernel, side),
            out_shape=(pltpu.VMEM((own, tok * group, width), BF16), pltpu.VMEM((tok, width), BF16)),
            in_specs=[hbm_spec] * 7,
            out_specs=(vmem_spec, vmem_spec),
            scratch_shapes=[
                pltpu.VMEM((tok2, width), BF16),
                pltpu.VMEM((width, half_q), BF16),
                pltpu.VMEM((width, CORES * half_kv), BF16),
                pltpu.VMEM((width, CORES * half_kv), BF16),
                pltpu.VMEM((2 * half_q, half_w), BF16),
                pltpu.VMEM((2, tok), jnp.int32),
                pltpu.VMEM((tok, experts), F32),
                pltpu.VMEM((CORES, tok, 2 * half_kv), BF16),
                pltpu.VMEM((chips, tok2, 2 * half_kv), BF16),
                pltpu.VMEM((CORES, 8, LANES), F32),
                pltpu.VMEM((chips, 8, LANES), F32),
                pltpu.VMEM((tok2, half_q), BF16),
                pltpu.VMEM((tok2, half_q), BF16),
                pltpu.VMEM((tok2, half_q), BF16),
                pltpu.VMEM((CORES, chips, tok2, half_w), BF16),
                pltpu.VMEM((CORES * side, own * side * tok2, side * tok2), BF16),
                pltpu.VMEM((CORES * side, own * side * tok2, LANES), F32),
                dma((n_loads,)),
                dma((3 + kv_half_heads,)), dma((3 + kv_half_heads,)),
                dma((CORES * side,)), dma((CORES * side,)),
                dma((side + chips,)), dma((side + chips,)), dma((side + chips,)), dma((side + chips,)),
                dma((side + chips,)), dma((side + chips,)),
                dma((chips,)), dma((chips,)),
            ],
            compiler_params=pltpu.CompilerParams(collective_id=0, has_side_effects=True,
                                                 vmem_limit_bytes=55 * 2 ** 20 + 850 * 1024),
            name='attention_block',
        )(x_loc, w_q, w_k, w_v, w_o, ids_loc.T, probs_loc)
        buf, h = pl.pallas_call(
            store_kernel,
            out_shape=(jax.ShapeDtypeStruct((own, tok * group, width), BF16), jax.ShapeDtypeStruct((tok, width), BF16)),
            in_specs=[vmem_spec, vmem_spec],
            out_specs=(any_spec, any_spec),
            scratch_shapes=[dma((own + 1,))],
            compiler_params=pltpu.CompilerParams(vmem_limit_bytes=16 * 2 ** 20),
            name='store_outputs',
        )(buf, h)
        return h, buf

    return jax.shard_map(device_step, mesh=mesh, in_specs=(row_spec, P(), P(), P(), P(), row_spec, row_spec), out_specs=(row_spec, buf_spec), check_vma=False)
```

```python
import functools
import math

import jax
import jax.numpy as jnp
from jax import lax
from jax.experimental import pallas as pl
from jax.experimental.pallas import tpu as pltpu
from jax.sharding import PartitionSpec as P

HEAD_DIM = 128
SCORE_SCALE = 1.0 / math.sqrt(HEAD_DIM)
MESH_IDS = pl.DeviceIdType.MESH
LANES = 128
CORES = 2
Q_COLS = 512
Q_EARLY = 0
B_COLS = 256
F32 = jnp.float32
BF16 = jnp.bfloat16


def group_rows(side, tok2, half, g, a):
    slot = (g + (a - g) * half) * side + a + (g - a) * half
    return pl.ds(pl.multiple_of(slot * tok2, tok2), tok2)


def build_group(side, tok2, n_exp, h_ref, sel_ref, gate_ref, half, g, put):
    g_tok = side * tok2
    n = half * side + g
    for q in range(h_ref.shape[3] // B_COLS):
        h_g = h_ref[half, pl.ds(g * side, side), :, q * B_COLS:(q + 1) * B_COLS].reshape(g_tok, B_COLS)
        rows = jnp.dot(sel_ref[n], h_g, preferred_element_type=F32)
        gate = gate_ref[n]
        rows = jnp.concatenate([rows[:, i * LANES:(i + 1) * LANES] * gate for i in range(B_COLS // LANES)], axis=1)
        rows = rows.astype(BF16)
        for a in range(side):
            for k in range(n_exp):
                put(a, k, q, rows[k * g_tok + a * tok2:k * g_tok + (a + 1) * tok2, :])


def block_kernel(side, x_hbm, wq_hbm, wk_hbm, wv_hbm, wo_hbm, ids_hbm, probs_hbm,
                 buf_out, h_buf, sel_s, gate_s,
                 xbuf, wq_v, wk_v, wv_v, wo_v, ids_v, probs_v, kv_own, kvbuf, meta_own, meta_buf, q_s, o_own, o_sib,
                 wsem, pair_send, pair_recv, kv_send, kv_recv, kv2_send, kv2_recv, mt_send, mt_recv, h_send, h_recv,
                 d_send, d_recv):
    tok = x_hbm.shape[0]
    tok2 = CORES * tok
    half_q = wq_v.shape[1]
    half_kv = wk_v.shape[1] // CORES
    half_w = wo_v.shape[1]
    kv_half_heads = half_kv // HEAD_DIM
    q_half_heads = half_q // HEAD_DIM
    per_kv = q_half_heads // kv_half_heads
    own_experts = buf_out.shape[0]
    experts = probs_v.shape[1]
    n_chips = side * side

    me = lax.axis_index('sp')
    core = me % CORES
    chip = me // CORES
    cy = chip // side
    cx = chip % side
    a0 = cx + (cy - cx) * core
    b0 = cy + (cx - cy) * core

    def chip_at(a, b):
        y = b + (a - b) * core
        x = a + (b - a) * core
        return y * side + x

    def peer(c):
        return {'sp': c * CORES + core}

    sib = {'sp': chip * CORES + (1 - core)}

    def remote(src, dst, ss, rs, dev):
        return pltpu.make_async_remote_copy(src_ref=src, dst_ref=dst, send_sem=ss, recv_sem=rs,
                                            device_id=dev, device_id_type=MESH_IDS)

    barrier = pltpu.get_barrier_semaphore()
    partners = [sib]
    for d in range(1, side):
        for c in range(CORES):
            partners.append({'sp': (cy * side + (cx + d) % side) * CORES + c})
            partners.append({'sp': ((cy + d) % side * side + cx) * CORES + c})
    for p in partners:
        pl.semaphore_signal(barrier, inc=1, device_id=p, device_id_type=MESH_IDS)

    my_rows = pl.ds(pl.multiple_of(core * tok, tok), tok)
    loads = {}

    def load(name, src, dst):
        loads[name] = pltpu.make_async_copy(src, dst, wsem.at[len(loads)])
        loads[name].start()

    load('x', x_hbm, xbuf.at[my_rows, :])
    load('ids', ids_hbm, ids_v)
    load('probs', probs_hbm, probs_v)
    load('k', wk_hbm, wk_v)
    load('v', wv_hbm, wv_v)
    n_q = half_q // Q_COLS
    for i in range(n_q):
        load(('q', i), wq_hbm.at[:, pl.ds(pl.multiple_of(core * half_q + i * Q_COLS, Q_COLS), Q_COLS)],
             wq_v.at[:, pl.ds(i * Q_COLS, Q_COLS)])
    o_cols = pl.ds(pl.multiple_of(core * half_w, half_w), half_w)
    load('o0', wo_hbm.at[pl.ds(pl.multiple_of(core * half_q, half_q), half_q), o_cols], wo_v.at[pl.ds(0, half_q), :])
    load('o1', wo_hbm.at[pl.ds(pl.multiple_of((1 - core) * half_q, half_q), half_q), o_cols],
         wo_v.at[pl.ds(half_q, half_q), :])

    for slot in range(n_chips):
        y, x = slot // side, slot % side

        @pl.when((slot > chip) & (y + (x - y) * core != b0))
        def _():
            kvbuf[slot] = jnp.zeros(kvbuf.shape[1:], BF16)

    loads['x'].wait()
    loads['ids'].wait()
    loads['probs'].wait()
    idf = ids_v[...].astype(F32)
    probs = probs_v[...]
    lane_e = lax.broadcasted_iota(jnp.int32, (tok, experts), 1).astype(F32)
    eye_t = lax.broadcasted_iota(jnp.int32, (tok, tok), 0) == lax.broadcasted_iota(jnp.int32, (tok, tok), 1)
    id0 = jnp.sum(jnp.where(eye_t, idf[0:1, :], 0.0), axis=1, keepdims=True)
    id1 = jnp.sum(jnp.where(eye_t, idf[1:2, :], 0.0), axis=1, keepdims=True)
    p0 = jnp.sum(jnp.where(lane_e == id0, probs, 0.0), axis=1, keepdims=True)
    p1 = jnp.sum(jnp.where(lane_e == id1, probs, 0.0), axis=1, keepdims=True)
    psum = p0 + p1
    lane_t = lax.broadcasted_iota(jnp.int32, (tok, LANES), 1)
    row_t = lax.broadcasted_iota(jnp.int32, (tok, LANES), 0)
    meta_rows = []
    for place in (cx, cy):
        eye = lane_t == row_t + core * tok + place * tok2
        for col in (id0, id1, p0 / psum, p1 / psum):
            meta_rows.append(jnp.sum(jnp.where(eye, col, 0.0), axis=0, keepdims=True))
    meta_own[0] = jnp.concatenate(meta_rows, axis=0)

    x_own = xbuf[my_rows, :]
    for name, w_ref, at in (('k', wk_v, 0), ('v', wv_v, half_kv)):
        loads[name].wait()
        out = jnp.dot(x_own, w_ref[...], preferred_element_type=F32).astype(BF16)
        for c in range(CORES):
            kv_own[c, :, at:at + half_kv] = out[:, c * half_kv:(c + 1) * half_kv]
    kvbuf[chip, my_rows, :] = kv_own[core]

    pl.semaphore_wait(barrier, len(partners))
    x_pair = remote(xbuf.at[my_rows, :], xbuf.at[my_rows, :], pair_send.at[0], pair_recv.at[0], sib)
    x_pair.start()
    m_pair = remote(meta_own.at[0], meta_own.at[1], pair_send.at[1], pair_recv.at[1], sib)
    m_pair.start()
    kv_pair = remote(kv_own.at[1 - core], kvbuf.at[chip, my_rows, :], pair_send.at[2], pair_recv.at[2], sib)
    kv_pair.start()

    def kv_first(d, c):
        y = (cy + d * c) % side
        x = (cx + d * (1 - c)) % side
        i = cx + (cy - cx) * c
        return remote(kv_own.at[c], kvbuf.at[chip, my_rows, :], kv_send.at[CORES * d + c],
                      kv_recv.at[CORES * i + core], {'sp': (y * side + x) * CORES + c})

    def kv_first_from(i, c):
        return remote(kv_own.at[c], kvbuf.at[chip_at(i, b0), pl.ds(c * tok, tok), :], kv_send.at[0],
                      kv_recv.at[CORES * i + c], sib)

    for d in (2, 1, side - 1):
        for c in range(CORES):
            kv_first(d, c).start()

    class Gather:
        def __init__(self, ref, ss, rs):
            self.ref, self.ss, self.rs = ref, ss, rs

        def copy(self, i, j, s, r, dev):
            return remote(self.ref(i, j), self.ref(i, j), self.ss.at[s], self.rs.at[r], dev)

        def first(self, d):
            return self.copy(a0, b0, d, a0, peer(chip_at((a0 + d) % side, b0)))

        def first_from(self, i):
            return self.copy(i, b0, 0, i, sib)

        def second(self, i, d):
            return self.copy(i, b0, side + i * side + d, side + i * side + b0, peer(chip_at(a0, (b0 + d) % side)))

        def relay(self, i, step):
            j = (b0 - step + side) % side
            return self.copy(i, j, side + i * side + 2, side + i * side + j,
                             peer(chip_at(a0, (b0 + step + side) % side)))

        def second_from(self, i, j):
            return self.copy(i, j, 0, side + i * side + j, sib)

        def open(self):
            for d in (2, 1, side - 1):
                self.first(d).start()
            self.spread(a0)

        def spread(self, i):
            for d in (2, 1, side - 1):
                self.second(i, d).start()

        def sent(self):
            for d in range(1, side):
                self.first(d).wait_send()
                for i in range(side):
                    self.second(i, d).wait_send()

    kvg = Gather(lambda i, j: kvbuf.at[chip_at(i, j)], kv2_send, kv2_recv)

    def kv_second(i, wait):
        slot = chip_at(i, b0)
        for d in (2, 1, side - 1):
            @pl.when(chip_at(a0, (b0 + d) % side) > slot)
            def _():
                c = kvg.second(i, d)
                if wait:
                    c.wait_send()
                else:
                    c.start()

    kv_pair.wait_recv()
    kv_second(a0, False)
    m_pair.wait_recv()
    meta_buf[chip] = meta_own[0] + meta_own[1]
    mt = Gather(lambda i, j: meta_buf.at[chip_at(i, j)], mt_send, mt_recv)
    mt.open()

    def project_q(chunks):
        for n in chunks:
            loads[('q', n)].wait()
            cols = slice(n * Q_COLS, (n + 1) * Q_COLS)
            q_s[:, cols] = jnp.dot(xbuf[...], wq_v[:, cols], preferred_element_type=F32).astype(BF16)

    x_pair.wait_recv()
    project_q(range(Q_EARLY))

    def kv_pass(i, carry):
        @pl.when(i != a0)
        def _():
            for c in range(CORES):
                kv_first_from(i, c).wait_recv()
            kv_second(i, False)
            mt.first_from(i).wait_recv()
            mt.spread(i)
        return carry

    lax.fori_loop(0, side, kv_pass, 0)

    project_q(range(Q_EARLY, n_q))

    def kv_done(n, carry):
        i, j = n // side, n % side

        @pl.when((j != b0) & (chip_at(i, j) < chip))
        def _():
            kvg.second_from(i, j).wait_recv()
        return carry

    lax.fori_loop(0, n_chips, kv_done, 0)

    seq = n_chips * tok2
    q_pos = chip * tok2 + lax.broadcasted_iota(jnp.int32, (per_kv * tok2, seq), 0) % tok2
    k_pos = lax.broadcasted_iota(jnp.int32, (per_kv * tok2, seq), 1)
    causal = k_pos <= q_pos
    o_pairs = []
    for g in range(kv_half_heads):
        kc = slice(g * HEAD_DIM, (g + 1) * HEAD_DIM)
        vc = slice(half_kv + g * HEAD_DIM, half_kv + (g + 1) * HEAD_DIM)
        k_all = kvbuf[:, :, kc].reshape(seq, HEAD_DIM)
        v_all = kvbuf[:, :, vc].reshape(seq, HEAD_DIM)
        q_g = jnp.concatenate([q_s[:, (g * per_kv + h) * HEAD_DIM:(g * per_kv + h + 1) * HEAD_DIM]
                               for h in range(per_kv)], axis=0)
        s = lax.dot_general(q_g, k_all, (((1,), (1,)), ((), ())), preferred_element_type=F32) * SCORE_SCALE
        s = jnp.where(causal, s, -1e30)
        e = jnp.exp(s - jnp.max(s, axis=1, keepdims=True))
        w = (e / jnp.sum(e, axis=1, keepdims=True)).astype(BF16)
        o_g = jnp.dot(w, v_all, preferred_element_type=F32).astype(BF16)
        gw = per_kv * HEAD_DIM
        for h in range(per_kv):
            o_own[:, g * gw + h * HEAD_DIM:g * gw + (h + 1) * HEAD_DIM] = o_g[h * tok2:(h + 1) * tok2, :]
        cols = pl.ds(g * gw, gw)
        c = remote(o_own.at[:, cols], o_sib.at[:, cols], pair_send.at[3 + g], pair_recv.at[3 + g], sib)
        c.start()
        o_pairs.append(c)

    loads['o0'].wait()
    acc = jnp.dot(o_own[...], wo_v[0:half_q, :], preferred_element_type=F32)
    loads['o1'].wait()
    for c in o_pairs:
        c.wait_recv()
    acc = acc + jnp.dot(o_sib[...], wo_v[half_q:2 * half_q, :], preferred_element_type=F32)
    my_cols = pl.ds(pl.multiple_of(core * half_w, half_w), half_w)
    h_buf[core, b0 * side + a0] = (xbuf[:, my_cols].astype(F32) + acc).astype(BF16)

    hg = Gather(lambda i, j: h_buf.at[core, j * side + i], h_send, h_recv)

    def cross(i, j):
        at = h_buf.at[core, j * side + i]
        return remote(at, at, d_send.at[j * side + i], d_recv.at[j * side + i], sib)

    def cross_from(n):
        at = h_buf.at[1 - core, n]
        return remote(at, at, d_send.at[n], d_recv.at[n], sib)

    relays = {0: 1, 1: -1, side - 1: -1}

    def back(at, d):
        return (at - d + side) % side

    def h_spread(k):
        for d in (1, side - 1) if k in relays else (1, side - 1, 2):
            hg.second(back(a0, k), d).start()

    for d in (1, side - 1, 2):
        hg.first(d).start()
    h_spread(0)
    cross(a0, b0).start()

    def meta_done(n, carry):
        i, j = n // side, n % side

        @pl.when(j != b0)
        def _():
            mt.second_from(i, j).wait_recv()
        return carry

    lax.fori_loop(0, n_chips, meta_done, 0)

    g_tok = side * tok2
    t_row = lax.broadcasted_iota(jnp.int32, (g_tok, g_tok), 0)
    t_col = lax.broadcasted_iota(jnp.int32, (g_tok, g_tok), 1)
    before = jnp.where((t_row < t_col) & (t_row // tok == t_col // tok), 1.0, 0.0).astype(BF16)
    lane_8 = lax.broadcasted_iota(jnp.int32, (8, g_tok), 1)
    source_base = (lane_8 // tok * tok).astype(F32)
    expert_8 = (lax.broadcasted_iota(jnp.int32, (8, g_tok), 0) + me * own_experts).astype(F32)
    slot_row = t_row.astype(F32)

    def select_rows(g, carry):
        for half in range(CORES):
            m = jnp.zeros((8, g_tok), F32)
            for a in range(side):
                m = m + meta_buf[a * side + g if half else g * side + a]
            m = m[4 * half:4 * half + 4, :]
            hit0 = m[0:1, :] == expert_8
            hit1 = m[1:2, :] == expert_8
            hit = hit0 | hit1
            slot = jnp.dot(jnp.where(hit, 1.0, 0.0).astype(BF16), before, preferred_element_type=F32)
            row = jnp.where(hit, slot + source_base, -1.0)
            gate = jnp.where(hit0, m[2:3, :], jnp.where(hit1, m[3:4, :], 0.0))
            for k in range(own_experts):
                rows = pl.ds(k * g_tok, g_tok)
                pick = slot_row == row[k:k + 1, :]
                sel_s[half * side + g, rows, :] = jnp.where(pick, 1.0, 0.0).astype(BF16)
                gate_k = jnp.sum(jnp.where(pick, gate[k:k + 1, :], 0.0), axis=1, keepdims=True)
                gate_s[half * side + g, rows, :] = jnp.broadcast_to(gate_k, (g_tok, LANES))
        return carry

    lax.fori_loop(0, side, select_rows, 0)

    def build(half, g):
        def put(a, k, q, rows):
            cols = pl.ds(pl.multiple_of(half * half_w + q * B_COLS, B_COLS), B_COLS)
            buf_out[k, group_rows(side, tok2, half, g, a), cols] = rows

        build_group(side, tok2, own_experts, h_buf, sel_s, gate_s, half, g, put)

    def take_first(k):
        i = back(a0, k)
        hg.first_from(i).wait_recv()
        h_spread(k)
        cross(i, b0).start()

    def take(k, d):
        i, j = back(a0, k), back(b0, d)
        hg.second_from(i, j).wait_recv()
        if k in relays and d == (relays[k] + side) % side:
            hg.relay(i, relays[k]).start()
        cross(i, j).start()

    def other_done(d):
        for a in range(side):
            cross_from(back(a0, d) * side + a).wait_recv()

    def build_other(d):
        other_done(d)
        build(1 - core, back(a0, d))

    take_first(1)
    take_first(side - 1)
    take(0, 1)
    take_first(2)
    build(core, b0)
    build_other(0)
    take(1, side - 1)
    take(side - 1, side - 1)
    for k in (1, side - 1, 2):
        take(k, 1)
    take(0, side - 1)
    take(2, side - 1)
    for k in (0, 2):
        take(k, 2)
    build(core, back(b0, 1))
    build_other(1)
    build(core, back(b0, side - 1))
    for k in (1, side - 1):
        take(k, 2)
    for d in (side - 1, 2):
        other_done(d)

    for c in [x_pair, m_pair, kv_pair] + o_pairs:
        c.wait_send()
    for d in range(1, side):
        for c in range(CORES):
            kv_first(d, c).wait_send()
    for i in range(side):
        kv_second(i, True)
    mt.sent()
    hg.sent()
    for i in range(side):
        for j in range(side):
            cross(i, j).wait_send()


def store_kernel(side, buf_ref, h_ref, sel_ref, gate_ref, buf_out, h_out, stage, sem, stage_sem, h_sem):
    n_exp = buf_ref.shape[0]
    tok2, half_w = h_ref.shape[2:]
    tok = h_out.shape[0]
    me = lax.axis_index('sp')
    core = me % CORES
    chip = me // CORES
    cy = chip // side
    cx = chip % side
    a0 = cx + (cy - cx) * core
    b0 = cy + (cx - cy) * core
    copies = []

    def start(src, dst, s):
        copies.append(pltpu.make_async_copy(src, dst, s))
        copies[-1].start()

    def cols(half):
        return pl.ds(pl.multiple_of(half * half_w, half_w), half_w)

    other = 1 - core
    done = [(core, b0), (core, (b0 - 1 + side) % side), (core, (b0 + 1) % side), (other, a0), (other, (a0 - 1 + side) % side)]
    for n, (half, g) in enumerate(done):
        for a in range(side):
            rows = group_rows(side, tok2, half, g, a)
            start(buf_ref.at[:, rows, cols(half)], buf_out.at[:, rows, cols(half)], sem.at[n * side + a])
    my_rows = pl.ds(pl.multiple_of(core * tok, tok), tok)
    for c in range(CORES):
        start(h_ref.at[c, cx * side + cy if c else chip, my_rows, :], h_out.at[:, pl.ds(c * half_w, half_w)], h_sem.at[c])
    rest = [(core, (b0 + 2) % side), (other, (a0 + 1) % side), (other, (a0 + 2) % side)]
    for n, (half, g) in enumerate(rest):
        def put(a, k, q, rows, n=n):
            stage[n, k, a * tok2:(a + 1) * tok2, q * B_COLS:(q + 1) * B_COLS] = rows

        build_group(side, tok2, n_exp, h_ref, sel_ref, gate_ref, half, g, put)
        for a in range(side):
            start(stage.at[n, :, pl.ds(a * tok2, tok2), :], buf_out.at[:, group_rows(side, tok2, half, g, a), cols(half)],
                  stage_sem.at[n * side + a])
    for c in copies:
        c.wait()


def solution(mesh):
    group = mesh.shape['sp']
    side = math.isqrt(group // CORES)
    row_spec = P(('dp', 'sp'), None)
    buf_spec = P(('dp', 'sp'), None, None)
    any_spec = pl.BlockSpec(memory_space=pl.ANY)
    hbm_spec = pl.BlockSpec(memory_space=pltpu.HBM)
    vmem_spec = pl.BlockSpec(memory_space=pltpu.VMEM)

    def device_step(x_loc, w_q, w_k, w_v, w_o, ids_loc, probs_loc):
        tok, width = x_loc.shape
        experts = probs_loc.shape[1]
        own = experts // group
        chips = side * side
        tok2 = CORES * tok
        half_q = w_q.shape[1] // CORES
        half_kv = w_k.shape[1] // CORES
        half_w = width // CORES
        dma = pltpu.SemaphoreType.DMA
        n_loads = 7 + half_q // Q_COLS
        kv_half_heads = half_kv // HEAD_DIM
        g_tok = side * tok2
        parts = pl.pallas_call(
            functools.partial(block_kernel, side),
            out_shape=(pltpu.VMEM((own, tok * group, width), BF16),
                       pltpu.VMEM((CORES, chips, tok2, half_w), BF16),
                       pltpu.VMEM((CORES * side, own * g_tok, g_tok), BF16),
                       pltpu.VMEM((CORES * side, own * g_tok, LANES), F32)),
            in_specs=[hbm_spec] * 7,
            out_specs=(vmem_spec,) * 4,
            scratch_shapes=[
                pltpu.VMEM((tok2, width), BF16),
                pltpu.VMEM((width, half_q), BF16),
                pltpu.VMEM((width, CORES * half_kv), BF16),
                pltpu.VMEM((width, CORES * half_kv), BF16),
                pltpu.VMEM((2 * half_q, half_w), BF16),
                pltpu.VMEM((2, tok), jnp.int32),
                pltpu.VMEM((tok, experts), F32),
                pltpu.VMEM((CORES, tok, 2 * half_kv), BF16),
                pltpu.VMEM((chips, tok2, 2 * half_kv), BF16),
                pltpu.VMEM((CORES, 8, LANES), F32),
                pltpu.VMEM((chips, 8, LANES), F32),
                pltpu.VMEM((tok2, half_q), BF16),
                pltpu.VMEM((tok2, half_q), BF16),
                pltpu.VMEM((tok2, half_q), BF16),
                dma((n_loads,)),
                dma((3 + kv_half_heads,)), dma((3 + kv_half_heads,)),
                dma((CORES * side,)), dma((CORES * side,)),
                dma((side + chips,)), dma((side + chips,)), dma((side + chips,)), dma((side + chips,)),
                dma((side + chips,)), dma((side + chips,)),
                dma((chips,)), dma((chips,)),
            ],
            compiler_params=pltpu.CompilerParams(collective_id=0, has_side_effects=True,
                                                 vmem_limit_bytes=50 * 2 ** 20 + 900 * 1024),
            name='attention_block',
        )(x_loc, w_q, w_k, w_v, w_o, ids_loc.T, probs_loc)
        buf, h = pl.pallas_call(
            functools.partial(store_kernel, side),
            out_shape=(jax.ShapeDtypeStruct((own, tok * group, width), BF16), jax.ShapeDtypeStruct((tok, width), BF16)),
            in_specs=[vmem_spec] * 4,
            out_specs=(any_spec, any_spec),
            scratch_shapes=[pltpu.VMEM((3, own, g_tok, half_w), BF16),
                            dma((5 * side,)), dma((3 * side,)), dma((CORES,))],
            compiler_params=pltpu.CompilerParams(vmem_limit_bytes=16 * 2 ** 20),
            name='store_outputs',
        )(*parts)
        return h, buf

    return jax.shard_map(device_step, mesh=mesh, in_specs=(row_spec, P(), P(), P(), P(), row_spec, row_spec), out_specs=(row_spec, buf_spec), check_vma=False)
```

```python
import functools
import math

import jax
import jax.numpy as jnp
from jax import lax
from jax.experimental import pallas as pl
from jax.experimental.pallas import tpu as pltpu
from jax.sharding import PartitionSpec as P

HEAD_DIM = 128
SCORE_SCALE = 1.0 / math.sqrt(HEAD_DIM)
MESH_IDS = pl.DeviceIdType.MESH
LANES = 128
CORES = 2
Q_COLS = 512
Q_EARLY = 0
B_COLS = 256
F32 = jnp.float32
BF16 = jnp.bfloat16


def group_rows(side, tok2, half, g, a):
    slot = (g + (a - g) * half) * side + a + (g - a) * half
    return pl.ds(pl.multiple_of(slot * tok2, tok2), tok2)


def build_group(side, tok2, n_exp, h_ref, sel_ref, gate_ref, half, g, put):
    g_tok = side * tok2
    n = half * side + g
    for q in range(h_ref.shape[3] // B_COLS):
        h_g = h_ref[half, pl.ds(g * side, side), :, q * B_COLS:(q + 1) * B_COLS].reshape(g_tok, B_COLS)
        rows = jnp.dot(sel_ref[n], h_g, preferred_element_type=F32)
        gate = gate_ref[n]
        rows = jnp.concatenate([rows[:, i * LANES:(i + 1) * LANES] * gate for i in range(B_COLS // LANES)], axis=1)
        rows = rows.astype(BF16)
        for a in range(side):
            for k in range(n_exp):
                put(a, k, q, rows[k * g_tok + a * tok2:k * g_tok + (a + 1) * tok2, :])


def block_kernel(side, x_hbm, wq_hbm, wk_hbm, wv_hbm, wo_hbm, ids_hbm, probs_hbm,
                 buf_out, h_buf, sel_s, gate_s,
                 xbuf, wq_v, wk_v, wv_v, wo_v, ids_v, probs_v, kv_own, kvbuf, meta_own, meta_buf, q_s, o_own, o_sib,
                 wsem, pair_send, pair_recv, kv_send, kv_recv, kv2_send, kv2_recv, mt_send, mt_recv, h_send, h_recv,
                 d_send, d_recv):
    tok = x_hbm.shape[0]
    tok2 = CORES * tok
    half_q = wq_v.shape[1]
    half_kv = wk_v.shape[1] // CORES
    half_w = wo_v.shape[1]
    kv_half_heads = half_kv // HEAD_DIM
    q_half_heads = half_q // HEAD_DIM
    per_kv = q_half_heads // kv_half_heads
    own_experts = buf_out.shape[0]
    experts = probs_v.shape[1]
    n_chips = side * side

    me = lax.axis_index('sp')
    core = me % CORES
    chip = me // CORES
    cy = chip // side
    cx = chip % side
    a0 = cx + (cy - cx) * core
    b0 = cy + (cx - cy) * core

    def chip_at(a, b):
        y = b + (a - b) * core
        x = a + (b - a) * core
        return y * side + x

    def peer(c):
        return {'sp': c * CORES + core}

    sib = {'sp': chip * CORES + (1 - core)}

    def remote(src, dst, ss, rs, dev):
        return pltpu.make_async_remote_copy(src_ref=src, dst_ref=dst, send_sem=ss, recv_sem=rs,
                                            device_id=dev, device_id_type=MESH_IDS)

    my_rows = pl.ds(pl.multiple_of(core * tok, tok), tok)
    loads = {}

    def load(name, src, dst):
        loads[name] = pltpu.make_async_copy(src, dst, wsem.at[len(loads)])
        loads[name].start()

    load('x', x_hbm, xbuf.at[my_rows, :])
    load('ids', ids_hbm, ids_v)
    load('probs', probs_hbm, probs_v)
    load('k', wk_hbm, wk_v)
    load('v', wv_hbm, wv_v)
    barrier = pltpu.get_barrier_semaphore()
    partners = [sib]
    for d in range(1, side):
        for c in range(CORES):
            partners.append({'sp': (cy * side + (cx + d) % side) * CORES + c})
            partners.append({'sp': ((cy + d) % side * side + cx) * CORES + c})
    for p in partners:
        pl.semaphore_signal(barrier, inc=1, device_id=p, device_id_type=MESH_IDS)

    n_q = half_q // Q_COLS
    for i in range(n_q):
        load(('q', i), wq_hbm.at[:, pl.ds(pl.multiple_of(core * half_q + i * Q_COLS, Q_COLS), Q_COLS)],
             wq_v.at[:, pl.ds(i * Q_COLS, Q_COLS)])
    o_cols = pl.ds(pl.multiple_of(core * half_w, half_w), half_w)
    load('o0', wo_hbm.at[pl.ds(pl.multiple_of(core * half_q, half_q), half_q), o_cols], wo_v.at[pl.ds(0, half_q), :])
    load('o1', wo_hbm.at[pl.ds(pl.multiple_of((1 - core) * half_q, half_q), half_q), o_cols],
         wo_v.at[pl.ds(half_q, half_q), :])

    for slot in range(n_chips):
        y, x = slot // side, slot % side

        @pl.when((slot > chip) & (y + (x - y) * core != b0))
        def _():
            kvbuf[slot] = jnp.zeros(kvbuf.shape[1:], BF16)

    loads['x'].wait()
    loads['ids'].wait()
    loads['probs'].wait()
    idf = ids_v[...].astype(F32)
    probs = probs_v[...]
    lane_e = lax.broadcasted_iota(jnp.int32, (tok, experts), 1).astype(F32)
    eye_t = lax.broadcasted_iota(jnp.int32, (tok, tok), 0) == lax.broadcasted_iota(jnp.int32, (tok, tok), 1)
    id0 = jnp.sum(jnp.where(eye_t, idf[0:1, :], 0.0), axis=1, keepdims=True)
    id1 = jnp.sum(jnp.where(eye_t, idf[1:2, :], 0.0), axis=1, keepdims=True)
    p0 = jnp.sum(jnp.where(lane_e == id0, probs, 0.0), axis=1, keepdims=True)
    p1 = jnp.sum(jnp.where(lane_e == id1, probs, 0.0), axis=1, keepdims=True)
    psum = p0 + p1
    lane_t = lax.broadcasted_iota(jnp.int32, (tok, LANES), 1)
    row_t = lax.broadcasted_iota(jnp.int32, (tok, LANES), 0)
    meta_rows = []
    for place in (cx, cy):
        eye = lane_t == row_t + core * tok + place * tok2
        for col in (id0, id1, p0 / psum, p1 / psum):
            meta_rows.append(jnp.sum(jnp.where(eye, col, 0.0), axis=0, keepdims=True))
    meta_own[0] = jnp.concatenate(meta_rows, axis=0)

    x_own = xbuf[my_rows, :]
    for name, w_ref, at in (('k', wk_v, 0), ('v', wv_v, half_kv)):
        loads[name].wait()
        out = jnp.dot(x_own, w_ref[...], preferred_element_type=F32).astype(BF16)
        for c in range(CORES):
            kv_own[c, :, at:at + half_kv] = out[:, c * half_kv:(c + 1) * half_kv]
    kvbuf[chip, my_rows, :] = kv_own[core]

    pl.semaphore_wait(barrier, len(partners))
    x_pair = remote(xbuf.at[my_rows, :], xbuf.at[my_rows, :], pair_send.at[0], pair_recv.at[0], sib)
    x_pair.start()
    m_pair = remote(meta_own.at[0], meta_own.at[1], pair_send.at[1], pair_recv.at[1], sib)
    m_pair.start()
    kv_pair = remote(kv_own.at[1 - core], kvbuf.at[chip, my_rows, :], pair_send.at[2], pair_recv.at[2], sib)
    kv_pair.start()

    def kv_first(d, c):
        y = (cy + d * c) % side
        x = (cx + d * (1 - c)) % side
        i = cx + (cy - cx) * c
        return remote(kv_own.at[c], kvbuf.at[chip, my_rows, :], kv_send.at[CORES * d + c],
                      kv_recv.at[CORES * i + core], {'sp': (y * side + x) * CORES + c})

    def kv_first_from(i, c):
        return remote(kv_own.at[c], kvbuf.at[chip_at(i, b0), pl.ds(c * tok, tok), :], kv_send.at[0],
                      kv_recv.at[CORES * i + c], sib)

    for d in (2, 1, side - 1):
        for c in range(CORES):
            kv_first(d, c).start()

    class Gather:
        def __init__(self, ref, ss, rs):
            self.ref, self.ss, self.rs = ref, ss, rs

        def copy(self, i, j, s, r, dev):
            return remote(self.ref(i, j), self.ref(i, j), self.ss.at[s], self.rs.at[r], dev)

        def first(self, d):
            return self.copy(a0, b0, d, a0, peer(chip_at((a0 + d) % side, b0)))

        def first_from(self, i):
            return self.copy(i, b0, 0, i, sib)

        def second(self, i, d):
            return self.copy(i, b0, side + i * side + d, side + i * side + b0, peer(chip_at(a0, (b0 + d) % side)))

        def relay(self, i, step):
            j = (b0 - step + side) % side
            return self.copy(i, j, side + i * side + 2, side + i * side + j,
                             peer(chip_at(a0, (b0 + step + side) % side)))

        def second_from(self, i, j):
            return self.copy(i, j, 0, side + i * side + j, sib)

        def open(self):
            for d in (2, 1, side - 1):
                self.first(d).start()
            self.spread(a0)

        def spread(self, i):
            for d in (2, 1, side - 1):
                self.second(i, d).start()

        def sent(self):
            for d in range(1, side):
                self.first(d).wait_send()
                for i in range(side):
                    self.second(i, d).wait_send()

    kvg = Gather(lambda i, j: kvbuf.at[chip_at(i, j)], kv2_send, kv2_recv)

    def kv_second(i, wait):
        slot = chip_at(i, b0)
        for d in (2, 1, side - 1):
            @pl.when(chip_at(a0, (b0 + d) % side) > slot)
            def _():
                c = kvg.second(i, d)
                if wait:
                    c.wait_send()
                else:
                    c.start()

    kv_pair.wait_recv()
    kv_second(a0, False)
    m_pair.wait_recv()
    meta_buf[chip] = meta_own[0] + meta_own[1]
    mt = Gather(lambda i, j: meta_buf.at[chip_at(i, j)], mt_send, mt_recv)
    mt.open()

    def project_q(chunks):
        for n in chunks:
            loads[('q', n)].wait()
            cols = slice(n * Q_COLS, (n + 1) * Q_COLS)
            q_s[:, cols] = jnp.dot(xbuf[...], wq_v[:, cols], preferred_element_type=F32).astype(BF16)

    x_pair.wait_recv()
    project_q(range(Q_EARLY))

    def kv_pass(i, carry):
        @pl.when(i != a0)
        def _():
            for c in range(CORES):
                kv_first_from(i, c).wait_recv()
            kv_second(i, False)
            mt.first_from(i).wait_recv()
            mt.spread(i)
        return carry

    lax.fori_loop(0, side, kv_pass, 0)

    project_q(range(Q_EARLY, n_q))

    def kv_done(n, carry):
        i, j = n // side, n % side

        @pl.when((j != b0) & (chip_at(i, j) < chip))
        def _():
            kvg.second_from(i, j).wait_recv()
        return carry

    lax.fori_loop(0, n_chips, kv_done, 0)

    seq = n_chips * tok2
    q_pos = chip * tok2 + lax.broadcasted_iota(jnp.int32, (per_kv * tok2, seq), 0) % tok2
    k_pos = lax.broadcasted_iota(jnp.int32, (per_kv * tok2, seq), 1)
    causal = k_pos <= q_pos
    o_pairs = []
    for g in range(kv_half_heads):
        kc = slice(g * HEAD_DIM, (g + 1) * HEAD_DIM)
        vc = slice(half_kv + g * HEAD_DIM, half_kv + (g + 1) * HEAD_DIM)
        k_all = kvbuf[:, :, kc].reshape(seq, HEAD_DIM)
        v_all = kvbuf[:, :, vc].reshape(seq, HEAD_DIM)
        q_g = jnp.concatenate([q_s[:, (g * per_kv + h) * HEAD_DIM:(g * per_kv + h + 1) * HEAD_DIM]
                               for h in range(per_kv)], axis=0)
        s = lax.dot_general(q_g, k_all, (((1,), (1,)), ((), ())), preferred_element_type=F32) * SCORE_SCALE
        s = jnp.where(causal, s, -1e30)
        e = jnp.exp(s - jnp.max(s, axis=1, keepdims=True))
        w = (e / jnp.sum(e, axis=1, keepdims=True)).astype(BF16)
        o_g = jnp.dot(w, v_all, preferred_element_type=F32).astype(BF16)
        gw = per_kv * HEAD_DIM
        for h in range(per_kv):
            o_own[:, g * gw + h * HEAD_DIM:g * gw + (h + 1) * HEAD_DIM] = o_g[h * tok2:(h + 1) * tok2, :]
        cols = pl.ds(g * gw, gw)
        c = remote(o_own.at[:, cols], o_sib.at[:, cols], pair_send.at[3 + g], pair_recv.at[3 + g], sib)
        c.start()
        o_pairs.append(c)

    loads['o0'].wait()
    acc = jnp.dot(o_own[...], wo_v[0:half_q, :], preferred_element_type=F32)
    loads['o1'].wait()
    for c in o_pairs:
        c.wait_recv()
    acc = acc + jnp.dot(o_sib[...], wo_v[half_q:2 * half_q, :], preferred_element_type=F32)
    my_cols = pl.ds(pl.multiple_of(core * half_w, half_w), half_w)
    h_buf[core, b0 * side + a0] = (xbuf[:, my_cols].astype(F32) + acc).astype(BF16)

    hg = Gather(lambda i, j: h_buf.at[core, j * side + i], h_send, h_recv)

    def cross(i, j):
        at = h_buf.at[core, j * side + i]
        return remote(at, at, d_send.at[j * side + i], d_recv.at[j * side + i], sib)

    def cross_from(n):
        at = h_buf.at[1 - core, n]
        return remote(at, at, d_send.at[n], d_recv.at[n], sib)

    relays = {0: 1, 1: -1, side - 1: -1}

    def back(at, d):
        return (at - d + side) % side

    def h_spread(k):
        for d in (1, side - 1) if k in relays else (1, side - 1, 2):
            hg.second(back(a0, k), d).start()

    for d in (1, side - 1, 2):
        hg.first(d).start()
    h_spread(0)
    cross(a0, b0).start()

    def meta_done(n, carry):
        i, j = n // side, n % side

        @pl.when(j != b0)
        def _():
            mt.second_from(i, j).wait_recv()
        return carry

    lax.fori_loop(0, n_chips, meta_done, 0)

    g_tok = side * tok2
    t_row = lax.broadcasted_iota(jnp.int32, (g_tok, g_tok), 0)
    t_col = lax.broadcasted_iota(jnp.int32, (g_tok, g_tok), 1)
    before = jnp.where((t_row < t_col) & (t_row // tok == t_col // tok), 1.0, 0.0).astype(BF16)
    lane_8 = lax.broadcasted_iota(jnp.int32, (8, g_tok), 1)
    source_base = (lane_8 // tok * tok).astype(F32)
    expert_8 = (lax.broadcasted_iota(jnp.int32, (8, g_tok), 0) + me * own_experts).astype(F32)
    slot_row = t_row.astype(F32)

    def select_rows(g, carry):
        for half in range(CORES):
            m = jnp.zeros((8, g_tok), F32)
            for a in range(side):
                m = m + meta_buf[a * side + g if half else g * side + a]
            m = m[4 * half:4 * half + 4, :]
            hit0 = m[0:1, :] == expert_8
            hit1 = m[1:2, :] == expert_8
            hit = hit0 | hit1
            slot = jnp.dot(jnp.where(hit, 1.0, 0.0).astype(BF16), before, preferred_element_type=F32)
            row = jnp.where(hit, slot + source_base, -1.0)
            gate = jnp.where(hit0, m[2:3, :], jnp.where(hit1, m[3:4, :], 0.0))
            for k in range(own_experts):
                rows = pl.ds(k * g_tok, g_tok)
                pick = slot_row == row[k:k + 1, :]
                sel_s[half * side + g, rows, :] = jnp.where(pick, 1.0, 0.0).astype(BF16)
                gate_k = jnp.sum(jnp.where(pick, gate[k:k + 1, :], 0.0), axis=1, keepdims=True)
                gate_s[half * side + g, rows, :] = jnp.broadcast_to(gate_k, (g_tok, LANES))
        return carry

    lax.fori_loop(0, side, select_rows, 0)

    def build(half, g):
        def put(a, k, q, rows):
            cols = pl.ds(pl.multiple_of(half * half_w + q * B_COLS, B_COLS), B_COLS)
            buf_out[k, group_rows(side, tok2, half, g, a), cols] = rows

        build_group(side, tok2, own_experts, h_buf, sel_s, gate_s, half, g, put)

    def take_first(k):
        i = back(a0, k)
        hg.first_from(i).wait_recv()
        h_spread(k)
        cross(i, b0).start()

    def take(k, d):
        i, j = back(a0, k), back(b0, d)
        hg.second_from(i, j).wait_recv()
        if k in relays and d == (relays[k] + side) % side:
            hg.relay(i, relays[k]).start()
        cross(i, j).start()

    def other_done(d):
        for a in range(side):
            cross_from(back(a0, d) * side + a).wait_recv()

    def build_other(d):
        other_done(d)
        build(1 - core, back(a0, d))

    take_first(1)
    take_first(side - 1)
    take(0, 1)
    take_first(2)
    build(core, b0)
    build_other(0)
    take(1, side - 1)
    take(side - 1, side - 1)
    for k in (1, side - 1, 2):
        take(k, 1)
    take(0, side - 1)
    take(2, side - 1)
    for k in (0, 2):
        take(k, 2)
    build(core, back(b0, 1))
    build_other(1)
    build(core, back(b0, side - 1))
    for k in (1, side - 1):
        take(k, 2)
    for d in (side - 1, 2):
        other_done(d)

    for c in [x_pair, m_pair, kv_pair] + o_pairs:
        c.wait_send()
    for d in range(1, side):
        for c in range(CORES):
            kv_first(d, c).wait_send()
    for i in range(side):
        kv_second(i, True)
    mt.sent()
    hg.sent()
    for i in range(side):
        for j in range(side):
            cross(i, j).wait_send()


def store_kernel(side, buf_ref, h_ref, sel_ref, gate_ref, buf_out, h_out, stage, sem, stage_sem, h_sem):
    n_exp = buf_ref.shape[0]
    tok2, half_w = h_ref.shape[2:]
    tok = h_out.shape[0]
    me = lax.axis_index('sp')
    core = me % CORES
    chip = me // CORES
    cy = chip // side
    cx = chip % side
    a0 = cx + (cy - cx) * core
    b0 = cy + (cx - cy) * core
    copies = []

    def start(src, dst, s):
        copies.append(pltpu.make_async_copy(src, dst, s))
        copies[-1].start()

    def cols(half):
        return pl.ds(pl.multiple_of(half * half_w, half_w), half_w)

    other = 1 - core
    done = [(core, b0), (core, (b0 - 1 + side) % side), (core, (b0 + 1) % side), (other, a0), (other, (a0 - 1 + side) % side)]
    for n, (half, g) in enumerate(done):
        for a in range(side):
            rows = group_rows(side, tok2, half, g, a)
            start(buf_ref.at[:, rows, cols(half)], buf_out.at[:, rows, cols(half)], sem.at[n * side + a])
    my_rows = pl.ds(pl.multiple_of(core * tok, tok), tok)
    for c in range(CORES):
        start(h_ref.at[c, cx * side + cy if c else chip, my_rows, :], h_out.at[:, pl.ds(c * half_w, half_w)], h_sem.at[c])
    rest = [(core, (b0 + 2) % side), (other, (a0 + 1) % side), (other, (a0 + 2) % side)]
    for n, (half, g) in enumerate(rest):
        def put(a, k, q, rows, n=n):
            stage[n, k, a * tok2:(a + 1) * tok2, q * B_COLS:(q + 1) * B_COLS] = rows

        build_group(side, tok2, n_exp, h_ref, sel_ref, gate_ref, half, g, put)
        for a in range(side):
            start(stage.at[n, :, pl.ds(a * tok2, tok2), :], buf_out.at[:, group_rows(side, tok2, half, g, a), cols(half)],
                  stage_sem.at[n * side + a])
    for c in copies:
        c.wait()


def solution(mesh):
    group = mesh.shape['sp']
    side = math.isqrt(group // CORES)
    row_spec = P(('dp', 'sp'), None)
    buf_spec = P(('dp', 'sp'), None, None)
    any_spec = pl.BlockSpec(memory_space=pl.ANY)
    hbm_spec = pl.BlockSpec(memory_space=pltpu.HBM)
    vmem_spec = pl.BlockSpec(memory_space=pltpu.VMEM)

    def device_step(x_loc, w_q, w_k, w_v, w_o, ids_loc, probs_loc):
        tok, width = x_loc.shape
        experts = probs_loc.shape[1]
        own = experts // group
        chips = side * side
        tok2 = CORES * tok
        half_q = w_q.shape[1] // CORES
        half_kv = w_k.shape[1] // CORES
        half_w = width // CORES
        dma = pltpu.SemaphoreType.DMA
        n_loads = 7 + half_q // Q_COLS
        kv_half_heads = half_kv // HEAD_DIM
        g_tok = side * tok2
        parts = pl.pallas_call(
            functools.partial(block_kernel, side),
            out_shape=(pltpu.VMEM((own, tok * group, width), BF16),
                       pltpu.VMEM((CORES, chips, tok2, half_w), BF16),
                       pltpu.VMEM((CORES * side, own * g_tok, g_tok), BF16),
                       pltpu.VMEM((CORES * side, own * g_tok, LANES), F32)),
            in_specs=[hbm_spec] * 7,
            out_specs=(vmem_spec,) * 4,
            scratch_shapes=[
                pltpu.VMEM((tok2, width), BF16),
                pltpu.VMEM((width, half_q), BF16),
                pltpu.VMEM((width, CORES * half_kv), BF16),
                pltpu.VMEM((width, CORES * half_kv), BF16),
                pltpu.VMEM((2 * half_q, half_w), BF16),
                pltpu.VMEM((2, tok), jnp.int32),
                pltpu.VMEM((tok, experts), F32),
                pltpu.VMEM((CORES, tok, 2 * half_kv), BF16),
                pltpu.VMEM((chips, tok2, 2 * half_kv), BF16),
                pltpu.VMEM((CORES, 8, LANES), F32),
                pltpu.VMEM((chips, 8, LANES), F32),
                pltpu.VMEM((tok2, half_q), BF16),
                pltpu.VMEM((tok2, half_q), BF16),
                pltpu.VMEM((tok2, half_q), BF16),
                dma((n_loads,)),
                dma((3 + kv_half_heads,)), dma((3 + kv_half_heads,)),
                dma((CORES * side,)), dma((CORES * side,)),
                dma((side + chips,)), dma((side + chips,)), dma((side + chips,)), dma((side + chips,)),
                dma((side + chips,)), dma((side + chips,)),
                dma((chips,)), dma((chips,)),
            ],
            compiler_params=pltpu.CompilerParams(collective_id=0, has_side_effects=True,
                                                 vmem_limit_bytes=50 * 2 ** 20 + 900 * 1024),
            name='attention_block',
        )(x_loc, w_q, w_k, w_v, w_o, ids_loc.T, probs_loc)
        buf, h = pl.pallas_call(
            functools.partial(store_kernel, side),
            out_shape=(jax.ShapeDtypeStruct((own, tok * group, width), BF16), jax.ShapeDtypeStruct((tok, width), BF16)),
            in_specs=[vmem_spec] * 4,
            out_specs=(any_spec, any_spec),
            scratch_shapes=[pltpu.VMEM((3, own, g_tok, half_w), BF16),
                            dma((5 * side,)), dma((3 * side,)), dma((CORES,))],
            compiler_params=pltpu.CompilerParams(vmem_limit_bytes=16 * 2 ** 20),
            name='store_outputs',
        )(*parts)
        return h, buf

    return jax.shard_map(device_step, mesh=mesh, in_specs=(row_spec, P(), P(), P(), P(), row_spec, row_spec), out_specs=(row_spec, buf_spec), check_vma=False)
```

```python
import functools
import math

import jax
import jax.numpy as jnp
from jax import lax
from jax.experimental import pallas as pl
from jax.experimental.pallas import tpu as pltpu
from jax.sharding import PartitionSpec as P

HEAD_DIM = 128
SCORE_SCALE = 1.0 / math.sqrt(HEAD_DIM)
MESH_IDS = pl.DeviceIdType.MESH
LANES = 128
CORES = 2
Q_COLS = 512
Q_EARLY = 0
B_COLS = 256
F32 = jnp.float32
BF16 = jnp.bfloat16


def group_rows(side, tok2, half, g, a):
    slot = (g + (a - g) * half) * side + a + (g - a) * half
    return pl.ds(pl.multiple_of(slot * tok2, tok2), tok2)


def build_group(side, tok2, n_exp, h_ref, sel_ref, gate_ref, half, g, put):
    g_tok = side * tok2
    n = half * side + g
    for q in range(h_ref.shape[3] // B_COLS):
        h_g = h_ref[half, pl.ds(g * side, side), :, q * B_COLS:(q + 1) * B_COLS].reshape(g_tok, B_COLS)
        rows = jnp.dot(sel_ref[n], h_g, preferred_element_type=F32)
        gate = gate_ref[n]
        rows = jnp.concatenate([rows[:, i * LANES:(i + 1) * LANES] * gate for i in range(B_COLS // LANES)], axis=1)
        rows = rows.astype(BF16)
        for a in range(side):
            for k in range(n_exp):
                put(a, k, q, rows[k * g_tok + a * tok2:k * g_tok + (a + 1) * tok2, :])


def block_kernel(side, x_hbm, wq_hbm, wk_hbm, wv_hbm, wo_hbm, ids_hbm, probs_hbm,
                 buf_out, h_buf, sel_s, gate_s,
                 xbuf, wq_v, wk_v, wv_v, wo_v, ids_v, probs_v, kv_own, kvbuf, meta_own, meta_buf, q_s, o_own, o_sib,
                 wsem, pair_send, pair_recv, kv_send, kv_recv, kv2_send, kv2_recv, mt_send, mt_recv, h_send, h_recv,
                 d_send, d_recv):
    tok = x_hbm.shape[0]
    tok2 = CORES * tok
    half_q = wq_v.shape[1]
    half_kv = wk_v.shape[1] // CORES
    half_w = wo_v.shape[1]
    kv_half_heads = half_kv // HEAD_DIM
    q_half_heads = half_q // HEAD_DIM
    per_kv = q_half_heads // kv_half_heads
    own_experts = buf_out.shape[0]
    experts = probs_v.shape[1]
    n_chips = side * side

    me = lax.axis_index('sp')
    core = me % CORES
    chip = me // CORES
    cy = chip // side
    cx = chip % side
    a0 = cx + (cy - cx) * core
    b0 = cy + (cx - cy) * core

    def chip_at(a, b):
        y = b + (a - b) * core
        x = a + (b - a) * core
        return y * side + x

    def peer(c):
        return {'sp': c * CORES + core}

    sib = {'sp': chip * CORES + (1 - core)}

    def remote(src, dst, ss, rs, dev):
        return pltpu.make_async_remote_copy(src_ref=src, dst_ref=dst, send_sem=ss, recv_sem=rs,
                                            device_id=dev, device_id_type=MESH_IDS)

    my_rows = pl.ds(pl.multiple_of(core * tok, tok), tok)
    loads = {}

    def load(name, src, dst):
        loads[name] = pltpu.make_async_copy(src, dst, wsem.at[len(loads)])
        loads[name].start()

    load('x', x_hbm, xbuf.at[my_rows, :])
    load('ids', ids_hbm, ids_v)
    load('probs', probs_hbm, probs_v)
    load('k', wk_hbm, wk_v)
    load('v', wv_hbm, wv_v)
    barrier = pltpu.get_barrier_semaphore()
    partners = [sib]
    for d in range(1, side):
        for c in range(CORES):
            partners.append({'sp': (cy * side + (cx + d) % side) * CORES + c})
            partners.append({'sp': ((cy + d) % side * side + cx) * CORES + c})
    for p in partners:
        pl.semaphore_signal(barrier, inc=1, device_id=p, device_id_type=MESH_IDS)

    n_q = half_q // Q_COLS
    for i in range(n_q):
        load(('q', i), wq_hbm.at[:, pl.ds(pl.multiple_of(core * half_q + i * Q_COLS, Q_COLS), Q_COLS)],
             wq_v.at[:, pl.ds(i * Q_COLS, Q_COLS)])
    o_cols = pl.ds(pl.multiple_of(core * half_w, half_w), half_w)
    load('o0', wo_hbm.at[pl.ds(pl.multiple_of(core * half_q, half_q), half_q), o_cols], wo_v.at[pl.ds(0, half_q), :])
    load('o1', wo_hbm.at[pl.ds(pl.multiple_of((1 - core) * half_q, half_q), half_q), o_cols],
         wo_v.at[pl.ds(half_q, half_q), :])

    for slot in range(n_chips):
        y, x = slot // side, slot % side

        @pl.when((slot > chip) & (y + (x - y) * core != b0))
        def _():
            kvbuf[slot] = jnp.zeros(kvbuf.shape[1:], BF16)

    loads['x'].wait()
    loads['ids'].wait()
    loads['probs'].wait()
    idf = ids_v[...].astype(F32)
    probs = probs_v[...]
    lane_e = lax.broadcasted_iota(jnp.int32, (tok, experts), 1).astype(F32)
    eye_t = lax.broadcasted_iota(jnp.int32, (tok, tok), 0) == lax.broadcasted_iota(jnp.int32, (tok, tok), 1)
    id0 = jnp.sum(jnp.where(eye_t, idf[0:1, :], 0.0), axis=1, keepdims=True)
    id1 = jnp.sum(jnp.where(eye_t, idf[1:2, :], 0.0), axis=1, keepdims=True)
    p0 = jnp.sum(jnp.where(lane_e == id0, probs, 0.0), axis=1, keepdims=True)
    p1 = jnp.sum(jnp.where(lane_e == id1, probs, 0.0), axis=1, keepdims=True)
    psum = p0 + p1
    lane_t = lax.broadcasted_iota(jnp.int32, (tok, LANES), 1)
    row_t = lax.broadcasted_iota(jnp.int32, (tok, LANES), 0)
    meta_rows = []
    for place in (cx, cy):
        eye = lane_t == row_t + core * tok + place * tok2
        for col in (id0, id1, p0 / psum, p1 / psum):
            meta_rows.append(jnp.sum(jnp.where(eye, col, 0.0), axis=0, keepdims=True))
    meta_own[0] = jnp.concatenate(meta_rows, axis=0)

    x_own = xbuf[my_rows, :]
    for name, w_ref, at in (('k', wk_v, 0), ('v', wv_v, half_kv)):
        loads[name].wait()
        out = jnp.dot(x_own, w_ref[...], preferred_element_type=F32).astype(BF16)
        for c in range(CORES):
            kv_own[c, :, at:at + half_kv] = out[:, c * half_kv:(c + 1) * half_kv]
    kvbuf[chip, my_rows, :] = kv_own[core]

    pl.semaphore_wait(barrier, len(partners))
    x_pair = remote(xbuf.at[my_rows, :], xbuf.at[my_rows, :], pair_send.at[0], pair_recv.at[0], sib)
    x_pair.start()
    m_pair = remote(meta_own.at[0], meta_own.at[1], pair_send.at[1], pair_recv.at[1], sib)
    m_pair.start()
    kv_pair = remote(kv_own.at[1 - core], kvbuf.at[chip, my_rows, :], pair_send.at[2], pair_recv.at[2], sib)
    kv_pair.start()

    def kv_first(d, c):
        y = (cy + d * c) % side
        x = (cx + d * (1 - c)) % side
        i = cx + (cy - cx) * c
        return remote(kv_own.at[c], kvbuf.at[chip, my_rows, :], kv_send.at[CORES * d + c],
                      kv_recv.at[CORES * i + core], {'sp': (y * side + x) * CORES + c})

    def kv_first_from(i, c):
        return remote(kv_own.at[c], kvbuf.at[chip_at(i, b0), pl.ds(c * tok, tok), :], kv_send.at[0],
                      kv_recv.at[CORES * i + c], sib)

    for d in (1, side - 1, 2):
        for c in range(CORES):
            kv_first(d, c).start()

    class Gather:
        def __init__(self, ref, ss, rs):
            self.ref, self.ss, self.rs = ref, ss, rs

        def copy(self, i, j, s, r, dev):
            return remote(self.ref(i, j), self.ref(i, j), self.ss.at[s], self.rs.at[r], dev)

        def first(self, d):
            return self.copy(a0, b0, d, a0, peer(chip_at((a0 + d) % side, b0)))

        def first_from(self, i):
            return self.copy(i, b0, 0, i, sib)

        def second(self, i, d):
            return self.copy(i, b0, side + i * side + d, side + i * side + b0, peer(chip_at(a0, (b0 + d) % side)))

        def relay(self, i, step):
            j = (b0 - step + side) % side
            return self.copy(i, j, side + i * side + 2, side + i * side + j,
                             peer(chip_at(a0, (b0 + step + side) % side)))

        def second_from(self, i, j):
            return self.copy(i, j, 0, side + i * side + j, sib)

        def open(self):
            for d in (2, 1, side - 1):
                self.first(d).start()
            self.spread(a0)

        def spread(self, i):
            for d in (2, 1, side - 1):
                self.second(i, d).start()

        def sent(self):
            for d in range(1, side):
                self.first(d).wait_send()
                for i in range(side):
                    self.second(i, d).wait_send()

    kvg = Gather(lambda i, j: kvbuf.at[chip_at(i, j)], kv2_send, kv2_recv)

    def kv_second(i, wait):
        slot = chip_at(i, b0)
        for d in (2, 1, side - 1):
            @pl.when(chip_at(a0, (b0 + d) % side) > slot)
            def _():
                c = kvg.second(i, d)
                if wait:
                    c.wait_send()
                else:
                    c.start()

    kv_pair.wait_recv()
    kv_second(a0, False)
    m_pair.wait_recv()
    meta_buf[chip] = meta_own[0] + meta_own[1]
    mt = Gather(lambda i, j: meta_buf.at[chip_at(i, j)], mt_send, mt_recv)
    mt.open()

    def project_q(chunks):
        for n in chunks:
            loads[('q', n)].wait()
            cols = slice(n * Q_COLS, (n + 1) * Q_COLS)
            q_s[:, cols] = jnp.dot(xbuf[...], wq_v[:, cols], preferred_element_type=F32).astype(BF16)

    x_pair.wait_recv()
    project_q(range(Q_EARLY))

    for d in (1, side - 1, 2):
        i = (a0 - d + side) % side
        for c in range(CORES):
            kv_first_from(i, c).wait_recv()
        kv_second(i, False)

    project_q(range(Q_EARLY, n_q))

    for d in (1, side - 1, 2):
        i = (a0 - d + side) % side
        mt.first_from(i).wait_recv()
        mt.spread(i)

    def kv_done(n, carry):
        i, j = n // side, n % side

        @pl.when((j != b0) & (chip_at(i, j) < chip))
        def _():
            kvg.second_from(i, j).wait_recv()
        return carry

    lax.fori_loop(0, n_chips, kv_done, 0)

    seq = n_chips * tok2
    q_pos = chip * tok2 + lax.broadcasted_iota(jnp.int32, (per_kv * tok2, seq), 0) % tok2
    k_pos = lax.broadcasted_iota(jnp.int32, (per_kv * tok2, seq), 1)
    causal = k_pos <= q_pos
    o_pairs = []
    for g in range(kv_half_heads):
        kc = slice(g * HEAD_DIM, (g + 1) * HEAD_DIM)
        vc = slice(half_kv + g * HEAD_DIM, half_kv + (g + 1) * HEAD_DIM)
        k_all = kvbuf[:, :, kc].reshape(seq, HEAD_DIM)
        v_all = kvbuf[:, :, vc].reshape(seq, HEAD_DIM)
        q_g = jnp.concatenate([q_s[:, (g * per_kv + h) * HEAD_DIM:(g * per_kv + h + 1) * HEAD_DIM]
                               for h in range(per_kv)], axis=0)
        s = lax.dot_general(q_g, k_all, (((1,), (1,)), ((), ())), preferred_element_type=F32) * SCORE_SCALE
        s = jnp.where(causal, s, -1e30)
        e = jnp.exp(s - jnp.max(s, axis=1, keepdims=True))
        w = (e / jnp.sum(e, axis=1, keepdims=True)).astype(BF16)
        o_g = jnp.dot(w, v_all, preferred_element_type=F32).astype(BF16)
        gw = per_kv * HEAD_DIM
        for h in range(per_kv):
            o_own[:, g * gw + h * HEAD_DIM:g * gw + (h + 1) * HEAD_DIM] = o_g[h * tok2:(h + 1) * tok2, :]
        cols = pl.ds(g * gw, gw)
        c = remote(o_own.at[:, cols], o_sib.at[:, cols], pair_send.at[3 + g], pair_recv.at[3 + g], sib)
        c.start()
        o_pairs.append(c)

    loads['o0'].wait()
    acc = jnp.dot(o_own[...], wo_v[0:half_q, :], preferred_element_type=F32)
    loads['o1'].wait()
    for c in o_pairs:
        c.wait_recv()
    acc = acc + jnp.dot(o_sib[...], wo_v[half_q:2 * half_q, :], preferred_element_type=F32)
    my_cols = pl.ds(pl.multiple_of(core * half_w, half_w), half_w)
    h_buf[core, b0 * side + a0] = (xbuf[:, my_cols].astype(F32) + acc).astype(BF16)

    hg = Gather(lambda i, j: h_buf.at[core, j * side + i], h_send, h_recv)

    def cross(i, j):
        at = h_buf.at[core, j * side + i]
        return remote(at, at, d_send.at[j * side + i], d_recv.at[j * side + i], sib)

    def cross_from(n):
        at = h_buf.at[1 - core, n]
        return remote(at, at, d_send.at[n], d_recv.at[n], sib)

    relays = {0: 1, 1: -1, side - 1: -1}

    def back(at, d):
        return (at - d + side) % side

    def h_spread(k):
        for d in (1, side - 1) if k in relays else (1, side - 1, 2):
            hg.second(back(a0, k), d).start()

    for d in (1, side - 1, 2):
        hg.first(d).start()
    h_spread(0)
    cross(a0, b0).start()

    def meta_done(n, carry):
        i, j = n // side, n % side

        @pl.when(j != b0)
        def _():
            mt.second_from(i, j).wait_recv()
        return carry

    lax.fori_loop(0, n_chips, meta_done, 0)

    g_tok = side * tok2
    t_row = lax.broadcasted_iota(jnp.int32, (g_tok, g_tok), 0)
    t_col = lax.broadcasted_iota(jnp.int32, (g_tok, g_tok), 1)
    before = jnp.where((t_row < t_col) & (t_row // tok == t_col // tok), 1.0, 0.0).astype(BF16)
    lane_8 = lax.broadcasted_iota(jnp.int32, (8, g_tok), 1)
    source_base = (lane_8 // tok * tok).astype(F32)
    expert_8 = (lax.broadcasted_iota(jnp.int32, (8, g_tok), 0) + me * own_experts).astype(F32)
    slot_row = t_row.astype(F32)

    def select_rows(g, carry):
        for half in range(CORES):
            m = jnp.zeros((8, g_tok), F32)
            for a in range(side):
                m = m + meta_buf[a * side + g if half else g * side + a]
            m = m[4 * half:4 * half + 4, :]
            hit0 = m[0:1, :] == expert_8
            hit1 = m[1:2, :] == expert_8
            hit = hit0 | hit1
            slot = jnp.dot(jnp.where(hit, 1.0, 0.0).astype(BF16), before, preferred_element_type=F32)
            row = jnp.where(hit, slot + source_base, -1.0)
            gate = jnp.where(hit0, m[2:3, :], jnp.where(hit1, m[3:4, :], 0.0))
            for k in range(own_experts):
                rows = pl.ds(k * g_tok, g_tok)
                pick = slot_row == row[k:k + 1, :]
                sel_s[half * side + g, rows, :] = jnp.where(pick, 1.0, 0.0).astype(BF16)
                gate_k = jnp.sum(jnp.where(pick, gate[k:k + 1, :], 0.0), axis=1, keepdims=True)
                gate_s[half * side + g, rows, :] = jnp.broadcast_to(gate_k, (g_tok, LANES))
        return carry

    lax.fori_loop(0, side, select_rows, 0)

    def build(half, g):
        def put(a, k, q, rows):
            cols = pl.ds(pl.multiple_of(half * half_w + q * B_COLS, B_COLS), B_COLS)
            buf_out[k, group_rows(side, tok2, half, g, a), cols] = rows

        build_group(side, tok2, own_experts, h_buf, sel_s, gate_s, half, g, put)

    def take_first(k):
        i = back(a0, k)
        hg.first_from(i).wait_recv()
        h_spread(k)
        cross(i, b0).start()

    def take(k, d):
        i, j = back(a0, k), back(b0, d)
        hg.second_from(i, j).wait_recv()
        if k in relays and d == (relays[k] + side) % side:
            hg.relay(i, relays[k]).start()
        cross(i, j).start()

    def other_done(d):
        for a in range(side):
            cross_from(back(a0, d) * side + a).wait_recv()

    def build_other(d):
        other_done(d)
        build(1 - core, back(a0, d))

    take_first(1)
    take_first(side - 1)
    take(0, 1)
    take_first(2)
    build(core, b0)
    build_other(0)
    take(1, side - 1)
    take(side - 1, side - 1)
    for k in (1, side - 1, 2):
        take(k, 1)
    take(0, side - 1)
    take(2, side - 1)
    for k in (0, 2):
        take(k, 2)
    build(core, back(b0, 1))
    build_other(1)
    build(core, back(b0, side - 1))
    for k in (1, side - 1):
        take(k, 2)
    for d in (side - 1, 2):
        other_done(d)

    for c in [x_pair, m_pair, kv_pair] + o_pairs:
        c.wait_send()
    for d in range(1, side):
        for c in range(CORES):
            kv_first(d, c).wait_send()
    for i in range(side):
        kv_second(i, True)
    mt.sent()
    hg.sent()
    for i in range(side):
        for j in range(side):
            cross(i, j).wait_send()


def store_kernel(side, buf_ref, h_ref, sel_ref, gate_ref, buf_out, h_out, stage, sem, stage_sem, h_sem):
    n_exp = buf_ref.shape[0]
    tok2, half_w = h_ref.shape[2:]
    tok = h_out.shape[0]
    me = lax.axis_index('sp')
    core = me % CORES
    chip = me // CORES
    cy = chip // side
    cx = chip % side
    a0 = cx + (cy - cx) * core
    b0 = cy + (cx - cy) * core
    copies = []

    def start(src, dst, s):
        copies.append(pltpu.make_async_copy(src, dst, s))
        copies[-1].start()

    def cols(half):
        return pl.ds(pl.multiple_of(half * half_w, half_w), half_w)

    other = 1 - core
    done = [(core, b0), (core, (b0 - 1 + side) % side), (core, (b0 + 1) % side), (other, a0), (other, (a0 - 1 + side) % side)]
    for n, (half, g) in enumerate(done):
        for a in range(side):
            rows = group_rows(side, tok2, half, g, a)
            start(buf_ref.at[:, rows, cols(half)], buf_out.at[:, rows, cols(half)], sem.at[n * side + a])
    my_rows = pl.ds(pl.multiple_of(core * tok, tok), tok)
    for c in range(CORES):
        start(h_ref.at[c, cx * side + cy if c else chip, my_rows, :], h_out.at[:, pl.ds(c * half_w, half_w)], h_sem.at[c])
    rest = [(core, (b0 + 2) % side), (other, (a0 + 1) % side), (other, (a0 + 2) % side)]
    for n, (half, g) in enumerate(rest):
        def put(a, k, q, rows, n=n):
            stage[n, k, a * tok2:(a + 1) * tok2, q * B_COLS:(q + 1) * B_COLS] = rows

        build_group(side, tok2, n_exp, h_ref, sel_ref, gate_ref, half, g, put)
        for a in range(side):
            start(stage.at[n, :, pl.ds(a * tok2, tok2), :], buf_out.at[:, group_rows(side, tok2, half, g, a), cols(half)],
                  stage_sem.at[n * side + a])
    for c in copies:
        c.wait()


def solution(mesh):
    group = mesh.shape['sp']
    side = math.isqrt(group // CORES)
    row_spec = P(('dp', 'sp'), None)
    buf_spec = P(('dp', 'sp'), None, None)
    any_spec = pl.BlockSpec(memory_space=pl.ANY)
    hbm_spec = pl.BlockSpec(memory_space=pltpu.HBM)
    vmem_spec = pl.BlockSpec(memory_space=pltpu.VMEM)

    def device_step(x_loc, w_q, w_k, w_v, w_o, ids_loc, probs_loc):
        tok, width = x_loc.shape
        experts = probs_loc.shape[1]
        own = experts // group
        chips = side * side
        tok2 = CORES * tok
        half_q = w_q.shape[1] // CORES
        half_kv = w_k.shape[1] // CORES
        half_w = width // CORES
        dma = pltpu.SemaphoreType.DMA
        n_loads = 7 + half_q // Q_COLS
        kv_half_heads = half_kv // HEAD_DIM
        g_tok = side * tok2
        parts = pl.pallas_call(
            functools.partial(block_kernel, side),
            out_shape=(pltpu.VMEM((own, tok * group, width), BF16),
                       pltpu.VMEM((CORES, chips, tok2, half_w), BF16),
                       pltpu.VMEM((CORES * side, own * g_tok, g_tok), BF16),
                       pltpu.VMEM((CORES * side, own * g_tok, LANES), F32)),
            in_specs=[hbm_spec] * 7,
            out_specs=(vmem_spec,) * 4,
            scratch_shapes=[
                pltpu.VMEM((tok2, width), BF16),
                pltpu.VMEM((width, half_q), BF16),
                pltpu.VMEM((width, CORES * half_kv), BF16),
                pltpu.VMEM((width, CORES * half_kv), BF16),
                pltpu.VMEM((2 * half_q, half_w), BF16),
                pltpu.VMEM((2, tok), jnp.int32),
                pltpu.VMEM((tok, experts), F32),
                pltpu.VMEM((CORES, tok, 2 * half_kv), BF16),
                pltpu.VMEM((chips, tok2, 2 * half_kv), BF16),
                pltpu.VMEM((CORES, 8, LANES), F32),
                pltpu.VMEM((chips, 8, LANES), F32),
                pltpu.VMEM((tok2, half_q), BF16),
                pltpu.VMEM((tok2, half_q), BF16),
                pltpu.VMEM((tok2, half_q), BF16),
                dma((n_loads,)),
                dma((3 + kv_half_heads,)), dma((3 + kv_half_heads,)),
                dma((CORES * side,)), dma((CORES * side,)),
                dma((side + chips,)), dma((side + chips,)), dma((side + chips,)), dma((side + chips,)),
                dma((side + chips,)), dma((side + chips,)),
                dma((chips,)), dma((chips,)),
            ],
            compiler_params=pltpu.CompilerParams(collective_id=0, has_side_effects=True,
                                                 vmem_limit_bytes=50 * 2 ** 20 + 900 * 1024),
            name='attention_block',
        )(x_loc, w_q, w_k, w_v, w_o, ids_loc.T, probs_loc)
        buf, h = pl.pallas_call(
            functools.partial(store_kernel, side),
            out_shape=(jax.ShapeDtypeStruct((own, tok * group, width), BF16), jax.ShapeDtypeStruct((tok, width), BF16)),
            in_specs=[vmem_spec] * 4,
            out_specs=(any_spec, any_spec),
            scratch_shapes=[pltpu.VMEM((3, own, g_tok, half_w), BF16),
                            dma((5 * side,)), dma((3 * side,)), dma((CORES,))],
            compiler_params=pltpu.CompilerParams(vmem_limit_bytes=16 * 2 ** 20),
            name='store_outputs',
        )(*parts)
        return h, buf

    return jax.shard_map(device_step, mesh=mesh, in_specs=(row_spec, P(), P(), P(), P(), row_spec, row_spec), out_specs=(row_spec, buf_spec), check_vma=False)
```

```python
import functools
import math

import jax
import jax.numpy as jnp
from jax import lax
from jax.experimental import pallas as pl
from jax.experimental.pallas import tpu as pltpu
from jax.sharding import PartitionSpec as P

HEAD_DIM = 128
SCORE_SCALE = 1.0 / math.sqrt(HEAD_DIM)
MESH_IDS = pl.DeviceIdType.MESH
LANES = 128
CORES = 2
Q_COLS = 512
Q_EARLY = 0
B_COLS = 256
F32 = jnp.float32
BF16 = jnp.bfloat16


def group_rows(side, tok2, half, g, a):
    slot = (g + (a - g) * half) * side + a + (g - a) * half
    return pl.ds(pl.multiple_of(slot * tok2, tok2), tok2)


def build_group(side, tok2, n_exp, h_ref, sel_ref, gate_ref, half, g, put):
    g_tok = side * tok2
    n = half * side + g
    for q in range(h_ref.shape[3] // B_COLS):
        h_g = h_ref[half, pl.ds(g * side, side), :, q * B_COLS:(q + 1) * B_COLS].reshape(g_tok, B_COLS)
        rows = jnp.dot(sel_ref[n], h_g, preferred_element_type=F32)
        gate = gate_ref[n]
        rows = jnp.concatenate([rows[:, i * LANES:(i + 1) * LANES] * gate for i in range(B_COLS // LANES)], axis=1)
        rows = rows.astype(BF16)
        for a in range(side):
            for k in range(n_exp):
                put(a, k, q, rows[k * g_tok + a * tok2:k * g_tok + (a + 1) * tok2, :])


def block_kernel(side, x_hbm, wq_hbm, wk_hbm, wv_hbm, wo_hbm, ids_hbm, probs_hbm,
                 buf_out, h_buf, sel_s, gate_s,
                 xbuf, wq_v, wk_v, wv_v, wo_v, ids_v, probs_v, kv_own, kvbuf, meta_own, meta_buf, q_s, o_own, o_sib,
                 wsem, pair_send, pair_recv, kv_send, kv_recv, kv2_send, kv2_recv, mt_send, mt_recv, h_send, h_recv,
                 d_send, d_recv):
    tok = x_hbm.shape[0]
    tok2 = CORES * tok
    half_q = wq_v.shape[1]
    half_kv = wk_v.shape[1] // CORES
    half_w = wo_v.shape[1]
    kv_half_heads = half_kv // HEAD_DIM
    q_half_heads = half_q // HEAD_DIM
    per_kv = q_half_heads // kv_half_heads
    own_experts = buf_out.shape[0]
    experts = probs_v.shape[1]
    n_chips = side * side

    me = lax.axis_index('sp')
    core = me % CORES
    chip = me // CORES
    cy = chip // side
    cx = chip % side
    a0 = cx + (cy - cx) * core
    b0 = cy + (cx - cy) * core

    def chip_at(a, b):
        y = b + (a - b) * core
        x = a + (b - a) * core
        return y * side + x

    def peer(c):
        return {'sp': c * CORES + core}

    sib = {'sp': chip * CORES + (1 - core)}

    def remote(src, dst, ss, rs, dev):
        return pltpu.make_async_remote_copy(src_ref=src, dst_ref=dst, send_sem=ss, recv_sem=rs,
                                            device_id=dev, device_id_type=MESH_IDS)

    my_rows = pl.ds(pl.multiple_of(core * tok, tok), tok)
    loads = {}

    def load(name, src, dst):
        loads[name] = pltpu.make_async_copy(src, dst, wsem.at[len(loads)])
        loads[name].start()

    load('x', x_hbm, xbuf.at[my_rows, :])
    load('ids', ids_hbm, ids_v)
    load('probs', probs_hbm, probs_v)
    load('k', wk_hbm, wk_v)
    load('v', wv_hbm, wv_v)
    barrier = pltpu.get_barrier_semaphore()
    partners = [sib]
    for d in range(1, side):
        for c in range(CORES):
            partners.append({'sp': (cy * side + (cx + d) % side) * CORES + c})
            partners.append({'sp': ((cy + d) % side * side + cx) * CORES + c})
    for p in partners:
        pl.semaphore_signal(barrier, inc=1, device_id=p, device_id_type=MESH_IDS)

    n_q = half_q // Q_COLS
    for i in range(n_q):
        load(('q', i), wq_hbm.at[:, pl.ds(pl.multiple_of(core * half_q + i * Q_COLS, Q_COLS), Q_COLS)],
             wq_v.at[:, pl.ds(i * Q_COLS, Q_COLS)])
    o_cols = pl.ds(pl.multiple_of(core * half_w, half_w), half_w)
    load('o0', wo_hbm.at[pl.ds(pl.multiple_of(core * half_q, half_q), half_q), o_cols], wo_v.at[pl.ds(0, half_q), :])
    load('o1', wo_hbm.at[pl.ds(pl.multiple_of((1 - core) * half_q, half_q), half_q), o_cols],
         wo_v.at[pl.ds(half_q, half_q), :])

    for slot in range(n_chips):
        y, x = slot // side, slot % side

        @pl.when((slot > chip) & (y + (x - y) * core != b0))
        def _():
            kvbuf[slot] = jnp.zeros(kvbuf.shape[1:], BF16)

    loads['x'].wait()
    loads['ids'].wait()
    loads['probs'].wait()
    idf = ids_v[...].astype(F32)
    probs = probs_v[...]
    lane_e = lax.broadcasted_iota(jnp.int32, (tok, experts), 1).astype(F32)
    eye_t = lax.broadcasted_iota(jnp.int32, (tok, tok), 0) == lax.broadcasted_iota(jnp.int32, (tok, tok), 1)
    id0 = jnp.sum(jnp.where(eye_t, idf[0:1, :], 0.0), axis=1, keepdims=True)
    id1 = jnp.sum(jnp.where(eye_t, idf[1:2, :], 0.0), axis=1, keepdims=True)
    p0 = jnp.sum(jnp.where(lane_e == id0, probs, 0.0), axis=1, keepdims=True)
    p1 = jnp.sum(jnp.where(lane_e == id1, probs, 0.0), axis=1, keepdims=True)
    psum = p0 + p1
    lane_t = lax.broadcasted_iota(jnp.int32, (tok, LANES), 1)
    row_t = lax.broadcasted_iota(jnp.int32, (tok, LANES), 0)
    meta_rows = []
    for place in (cx, cy):
        eye = lane_t == row_t + core * tok + place * tok2
        for col in (id0, id1, p0 / psum, p1 / psum):
            meta_rows.append(jnp.sum(jnp.where(eye, col, 0.0), axis=0, keepdims=True))
    meta_own[0] = jnp.concatenate(meta_rows, axis=0)

    x_own = xbuf[my_rows, :]
    for name, w_ref, at in (('k', wk_v, 0), ('v', wv_v, half_kv)):
        loads[name].wait()
        out = jnp.dot(x_own, w_ref[...], preferred_element_type=F32).astype(BF16)
        for c in range(CORES):
            kv_own[c, :, at:at + half_kv] = out[:, c * half_kv:(c + 1) * half_kv]
    kvbuf[chip, my_rows, :] = kv_own[core]

    pl.semaphore_wait(barrier, len(partners))
    x_pair = remote(xbuf.at[my_rows, :], xbuf.at[my_rows, :], pair_send.at[0], pair_recv.at[0], sib)
    x_pair.start()
    m_pair = remote(meta_own.at[0], meta_own.at[1], pair_send.at[1], pair_recv.at[1], sib)
    m_pair.start()
    kv_pair = remote(kv_own.at[1 - core], kvbuf.at[chip, my_rows, :], pair_send.at[2], pair_recv.at[2], sib)
    kv_pair.start()

    def kv_first(d, c):
        y = (cy + d * c) % side
        x = (cx + d * (1 - c)) % side
        i = cx + (cy - cx) * c
        return remote(kv_own.at[c], kvbuf.at[chip, my_rows, :], kv_send.at[CORES * d + c],
                      kv_recv.at[CORES * i + core], {'sp': (y * side + x) * CORES + c})

    def kv_first_from(i, c):
        return remote(kv_own.at[c], kvbuf.at[chip_at(i, b0), pl.ds(c * tok, tok), :], kv_send.at[0],
                      kv_recv.at[CORES * i + c], sib)

    for d in (1, side - 1, 2):
        for c in range(CORES):
            kv_first(d, c).start()

    class Gather:
        def __init__(self, ref, ss, rs):
            self.ref, self.ss, self.rs = ref, ss, rs

        def copy(self, i, j, s, r, dev):
            return remote(self.ref(i, j), self.ref(i, j), self.ss.at[s], self.rs.at[r], dev)

        def first(self, d):
            return self.copy(a0, b0, d, a0, peer(chip_at((a0 + d) % side, b0)))

        def first_from(self, i):
            return self.copy(i, b0, 0, i, sib)

        def second(self, i, d):
            return self.copy(i, b0, side + i * side + d, side + i * side + b0, peer(chip_at(a0, (b0 + d) % side)))

        def relay(self, i, step):
            j = (b0 - step + side) % side
            return self.copy(i, j, side + i * side + 2, side + i * side + j,
                             peer(chip_at(a0, (b0 + step + side) % side)))

        def second_from(self, i, j):
            return self.copy(i, j, 0, side + i * side + j, sib)

        def open(self):
            for d in (2, 1, side - 1):
                self.first(d).start()
            self.spread(a0)

        def spread(self, i):
            for d in (2, 1, side - 1):
                self.second(i, d).start()

        def sent(self):
            for d in range(1, side):
                self.first(d).wait_send()
                for i in range(side):
                    self.second(i, d).wait_send()

    kvg = Gather(lambda i, j: kvbuf.at[chip_at(i, j)], kv2_send, kv2_recv)

    def kv_second(i, wait):
        slot = chip_at(i, b0)
        for d in (2, 1, side - 1):
            @pl.when(chip_at(a0, (b0 + d) % side) > slot)
            def _():
                c = kvg.second(i, d)
                if wait:
                    c.wait_send()
                else:
                    c.start()

    kv_pair.wait_recv()
    kv_second(a0, False)
    m_pair.wait_recv()
    meta_buf[chip] = meta_own[0] + meta_own[1]
    mt = Gather(lambda i, j: meta_buf.at[chip_at(i, j)], mt_send, mt_recv)
    mt.open()

    def project_q(chunks):
        for n in chunks:
            loads[('q', n)].wait()
            cols = slice(n * Q_COLS, (n + 1) * Q_COLS)
            q_s[:, cols] = jnp.dot(xbuf[...], wq_v[:, cols], preferred_element_type=F32).astype(BF16)

    x_pair.wait_recv()
    project_q(range(Q_EARLY))

    for d in (1, side - 1, 2):
        i = (a0 - d + side) % side
        for c in range(CORES):
            kv_first_from(i, c).wait_recv()
        kv_second(i, False)

    project_q(range(Q_EARLY, n_q))

    for d in (1, side - 1, 2):
        i = (a0 - d + side) % side
        mt.first_from(i).wait_recv()
        mt.spread(i)

    def kv_done(n, carry):
        i, j = n // side, n % side

        @pl.when((j != b0) & (chip_at(i, j) < chip))
        def _():
            kvg.second_from(i, j).wait_recv()
        return carry

    lax.fori_loop(0, n_chips, kv_done, 0)

    seq = n_chips * tok2
    q_pos = chip * tok2 + lax.broadcasted_iota(jnp.int32, (per_kv * tok2, seq), 0) % tok2
    k_pos = lax.broadcasted_iota(jnp.int32, (per_kv * tok2, seq), 1)
    causal = k_pos <= q_pos
    o_pairs = []
    for g in range(kv_half_heads):
        kc = slice(g * HEAD_DIM, (g + 1) * HEAD_DIM)
        vc = slice(half_kv + g * HEAD_DIM, half_kv + (g + 1) * HEAD_DIM)
        k_all = kvbuf[:, :, kc].reshape(seq, HEAD_DIM)
        v_all = kvbuf[:, :, vc].reshape(seq, HEAD_DIM)
        q_g = jnp.concatenate([q_s[:, (g * per_kv + h) * HEAD_DIM:(g * per_kv + h + 1) * HEAD_DIM]
                               for h in range(per_kv)], axis=0)
        s = lax.dot_general(q_g, k_all, (((1,), (1,)), ((), ())), preferred_element_type=F32) * SCORE_SCALE
        s = jnp.where(causal, s, -1e30)
        e = jnp.exp(s - jnp.max(s, axis=1, keepdims=True))
        w = (e / jnp.sum(e, axis=1, keepdims=True)).astype(BF16)
        o_g = jnp.dot(w, v_all, preferred_element_type=F32).astype(BF16)
        gw = per_kv * HEAD_DIM
        for h in range(per_kv):
            o_own[:, g * gw + h * HEAD_DIM:g * gw + (h + 1) * HEAD_DIM] = o_g[h * tok2:(h + 1) * tok2, :]
        cols = pl.ds(g * gw, gw)
        c = remote(o_own.at[:, cols], o_sib.at[:, cols], pair_send.at[3 + g], pair_recv.at[3 + g], sib)
        c.start()
        o_pairs.append(c)

    loads['o0'].wait()
    acc = jnp.dot(o_own[...], wo_v[0:half_q, :], preferred_element_type=F32)
    loads['o1'].wait()
    for c in o_pairs:
        c.wait_recv()
    acc = acc + jnp.dot(o_sib[...], wo_v[half_q:2 * half_q, :], preferred_element_type=F32)
    my_cols = pl.ds(pl.multiple_of(core * half_w, half_w), half_w)
    h_buf[core, b0 * side + a0] = (xbuf[:, my_cols].astype(F32) + acc).astype(BF16)

    hg = Gather(lambda i, j: h_buf.at[core, j * side + i], h_send, h_recv)

    def cross(i, j):
        at = h_buf.at[core, j * side + i]
        return remote(at, at, d_send.at[j * side + i], d_recv.at[j * side + i], sib)

    def cross_from(n):
        at = h_buf.at[1 - core, n]
        return remote(at, at, d_send.at[n], d_recv.at[n], sib)

    relays = {0: 1, 1: -1, side - 1: -1}

    def back(at, d):
        return (at - d + side) % side

    def h_spread(k):
        for d in (1, side - 1) if k in relays else (1, side - 1, 2):
            hg.second(back(a0, k), d).start()

    for d in (1, side - 1, 2):
        hg.first(d).start()
    h_spread(0)
    cross(a0, b0).start()

    def meta_done(n, carry):
        i, j = n // side, n % side

        @pl.when(j != b0)
        def _():
            mt.second_from(i, j).wait_recv()
        return carry

    lax.fori_loop(0, n_chips, meta_done, 0)

    g_tok = side * tok2
    t_row = lax.broadcasted_iota(jnp.int32, (g_tok, g_tok), 0)
    t_col = lax.broadcasted_iota(jnp.int32, (g_tok, g_tok), 1)
    before = jnp.where((t_row < t_col) & (t_row // tok == t_col // tok), 1.0, 0.0).astype(BF16)
    lane_8 = lax.broadcasted_iota(jnp.int32, (8, g_tok), 1)
    source_base = (lane_8 // tok * tok).astype(F32)
    expert_8 = (lax.broadcasted_iota(jnp.int32, (8, g_tok), 0) + me * own_experts).astype(F32)
    slot_row = t_row.astype(F32)

    def select_rows(g, carry):
        for half in range(CORES):
            m = jnp.zeros((8, g_tok), F32)
            for a in range(side):
                m = m + meta_buf[a * side + g if half else g * side + a]
            m = m[4 * half:4 * half + 4, :]
            hit0 = m[0:1, :] == expert_8
            hit1 = m[1:2, :] == expert_8
            hit = hit0 | hit1
            slot = jnp.dot(jnp.where(hit, 1.0, 0.0).astype(BF16), before, preferred_element_type=F32)
            row = jnp.where(hit, slot + source_base, -1.0)
            gate = jnp.where(hit0, m[2:3, :], jnp.where(hit1, m[3:4, :], 0.0))
            for k in range(own_experts):
                rows = pl.ds(k * g_tok, g_tok)
                pick = slot_row == row[k:k + 1, :]
                sel_s[half * side + g, rows, :] = jnp.where(pick, 1.0, 0.0).astype(BF16)
                gate_k = jnp.sum(jnp.where(pick, gate[k:k + 1, :], 0.0), axis=1, keepdims=True)
                gate_s[half * side + g, rows, :] = jnp.broadcast_to(gate_k, (g_tok, LANES))
        return carry

    lax.fori_loop(0, side, select_rows, 0)

    def build(half, g):
        def put(a, k, q, rows):
            cols = pl.ds(pl.multiple_of(half * half_w + q * B_COLS, B_COLS), B_COLS)
            buf_out[k, group_rows(side, tok2, half, g, a), cols] = rows

        build_group(side, tok2, own_experts, h_buf, sel_s, gate_s, half, g, put)

    def take_first(k):
        i = back(a0, k)
        hg.first_from(i).wait_recv()
        h_spread(k)
        cross(i, b0).start()

    def take(k, d):
        i, j = back(a0, k), back(b0, d)
        hg.second_from(i, j).wait_recv()
        if k in relays and d == (relays[k] + side) % side:
            hg.relay(i, relays[k]).start()
        cross(i, j).start()

    def other_done(d):
        for a in range(side):
            cross_from(back(a0, d) * side + a).wait_recv()

    def build_other(d):
        other_done(d)
        build(1 - core, back(a0, d))

    take_first(1)
    take_first(side - 1)
    take(0, 1)
    take_first(2)
    build(core, b0)
    build_other(0)
    take(1, side - 1)
    take(side - 1, side - 1)
    for k in (1, side - 1, 2):
        take(k, 1)
    take(0, side - 1)
    take(2, side - 1)
    for k in (0, 2):
        take(k, 2)
    build(core, back(b0, 1))
    for k in (1, side - 1):
        take(k, 2)
    for d in (1, side - 1, 2):
        other_done(d)

    for c in [x_pair, m_pair, kv_pair] + o_pairs:
        c.wait_send()
    for d in range(1, side):
        for c in range(CORES):
            kv_first(d, c).wait_send()
    for i in range(side):
        kv_second(i, True)
    mt.sent()
    hg.sent()
    for i in range(side):
        for j in range(side):
            cross(i, j).wait_send()


def store_kernel(side, buf_ref, h_ref, sel_ref, gate_ref, buf_out, h_out, stage, sem, stage_sem, h_sem):
    n_exp = buf_ref.shape[0]
    tok2, half_w = h_ref.shape[2:]
    tok = h_out.shape[0]
    me = lax.axis_index('sp')
    core = me % CORES
    chip = me // CORES
    cy = chip // side
    cx = chip % side
    a0 = cx + (cy - cx) * core
    b0 = cy + (cx - cy) * core
    copies = []

    def start(src, dst, s):
        copies.append(pltpu.make_async_copy(src, dst, s))
        copies[-1].start()

    def cols(half):
        return pl.ds(pl.multiple_of(half * half_w, half_w), half_w)

    other = 1 - core
    done = [(core, b0), (core, (b0 - 1 + side) % side), (other, a0)]
    for n, (half, g) in enumerate(done):
        for a in range(side):
            rows = group_rows(side, tok2, half, g, a)
            start(buf_ref.at[:, rows, cols(half)], buf_out.at[:, rows, cols(half)], sem.at[n * side + a])
    my_rows = pl.ds(pl.multiple_of(core * tok, tok), tok)
    for c in range(CORES):
        start(h_ref.at[c, cx * side + cy if c else chip, my_rows, :], h_out.at[:, pl.ds(c * half_w, half_w)], h_sem.at[c])
    rest = [(other, (a0 - 1 + side) % side), (core, (b0 + 1) % side), (core, (b0 + 2) % side), (other, (a0 + 1) % side), (other, (a0 + 2) % side)]
    for n, (half, g) in enumerate(rest):
        def put(a, k, q, rows, n=n):
            stage[n, k, a * tok2:(a + 1) * tok2, q * B_COLS:(q + 1) * B_COLS] = rows

        build_group(side, tok2, n_exp, h_ref, sel_ref, gate_ref, half, g, put)
        for a in range(side):
            start(stage.at[n, :, pl.ds(a * tok2, tok2), :], buf_out.at[:, group_rows(side, tok2, half, g, a), cols(half)],
                  stage_sem.at[n * side + a])
    for c in copies:
        c.wait()


def solution(mesh):
    group = mesh.shape['sp']
    side = math.isqrt(group // CORES)
    row_spec = P(('dp', 'sp'), None)
    buf_spec = P(('dp', 'sp'), None, None)
    any_spec = pl.BlockSpec(memory_space=pl.ANY)
    hbm_spec = pl.BlockSpec(memory_space=pltpu.HBM)
    vmem_spec = pl.BlockSpec(memory_space=pltpu.VMEM)

    def device_step(x_loc, w_q, w_k, w_v, w_o, ids_loc, probs_loc):
        tok, width = x_loc.shape
        experts = probs_loc.shape[1]
        own = experts // group
        chips = side * side
        tok2 = CORES * tok
        half_q = w_q.shape[1] // CORES
        half_kv = w_k.shape[1] // CORES
        half_w = width // CORES
        dma = pltpu.SemaphoreType.DMA
        n_loads = 7 + half_q // Q_COLS
        kv_half_heads = half_kv // HEAD_DIM
        g_tok = side * tok2
        parts = pl.pallas_call(
            functools.partial(block_kernel, side),
            out_shape=(pltpu.VMEM((own, tok * group, width), BF16),
                       pltpu.VMEM((CORES, chips, tok2, half_w), BF16),
                       pltpu.VMEM((CORES * side, own * g_tok, g_tok), BF16),
                       pltpu.VMEM((CORES * side, own * g_tok, LANES), F32)),
            in_specs=[hbm_spec] * 7,
            out_specs=(vmem_spec,) * 4,
            scratch_shapes=[
                pltpu.VMEM((tok2, width), BF16),
                pltpu.VMEM((width, half_q), BF16),
                pltpu.VMEM((width, CORES * half_kv), BF16),
                pltpu.VMEM((width, CORES * half_kv), BF16),
                pltpu.VMEM((2 * half_q, half_w), BF16),
                pltpu.VMEM((2, tok), jnp.int32),
                pltpu.VMEM((tok, experts), F32),
                pltpu.VMEM((CORES, tok, 2 * half_kv), BF16),
                pltpu.VMEM((chips, tok2, 2 * half_kv), BF16),
                pltpu.VMEM((CORES, 8, LANES), F32),
                pltpu.VMEM((chips, 8, LANES), F32),
                pltpu.VMEM((tok2, half_q), BF16),
                pltpu.VMEM((tok2, half_q), BF16),
                pltpu.VMEM((tok2, half_q), BF16),
                dma((n_loads,)),
                dma((3 + kv_half_heads,)), dma((3 + kv_half_heads,)),
                dma((CORES * side,)), dma((CORES * side,)),
                dma((side + chips,)), dma((side + chips,)), dma((side + chips,)), dma((side + chips,)),
                dma((side + chips,)), dma((side + chips,)),
                dma((chips,)), dma((chips,)),
            ],
            compiler_params=pltpu.CompilerParams(collective_id=0, has_side_effects=True,
                                                 vmem_limit_bytes=50 * 2 ** 20 + 900 * 1024),
            name='attention_block',
        )(x_loc, w_q, w_k, w_v, w_o, ids_loc.T, probs_loc)
        buf, h = pl.pallas_call(
            functools.partial(store_kernel, side),
            out_shape=(jax.ShapeDtypeStruct((own, tok * group, width), BF16), jax.ShapeDtypeStruct((tok, width), BF16)),
            in_specs=[vmem_spec] * 4,
            out_specs=(any_spec, any_spec),
            scratch_shapes=[pltpu.VMEM((5, own, g_tok, half_w), BF16),
                            dma((3 * side,)), dma((5 * side,)), dma((CORES,))],
            compiler_params=pltpu.CompilerParams(vmem_limit_bytes=16 * 2 ** 20),
            name='store_outputs',
        )(*parts)
        return h, buf

    return jax.shard_map(device_step, mesh=mesh, in_specs=(row_spec, P(), P(), P(), P(), row_spec, row_spec), out_specs=(row_spec, buf_spec), check_vma=False)
```

```python
import functools
import math

import jax
import jax.numpy as jnp
from jax import lax
from jax.experimental import pallas as pl
from jax.experimental.pallas import tpu as pltpu
from jax.sharding import PartitionSpec as P

HEAD_DIM = 128
SCORE_SCALE = 1.0 / math.sqrt(HEAD_DIM)
MESH_IDS = pl.DeviceIdType.MESH
LANES = 128
CORES = 2
Q_COLS = 512
Q_EARLY = 0
B_COLS = 256
F32 = jnp.float32
BF16 = jnp.bfloat16


def group_rows(side, tok2, half, g, a):
    slot = (g + (a - g) * half) * side + a + (g - a) * half
    return pl.ds(pl.multiple_of(slot * tok2, tok2), tok2)


def build_group(side, tok2, n_exp, h_ref, sel_ref, gate_ref, half, g, put):
    g_tok = side * tok2
    n = half * side + g
    for q in range(h_ref.shape[3] // B_COLS):
        h_g = h_ref[half, pl.ds(g * side, side), :, q * B_COLS:(q + 1) * B_COLS].reshape(g_tok, B_COLS)
        rows = jnp.dot(sel_ref[n], h_g, preferred_element_type=F32)
        gate = gate_ref[n]
        rows = jnp.concatenate([rows[:, i * LANES:(i + 1) * LANES] * gate for i in range(B_COLS // LANES)], axis=1)
        rows = rows.astype(BF16)
        for a in range(side):
            for k in range(n_exp):
                put(a, k, q, rows[k * g_tok + a * tok2:k * g_tok + (a + 1) * tok2, :])


def block_kernel(side, x_hbm, wq_hbm, wk_hbm, wv_hbm, wo_hbm, ids_hbm, probs_hbm,
                 buf_out, h_buf, sel_s, gate_s,
                 xbuf, wq_v, wk_v, wv_v, wo_v, ids_v, probs_v, kv_own, kvbuf, meta_own, meta_buf, q_s, o_own, o_sib,
                 wsem, pair_send, pair_recv, kv_send, kv_recv, kv2_send, kv2_recv, mt_send, mt_recv, h_send, h_recv,
                 d_send, d_recv):
    tok = x_hbm.shape[0]
    tok2 = CORES * tok
    half_q = wq_v.shape[1]
    half_kv = wk_v.shape[1] // CORES
    half_w = wo_v.shape[1]
    kv_half_heads = half_kv // HEAD_DIM
    q_half_heads = half_q // HEAD_DIM
    per_kv = q_half_heads // kv_half_heads
    own_experts = buf_out.shape[0]
    experts = probs_v.shape[1]
    n_chips = side * side

    me = lax.axis_index('sp')
    core = me % CORES
    chip = me // CORES
    cy = chip // side
    cx = chip % side
    a0 = cx + (cy - cx) * core
    b0 = cy + (cx - cy) * core

    def chip_at(a, b):
        y = b + (a - b) * core
        x = a + (b - a) * core
        return y * side + x

    def peer(c):
        return {'sp': c * CORES + core}

    sib = {'sp': chip * CORES + (1 - core)}

    def remote(src, dst, ss, rs, dev):
        return pltpu.make_async_remote_copy(src_ref=src, dst_ref=dst, send_sem=ss, recv_sem=rs,
                                            device_id=dev, device_id_type=MESH_IDS)

    my_rows = pl.ds(pl.multiple_of(core * tok, tok), tok)
    loads = {}

    def load(name, src, dst):
        loads[name] = pltpu.make_async_copy(src, dst, wsem.at[len(loads)])
        loads[name].start()

    load('x', x_hbm, xbuf.at[my_rows, :])
    load('ids', ids_hbm, ids_v)
    load('probs', probs_hbm, probs_v)
    load('k', wk_hbm, wk_v)
    load('v', wv_hbm, wv_v)
    barrier = pltpu.get_barrier_semaphore()
    partners = [sib]
    for d in range(1, side):
        for c in range(CORES):
            partners.append({'sp': (cy * side + (cx + d) % side) * CORES + c})
            partners.append({'sp': ((cy + d) % side * side + cx) * CORES + c})
    for p in partners:
        pl.semaphore_signal(barrier, inc=1, device_id=p, device_id_type=MESH_IDS)

    n_q = half_q // Q_COLS
    for i in range(n_q):
        load(('q', i), wq_hbm.at[:, pl.ds(pl.multiple_of(core * half_q + i * Q_COLS, Q_COLS), Q_COLS)],
             wq_v.at[:, pl.ds(i * Q_COLS, Q_COLS)])
    o_cols = pl.ds(pl.multiple_of(core * half_w, half_w), half_w)
    load('o0', wo_hbm.at[pl.ds(pl.multiple_of(core * half_q, half_q), half_q), o_cols], wo_v.at[pl.ds(0, half_q), :])
    load('o1', wo_hbm.at[pl.ds(pl.multiple_of((1 - core) * half_q, half_q), half_q), o_cols],
         wo_v.at[pl.ds(half_q, half_q), :])

    for slot in range(n_chips):
        y, x = slot // side, slot % side

        @pl.when((slot > chip) & (y + (x - y) * core != b0))
        def _():
            kvbuf[slot] = jnp.zeros(kvbuf.shape[1:], BF16)

    loads['x'].wait()
    loads['ids'].wait()
    loads['probs'].wait()
    idf = ids_v[...].astype(F32)
    probs = probs_v[...]
    lane_e = lax.broadcasted_iota(jnp.int32, (tok, experts), 1).astype(F32)
    eye_t = lax.broadcasted_iota(jnp.int32, (tok, tok), 0) == lax.broadcasted_iota(jnp.int32, (tok, tok), 1)
    id0 = jnp.sum(jnp.where(eye_t, idf[0:1, :], 0.0), axis=1, keepdims=True)
    id1 = jnp.sum(jnp.where(eye_t, idf[1:2, :], 0.0), axis=1, keepdims=True)
    p0 = jnp.sum(jnp.where(lane_e == id0, probs, 0.0), axis=1, keepdims=True)
    p1 = jnp.sum(jnp.where(lane_e == id1, probs, 0.0), axis=1, keepdims=True)
    psum = p0 + p1
    lane_t = lax.broadcasted_iota(jnp.int32, (tok, LANES), 1)
    row_t = lax.broadcasted_iota(jnp.int32, (tok, LANES), 0)
    meta_rows = []
    for place in (cx, cy):
        eye = lane_t == row_t + core * tok + place * tok2
        for col in (id0, id1, p0 / psum, p1 / psum):
            meta_rows.append(jnp.sum(jnp.where(eye, col, 0.0), axis=0, keepdims=True))
    meta_own[0] = jnp.concatenate(meta_rows, axis=0)

    x_own = xbuf[my_rows, :]
    for name, w_ref, at in (('k', wk_v, 0), ('v', wv_v, half_kv)):
        loads[name].wait()
        out = jnp.dot(x_own, w_ref[...], preferred_element_type=F32).astype(BF16)
        for c in range(CORES):
            kv_own[c, :, at:at + half_kv] = out[:, c * half_kv:(c + 1) * half_kv]
    kvbuf[chip, my_rows, :] = kv_own[core]

    pl.semaphore_wait(barrier, len(partners))
    def kv_first(d, c):
        y = (cy + d * c) % side
        x = (cx + d * (1 - c)) % side
        i = cx + (cy - cx) * c
        return remote(kv_own.at[c], kvbuf.at[chip, my_rows, :], kv_send.at[CORES * d + c],
                      kv_recv.at[CORES * i + core], {'sp': (y * side + x) * CORES + c})

    def kv_first_from(i, c):
        return remote(kv_own.at[c], kvbuf.at[chip_at(i, b0), pl.ds(c * tok, tok), :], kv_send.at[0],
                      kv_recv.at[CORES * i + c], sib)

    for d in (1, side - 1, 2):
        for c in range(CORES):
            kv_first(d, c).start()

    x_pair = remote(xbuf.at[my_rows, :], xbuf.at[my_rows, :], pair_send.at[0], pair_recv.at[0], sib)
    x_pair.start()
    m_pair = remote(meta_own.at[0], meta_own.at[1], pair_send.at[1], pair_recv.at[1], sib)
    m_pair.start()
    kv_pair = remote(kv_own.at[1 - core], kvbuf.at[chip, my_rows, :], pair_send.at[2], pair_recv.at[2], sib)
    kv_pair.start()

    class Gather:
        def __init__(self, ref, ss, rs):
            self.ref, self.ss, self.rs = ref, ss, rs

        def copy(self, i, j, s, r, dev):
            return remote(self.ref(i, j), self.ref(i, j), self.ss.at[s], self.rs.at[r], dev)

        def first(self, d):
            return self.copy(a0, b0, d, a0, peer(chip_at((a0 + d) % side, b0)))

        def first_from(self, i):
            return self.copy(i, b0, 0, i, sib)

        def second(self, i, d):
            return self.copy(i, b0, side + i * side + d, side + i * side + b0, peer(chip_at(a0, (b0 + d) % side)))

        def relay(self, i, step):
            j = (b0 - step + side) % side
            return self.copy(i, j, side + i * side + 2, side + i * side + j,
                             peer(chip_at(a0, (b0 + step + side) % side)))

        def second_from(self, i, j):
            return self.copy(i, j, 0, side + i * side + j, sib)

        def open(self):
            for d in (2, 1, side - 1):
                self.first(d).start()
            self.spread(a0)

        def spread(self, i):
            for d in (2, 1, side - 1):
                self.second(i, d).start()

        def sent(self):
            for d in range(1, side):
                self.first(d).wait_send()
                for i in range(side):
                    self.second(i, d).wait_send()

    kvg = Gather(lambda i, j: kvbuf.at[chip_at(i, j)], kv2_send, kv2_recv)

    def kv_second(i, wait):
        slot = chip_at(i, b0)
        for d in (2, 1, side - 1):
            @pl.when(chip_at(a0, (b0 + d) % side) > slot)
            def _():
                c = kvg.second(i, d)
                if wait:
                    c.wait_send()
                else:
                    c.start()

    kv_pair.wait_recv()
    kv_second(a0, False)
    m_pair.wait_recv()
    meta_buf[chip] = meta_own[0] + meta_own[1]
    mt = Gather(lambda i, j: meta_buf.at[chip_at(i, j)], mt_send, mt_recv)
    mt.open()

    def project_q(chunks):
        for n in chunks:
            loads[('q', n)].wait()
            cols = slice(n * Q_COLS, (n + 1) * Q_COLS)
            q_s[:, cols] = jnp.dot(xbuf[...], wq_v[:, cols], preferred_element_type=F32).astype(BF16)

    x_pair.wait_recv()
    project_q(range(Q_EARLY))

    for d in (1, side - 1, 2):
        i = (a0 - d + side) % side
        for c in range(CORES):
            kv_first_from(i, c).wait_recv()
        kv_second(i, False)

    project_q(range(Q_EARLY, n_q))

    for d in (1, side - 1, 2):
        i = (a0 - d + side) % side
        mt.first_from(i).wait_recv()
        mt.spread(i)

    def kv_done(n, carry):
        i, j = n // side, n % side

        @pl.when((j != b0) & (chip_at(i, j) < chip))
        def _():
            kvg.second_from(i, j).wait_recv()
        return carry

    lax.fori_loop(0, n_chips, kv_done, 0)

    seq = n_chips * tok2
    q_pos = chip * tok2 + lax.broadcasted_iota(jnp.int32, (per_kv * tok2, seq), 0) % tok2
    k_pos = lax.broadcasted_iota(jnp.int32, (per_kv * tok2, seq), 1)
    causal = k_pos <= q_pos
    o_pairs = []
    for g in range(kv_half_heads):
        kc = slice(g * HEAD_DIM, (g + 1) * HEAD_DIM)
        vc = slice(half_kv + g * HEAD_DIM, half_kv + (g + 1) * HEAD_DIM)
        k_all = kvbuf[:, :, kc].reshape(seq, HEAD_DIM)
        v_all = kvbuf[:, :, vc].reshape(seq, HEAD_DIM)
        q_g = jnp.concatenate([q_s[:, (g * per_kv + h) * HEAD_DIM:(g * per_kv + h + 1) * HEAD_DIM]
                               for h in range(per_kv)], axis=0)
        s = lax.dot_general(q_g, k_all, (((1,), (1,)), ((), ())), preferred_element_type=F32) * SCORE_SCALE
        s = jnp.where(causal, s, -1e30)
        e = jnp.exp(s - jnp.max(s, axis=1, keepdims=True))
        w = (e / jnp.sum(e, axis=1, keepdims=True)).astype(BF16)
        o_g = jnp.dot(w, v_all, preferred_element_type=F32).astype(BF16)
        gw = per_kv * HEAD_DIM
        for h in range(per_kv):
            o_own[:, g * gw + h * HEAD_DIM:g * gw + (h + 1) * HEAD_DIM] = o_g[h * tok2:(h + 1) * tok2, :]
        cols = pl.ds(g * gw, gw)
        c = remote(o_own.at[:, cols], o_sib.at[:, cols], pair_send.at[3 + g], pair_recv.at[3 + g], sib)
        c.start()
        o_pairs.append(c)

    loads['o0'].wait()
    acc = jnp.dot(o_own[...], wo_v[0:half_q, :], preferred_element_type=F32)
    loads['o1'].wait()
    for c in o_pairs:
        c.wait_recv()
    acc = acc + jnp.dot(o_sib[...], wo_v[half_q:2 * half_q, :], preferred_element_type=F32)
    my_cols = pl.ds(pl.multiple_of(core * half_w, half_w), half_w)
    h_buf[core, b0 * side + a0] = (xbuf[:, my_cols].astype(F32) + acc).astype(BF16)

    hg = Gather(lambda i, j: h_buf.at[core, j * side + i], h_send, h_recv)

    def cross(i, j):
        at = h_buf.at[core, j * side + i]
        return remote(at, at, d_send.at[j * side + i], d_recv.at[j * side + i], sib)

    def cross_from(n):
        at = h_buf.at[1 - core, n]
        return remote(at, at, d_send.at[n], d_recv.at[n], sib)

    relays = {0: 1, 1: -1, side - 1: -1}

    def back(at, d):
        return (at - d + side) % side

    def h_spread(k):
        for d in (1, side - 1) if k in relays else (1, side - 1, 2):
            hg.second(back(a0, k), d).start()

    for d in (1, side - 1, 2):
        hg.first(d).start()
    h_spread(0)
    cross(a0, b0).start()

    def meta_done(n, carry):
        i, j = n // side, n % side

        @pl.when(j != b0)
        def _():
            mt.second_from(i, j).wait_recv()
        return carry

    lax.fori_loop(0, n_chips, meta_done, 0)

    g_tok = side * tok2
    t_row = lax.broadcasted_iota(jnp.int32, (g_tok, g_tok), 0)
    t_col = lax.broadcasted_iota(jnp.int32, (g_tok, g_tok), 1)
    before = jnp.where((t_row < t_col) & (t_row // tok == t_col // tok), 1.0, 0.0).astype(BF16)
    lane_8 = lax.broadcasted_iota(jnp.int32, (8, g_tok), 1)
    source_base = (lane_8 // tok * tok).astype(F32)
    expert_8 = (lax.broadcasted_iota(jnp.int32, (8, g_tok), 0) + me * own_experts).astype(F32)
    slot_row = t_row.astype(F32)

    def select_rows(g, carry):
        for half in range(CORES):
            m = jnp.zeros((8, g_tok), F32)
            for a in range(side):
                m = m + meta_buf[a * side + g if half else g * side + a]
            m = m[4 * half:4 * half + 4, :]
            hit0 = m[0:1, :] == expert_8
            hit1 = m[1:2, :] == expert_8
            hit = hit0 | hit1
            slot = jnp.dot(jnp.where(hit, 1.0, 0.0).astype(BF16), before, preferred_element_type=F32)
            row = jnp.where(hit, slot + source_base, -1.0)
            gate = jnp.where(hit0, m[2:3, :], jnp.where(hit1, m[3:4, :], 0.0))
            for k in range(own_experts):
                rows = pl.ds(k * g_tok, g_tok)
                pick = slot_row == row[k:k + 1, :]
                sel_s[half * side + g, rows, :] = jnp.where(pick, 1.0, 0.0).astype(BF16)
                gate_k = jnp.sum(jnp.where(pick, gate[k:k + 1, :], 0.0), axis=1, keepdims=True)
                gate_s[half * side + g, rows, :] = jnp.broadcast_to(gate_k, (g_tok, LANES))
        return carry

    lax.fori_loop(0, side, select_rows, 0)

    def build(half, g):
        def put(a, k, q, rows):
            cols = pl.ds(pl.multiple_of(half * half_w + q * B_COLS, B_COLS), B_COLS)
            buf_out[k, group_rows(side, tok2, half, g, a), cols] = rows

        build_group(side, tok2, own_experts, h_buf, sel_s, gate_s, half, g, put)

    def take_first(k):
        i = back(a0, k)
        hg.first_from(i).wait_recv()
        h_spread(k)
        cross(i, b0).start()

    def take(k, d):
        i, j = back(a0, k), back(b0, d)
        hg.second_from(i, j).wait_recv()
        if k in relays and d == (relays[k] + side) % side:
            hg.relay(i, relays[k]).start()
        cross(i, j).start()

    def other_done(d):
        for a in range(side):
            cross_from(back(a0, d) * side + a).wait_recv()

    def build_other(d):
        other_done(d)
        build(1 - core, back(a0, d))

    take_first(1)
    take_first(side - 1)
    take(0, 1)
    take_first(2)
    build(core, b0)
    take(1, side - 1)
    take(side - 1, side - 1)
    build_other(0)
    for k in (1, side - 1, 2):
        take(k, 1)
    take(0, side - 1)
    take(2, side - 1)
    for k in (0, 2):
        take(k, 2)
    build(core, back(b0, 1))
    for k in (1, side - 1):
        take(k, 2)
    for d in (1, side - 1, 2):
        other_done(d)

    for c in [x_pair, m_pair, kv_pair] + o_pairs:
        c.wait_send()
    for d in range(1, side):
        for c in range(CORES):
            kv_first(d, c).wait_send()
    for i in range(side):
        kv_second(i, True)
    mt.sent()
    hg.sent()
    for i in range(side):
        for j in range(side):
            cross(i, j).wait_send()


def store_kernel(side, buf_ref, h_ref, sel_ref, gate_ref, buf_out, h_out, stage, sem, stage_sem, h_sem):
    n_exp = buf_ref.shape[0]
    tok2, half_w = h_ref.shape[2:]
    tok = h_out.shape[0]
    me = lax.axis_index('sp')
    core = me % CORES
    chip = me // CORES
    cy = chip // side
    cx = chip % side
    a0 = cx + (cy - cx) * core
    b0 = cy + (cx - cy) * core
    copies = []

    def start(src, dst, s):
        copies.append(pltpu.make_async_copy(src, dst, s))
        copies[-1].start()

    def cols(half):
        return pl.ds(pl.multiple_of(half * half_w, half_w), half_w)

    other = 1 - core
    done = [(core, b0), (core, (b0 - 1 + side) % side), (other, a0)]
    for n, (half, g) in enumerate(done):
        for a in range(side):
            rows = group_rows(side, tok2, half, g, a)
            start(buf_ref.at[:, rows, cols(half)], buf_out.at[:, rows, cols(half)], sem.at[n * side + a])
    my_rows = pl.ds(pl.multiple_of(core * tok, tok), tok)
    for c in range(CORES):
        start(h_ref.at[c, cx * side + cy if c else chip, my_rows, :], h_out.at[:, pl.ds(c * half_w, half_w)], h_sem.at[c])
    rest = [(other, (a0 - 1 + side) % side), (core, (b0 + 1) % side), (core, (b0 + 2) % side), (other, (a0 + 1) % side), (other, (a0 + 2) % side)]
    for n, (half, g) in enumerate(rest):
        def put(a, k, q, rows, n=n):
            stage[n, k, a * tok2:(a + 1) * tok2, q * B_COLS:(q + 1) * B_COLS] = rows

        build_group(side, tok2, n_exp, h_ref, sel_ref, gate_ref, half, g, put)
        for a in range(side):
            start(stage.at[n, :, pl.ds(a * tok2, tok2), :], buf_out.at[:, group_rows(side, tok2, half, g, a), cols(half)],
                  stage_sem.at[n * side + a])
    for c in copies:
        c.wait()


def solution(mesh):
    group = mesh.shape['sp']
    side = math.isqrt(group // CORES)
    row_spec = P(('dp', 'sp'), None)
    buf_spec = P(('dp', 'sp'), None, None)
    any_spec = pl.BlockSpec(memory_space=pl.ANY)
    hbm_spec = pl.BlockSpec(memory_space=pltpu.HBM)
    vmem_spec = pl.BlockSpec(memory_space=pltpu.VMEM)

    def device_step(x_loc, w_q, w_k, w_v, w_o, ids_loc, probs_loc):
        tok, width = x_loc.shape
        experts = probs_loc.shape[1]
        own = experts // group
        chips = side * side
        tok2 = CORES * tok
        half_q = w_q.shape[1] // CORES
        half_kv = w_k.shape[1] // CORES
        half_w = width // CORES
        dma = pltpu.SemaphoreType.DMA
        n_loads = 7 + half_q // Q_COLS
        kv_half_heads = half_kv // HEAD_DIM
        g_tok = side * tok2
        parts = pl.pallas_call(
            functools.partial(block_kernel, side),
            out_shape=(pltpu.VMEM((own, tok * group, width), BF16),
                       pltpu.VMEM((CORES, chips, tok2, half_w), BF16),
                       pltpu.VMEM((CORES * side, own * g_tok, g_tok), BF16),
                       pltpu.VMEM((CORES * side, own * g_tok, LANES), F32)),
            in_specs=[hbm_spec] * 7,
            out_specs=(vmem_spec,) * 4,
            scratch_shapes=[
                pltpu.VMEM((tok2, width), BF16),
                pltpu.VMEM((width, half_q), BF16),
                pltpu.VMEM((width, CORES * half_kv), BF16),
                pltpu.VMEM((width, CORES * half_kv), BF16),
                pltpu.VMEM((2 * half_q, half_w), BF16),
                pltpu.VMEM((2, tok), jnp.int32),
                pltpu.VMEM((tok, experts), F32),
                pltpu.VMEM((CORES, tok, 2 * half_kv), BF16),
                pltpu.VMEM((chips, tok2, 2 * half_kv), BF16),
                pltpu.VMEM((CORES, 8, LANES), F32),
                pltpu.VMEM((chips, 8, LANES), F32),
                pltpu.VMEM((tok2, half_q), BF16),
                pltpu.VMEM((tok2, half_q), BF16),
                pltpu.VMEM((tok2, half_q), BF16),
                dma((n_loads,)),
                dma((3 + kv_half_heads,)), dma((3 + kv_half_heads,)),
                dma((CORES * side,)), dma((CORES * side,)),
                dma((side + chips,)), dma((side + chips,)), dma((side + chips,)), dma((side + chips,)),
                dma((side + chips,)), dma((side + chips,)),
                dma((chips,)), dma((chips,)),
            ],
            compiler_params=pltpu.CompilerParams(collective_id=0, has_side_effects=True,
                                                 vmem_limit_bytes=50 * 2 ** 20 + 900 * 1024),
            name='attention_block',
        )(x_loc, w_q, w_k, w_v, w_o, ids_loc.T, probs_loc)
        buf, h = pl.pallas_call(
            functools.partial(store_kernel, side),
            out_shape=(jax.ShapeDtypeStruct((own, tok * group, width), BF16), jax.ShapeDtypeStruct((tok, width), BF16)),
            in_specs=[vmem_spec] * 4,
            out_specs=(any_spec, any_spec),
            scratch_shapes=[pltpu.VMEM((5, own, g_tok, half_w), BF16),
                            dma((3 * side,)), dma((5 * side,)), dma((CORES,))],
            compiler_params=pltpu.CompilerParams(vmem_limit_bytes=16 * 2 ** 20),
            name='store_outputs',
        )(*parts)
        return h, buf

    return jax.shard_map(device_step, mesh=mesh, in_specs=(row_spec, P(), P(), P(), P(), row_spec, row_spec), out_specs=(row_spec, buf_spec), check_vma=False)
```
